32 devices in a mesh: graph: 16 (over z, y, core), chan: 2 (over x).
Axes of the slice: x: 2, y: 2, z: 4, core: 2. Of those that a mesh axis runs over, the one named last changes fastest.
Arguments:
- embed: bfloat16 [25, 512, 2048], P(None, 'chan', 'graph'), may hold values from -200 to 200
- gain: float32 [5, 512], P(None, 'chan'), may hold values from 0.25 to 1.75
- w_zero: bfloat16 [5, 512, 2560], P(None, 'chan'), may hold values from -0.125 to 0.125
- w_one: bfloat16 [2, 4, 512, 2048], P(None, None, 'chan'), may hold values from -0.125 to 0.125
- w_two: bfloat16 [2, 3, 512, 1536], P(None, None, 'chan'), may hold values from -0.15625 to 0.15625
- rot_table: float32 [19, 25, 256], replicated, may hold values from -1 to 1, as said below
- face_atoms: int32 [512], P('graph'), may hold values from 0 to 127, as said below
- edge_source: int32 [2048], P('graph'), may hold values from 0 to 159
- edge_target: int32 [2048], P('graph'), may hold values from 0 to 127
- rot_index: int32 [2048], P('graph'), may hold values from 0 to 255
- edge_weight: float32 [2048], P('graph'), may hold values from 0.2 to 1
- cotangent: bfloat16 [25, 512, 2048], P(None, 'chan', 'graph'), may hold values from -1.5 to 1.5
Outputs:
- update: bfloat16 [25, 512, 2048], P(None, 'chan', 'graph')
- grad_embed: bfloat16 [25, 512, 2048], P(None, 'chan', 'graph')
- grad_zero: float32 [5, 512, 2560], P(None, 'chan', 'graph')
- grad_one: float32 [2, 4, 512, 2048], P(None, None, 'chan', 'graph')
- grad_two: float32 [2, 3, 512, 1536], P(None, None, 'chan', 'graph')
The draws below stay inside these ranges and needn't reach their ends.
Inputs may be any that keep to these rules, and one draw needn't show every extreme that they name: `rot_table`: for every rotation, frame row (m, l) is nonzero only on the 2l + 1 coefficients of degree l, where it is row l + m of an orthogonal (2l + 1)-square matrix shared by the rows of that degree; the degree-0 entry is 1. `face_atoms`: block b holds 32 distinct atom indices counted from the first atom of block b: the first 16 lie at the face toward block b - 1, the last 16 at the face toward block b + 1. `edge_source`: read as in the step that defines src. `edge_target`: counted from the first atom of the edge's block.
All inputs are finite; a program needn't handle non-finite values.
Results may differ from the reference program's by a relative error of at most 0.0062.
Values may be sent and summed in bfloat16 or wider, within the bound.
A program may use at most 192 MiB of HBM per device.

```python
import math
import jax
import jax.numpy as jnp
from jax import lax

C = 512
ATOM_DEV = 128
HALO = 16
EDGE_DEV = 128
ROTS = 256
ATOMS = 2048
EDGES = 2048
FACES = 512
N_GRAPH = 16


FRAME = ((0, 0), (1, 0), (2, 0), (3, 0), (4, 0), (1, 1), (2, 1), (3, 1), (4, 1), (1, -1), (2, -1), (3, -1), (4, -1), (2, 2), (3, 2), (4, 2), (2, -2), (3, -2), (4, -2))


def draw_embed(key, part):
    keys = jax.random.split(key, 4)
    ramp = jnp.arange(C, dtype=jnp.float32) / C - 0.5
    channel_scale = jnp.exp(math.log(10.0) * ramp) * jax.random.uniform(keys[1], (C,), jnp.float32, 0.7, 1.4)
    atom_scale = jnp.exp(jax.random.uniform(keys[2], (ATOMS,), jnp.float32, math.log(0.3), math.log(3.0)))
    raw = jnp.clip(jax.random.normal(keys[0], (25, C, ATOMS), jnp.float32), -6.0, 6.0)
    values = raw * channel_scale[None, :, None] * atom_scale[None, None, :]
    return jnp.clip(values, -200.0, 200.0).astype(jnp.bfloat16)


def reflect_block(key, size):
    matrix = jnp.broadcast_to(jnp.eye(size, dtype=jnp.float32), (ROTS, size, size))
    for index in range(size):
        vector = jax.random.normal(jax.random.fold_in(key, index), (ROTS, size), jnp.float32)
        vector = vector / jnp.sqrt(jnp.sum(vector * vector, axis=1, keepdims=True) + 1e-12)
        folded = jnp.einsum('rj,rjk->rk', vector, matrix)
        matrix = matrix - 2.0 * vector[:, :, None] * folded[:, None, :]
    return matrix


def draw_rot_table(key, part):
    blocks = [jnp.ones((ROTS, 1, 1), jnp.float32)]
    for degree in range(1, 5):
        blocks.append(reflect_block(jax.random.fold_in(key, 100 + degree), 2 * degree + 1))
    lines = []
    for pair in FRAME:
        degree = pair[0]
        line = jnp.zeros((ROTS, 25), jnp.float32)
        line = line.at[:, degree * degree:(degree + 1) * (degree + 1)].set(blocks[degree][:, degree + pair[1], :])
        lines.append(line)
    table = jnp.stack(lines, axis=0)
    return jnp.transpose(table, (0, 2, 1))


def draw_face_atoms(key, part):
    count = FACES // (2 * HALO)
    keys = jax.random.split(key, count)
    picks = jax.vmap(lambda single: jax.random.permutation(single, ATOM_DEV)[:2 * HALO])(keys)
    return picks.reshape(FACES).astype(jnp.int32)


def with_ends(entries, own_key, low, largest):
    longest = entries.shape.index(max(entries.shape))
    spots = []
    for shift in (0, 1):
        where = [jax.random.randint(jax.random.fold_in(own_key, axis), (), 0, length) for axis, length in enumerate(entries.shape)]
        where[longest] = (where[longest] + shift) % entries.shape[longest]
        spots.append(tuple(where))
    return entries.at[spots[0]].set(low).at[spots[1]].set(largest)


def steps_of(own_key, extent, shards, low, high):
    def one(axis_at, blocks):
        heights = jax.random.uniform(jax.random.fold_in(jax.random.fold_in(own_key, 6), axis_at), (blocks,), jnp.float32, low / len(shards), high / len(shards))
        return jnp.repeat(jnp.exp(heights), extent[axis_at] // blocks).reshape((-1,) + (1,) * (len(extent) - axis_at - 1))

    factor_of = one(*shards[0])
    for cut in shards[1:]:
        factor_of = factor_of * one(*cut)
    return factor_of


def normal_values(rng, dims, scale, reach, cuts=(), kind=jnp.bfloat16):
    entries = scale * jax.random.normal(rng, dims, jnp.float32)
    if cuts:
        entries = entries * steps_of(rng, dims, cuts, -0.22, 0.18)
    return jnp.clip(entries, -reach, reach).astype(kind)


def setup_inputs(seed: int = 0) -> dict:
    splits = jax.random.split(jax.random.key(seed), 13)
    embed = draw_embed(jax.random.fold_in(splits[12], 71), 0)
    gain = jnp.clip(1.0 + 0.15 * jax.random.normal(splits[1], (5, C), jnp.float32), 0.25, 1.75)
    w_zero = normal_values(splits[2], (5, C, 5 * C), (5 * C) ** -0.5, 0.125, ((1, 2),))
    w_one = normal_values(splits[3], (2, 4, C, 4 * C), (4 * C) ** -0.5, 0.125, ((2, 2),))
    w_two = normal_values(splits[4], (2, 3, C, 3 * C), (3 * C) ** -0.5, 0.15625, ((2, 2),))
    rot_table = draw_rot_table(jax.random.fold_in(splits[12], 71), 0)
    face_atoms = draw_face_atoms(jax.random.fold_in(splits[12], 71), 0)
    edge_source = with_ends(jax.random.randint(splits[7], (EDGES,), 0, ATOM_DEV + 2 * HALO), jax.random.fold_in(splits[7], 1), 0, (ATOM_DEV + 2 * HALO) - 1).astype(jnp.int32)
    edge_target = with_ends(jax.random.randint(splits[8], (EDGES,), 0, ATOM_DEV), jax.random.fold_in(splits[8], 1), 0, ATOM_DEV - 1).astype(jnp.int32)
    rot_index = with_ends(jax.random.randint(splits[9], (EDGES,), 0, ROTS), jax.random.fold_in(splits[9], 1), 0, ROTS - 1).astype(jnp.int32)
    edge_weight = jnp.clip(jnp.exp(math.log(1.0) - 1.609438 * jax.random.uniform(splits[10], (EDGES,), jnp.float32) ** steps_of(splits[10], (EDGES,), ((0, 16),), -0.2, 0.2)), 0.2, 1.0)
    cotangent = normal_values(splits[11], (25, C, ATOMS), 0.25, 1.5, ((1, 2), (2, 16)))
    return {"embed": embed, "gain": gain, "w_zero": w_zero, "w_one": w_one, "w_two": w_two, "rot_table": rot_table, "face_atoms": face_atoms, "edge_source": edge_source, "edge_target": edge_target, "rot_index": rot_index, "edge_weight": edge_weight, "cotangent": cotangent}


EPSILON = 1e-06
HIGHEST = lax.Precision.HIGHEST
FRAME = ((0, 0), (1, 0), (2, 0), (3, 0), (4, 0), (1, 1), (2, 1), (3, 1), (4, 1), (1, -1), (2, -1), (3, -1), (4, -1), (2, 2), (3, 2), (4, 2), (2, -2), (3, -2), (4, -2))

def gain_rows(gain):
    pieces = [jnp.broadcast_to(gain[degree:degree + 1], (2 * degree + 1, gain.shape[1])) for degree in range(5)]
    return jnp.concatenate(pieces, axis=0)

def product(left, right):
    return jnp.dot(left, right, preferred_element_type=jnp.float32)

def across(left, right):
    return lax.dot_general(left, right, (((0,), (0,)), ((), ())), preferred_element_type=jnp.float32)

def outer(left, right):
    return lax.dot_general(left, right, (((1,), (1,)), ((), ())), preferred_element_type=jnp.float32)

def stack_frame(parts, width, edges):
    row_counts = (5, 4, 4, 3, 3)
    return jnp.concatenate([part.reshape(rows, width, edges) for part, rows in zip(parts, row_counts)], axis=0)

def mix_part(w_zero, w_one, w_two, piece, start):
    count = piece.shape[1]
    edges = piece.shape[2]
    outputs = w_zero.shape[1]

    def columns(weight, blocks):
        shaped = weight.reshape(blocks * outputs, blocks, weight.shape[-1] // blocks)
        return lax.dynamic_slice_in_dim(shaped, start, count, 2).reshape(blocks * outputs, blocks * count)

    def frame_rows(first, blocks):
        return piece[first:first + blocks].reshape(blocks * count, edges)
    parts = [product(columns(w_zero, 5), frame_rows(0, 5))]
    for weights, first, blocks in ((w_one, 5, 4), (w_two, 13, 3)):
        real_part = columns(weights[0], blocks)
        imag_part = columns(weights[1], blocks)
        plus = frame_rows(first, blocks)
        minus = frame_rows(first + blocks, blocks)
        parts.append(product(real_part, plus) - product(imag_part, minus))
        parts.append(product(real_part, minus) + product(imag_part, plus))
    return tuple(parts)

def mix_backward(w_zero, w_one, w_two, grads, frame):
    outputs = grads.shape[1]
    width = frame.shape[1]
    edges = grads.shape[2]

    def grad_rows(first, blocks):
        return grads[first:first + blocks].reshape(blocks * outputs, edges)

    def frame_rows(first, blocks):
        return frame[first:first + blocks].reshape(blocks * width, edges)
    zero_weight = w_zero.reshape(5 * outputs, 5 * width)
    grad_first = grad_rows(0, 5)
    back = [across(zero_weight, grad_first)]
    weight_zero = outer(grad_first, frame_rows(0, 5)).reshape(5, outputs, 5 * width)
    pairs = []
    for weights, first, blocks in ((w_one, 5, 4), (w_two, 13, 3)):
        real_part = weights[0].reshape(blocks * outputs, blocks * width)
        imag_part = weights[1].reshape(blocks * outputs, blocks * width)
        grad_plus = grad_rows(first, blocks)
        grad_minus = grad_rows(first + blocks, blocks)
        frame_plus = frame_rows(first, blocks)
        frame_minus = frame_rows(first + blocks, blocks)
        back.append(across(real_part, grad_plus) + across(imag_part, grad_minus))
        back.append(across(real_part, grad_minus) - across(imag_part, grad_plus))
        real_grad = outer(grad_plus, frame_plus) + outer(grad_minus, frame_minus)
        imag_grad = outer(grad_minus, frame_plus) - outer(grad_plus, frame_minus)
        pairs.append(jnp.stack([real_grad.reshape(blocks, outputs, blocks * width), imag_grad.reshape(blocks, outputs, blocks * width)]))
    return (stack_frame(back, width, edges), weight_zero, pairs[0], pairs[1])

def reference(embed, gain, w_zero, w_one, w_two, rot_table, face_atoms, edge_source, edge_target, rot_index, edge_weight, cotangent):
    values = embed.astype(jnp.float32)
    gains = gain_rows(gain)
    inverse = lax.rsqrt(lax.optimization_barrier(jnp.sum(values * values, axis=(0, 1))) / (25 * C) + EPSILON)
    normed = (values * inverse[None, None, :] * gains[:, :, None]).astype(jnp.bfloat16)
    positions = jnp.arange(ATOM_DEV, dtype=jnp.int32)

    def shard_step(carry, shard):
        update, grad_normed, grad_zero, grad_one, grad_two = carry
        left = (shard - 1) % N_GRAPH
        right = (shard + 1) % N_GRAPH
        from_left = lax.dynamic_slice_in_dim(face_atoms, left * (2 * HALO) + HALO, HALO)
        from_right = lax.dynamic_slice_in_dim(face_atoms, right * (2 * HALO), HALO)
        lookup = jnp.concatenate([shard * ATOM_DEV + positions, left * ATOM_DEV + from_left, right * ATOM_DEV + from_right]).astype(jnp.int32)
        first = (shard * EDGE_DEV).astype(jnp.int32)
        sources = lookup[lax.dynamic_slice_in_dim(edge_source, first, EDGE_DEV)]
        targets = (shard * ATOM_DEV + lax.dynamic_slice_in_dim(edge_target, first, EDGE_DEV)).astype(jnp.int32)
        rotations = jnp.take(rot_table, lax.dynamic_slice_in_dim(rot_index, first, EDGE_DEV), axis=2)
        scale = lax.dynamic_slice_in_dim(edge_weight, first, EDGE_DEV)
        gathered = jnp.take(normed, sources, axis=2).astype(jnp.float32)
        frame = jnp.einsum('jke,kce->jce', rotations, gathered, precision=HIGHEST).astype(jnp.bfloat16)
        mixed = stack_frame(mix_part(w_zero, w_one, w_two, frame, 0), C, EDGE_DEV)
        message = jnp.einsum('jke,jce->kce', rotations, mixed * scale[None, None, :], precision=HIGHEST).astype(jnp.bfloat16)
        update = update.at[:, :, targets].add(message.astype(jnp.float32))
        arriving = jnp.take(cotangent, targets, axis=2).astype(jnp.float32)
        grads = (jnp.einsum('jke,kce->jce', rotations, arriving, precision=HIGHEST) * scale[None, None, :]).astype(jnp.bfloat16)
        back, part_zero, part_one, part_two = mix_backward(w_zero, w_one, w_two, grads, frame)
        spread = jnp.einsum('jke,jce->kce', rotations, back, precision=HIGHEST)
        grad_normed = grad_normed.at[:, :, sources].add(spread)
        return ((update, grad_normed, grad_zero + part_zero, grad_one + part_one, grad_two + part_two), None)
    start = (jnp.zeros((25, C, ATOMS), jnp.float32), jnp.zeros((25, C, ATOMS), jnp.float32), jnp.zeros((5, C, 5 * C), jnp.float32), jnp.zeros((2, 4, C, 4 * C), jnp.float32), jnp.zeros((2, 3, C, 3 * C), jnp.float32))
    final, unused = lax.scan(shard_step, start, jnp.arange(N_GRAPH, dtype=jnp.int32))
    update, grad_normed, grad_zero, grad_one, grad_two = final
    tally = lax.optimization_barrier(jnp.sum(values * gains[:, :, None] * grad_normed, axis=(0, 1)))
    grad_embed = (inverse[None, None, :] * gains[:, :, None] * grad_normed - values * (inverse ** 3 * tally / (25 * C))[None, None, :]).astype(jnp.bfloat16)
    return (update.astype(jnp.bfloat16), grad_embed, grad_zero, grad_one, grad_two)
```

```python
import functools

import jax
import jax.numpy as jnp
from jax import lax
from jax.experimental import pallas as pl
from jax.experimental.pallas import tpu as pltpu
from jax.sharding import PartitionSpec as P


EPSILON = 1e-06
HIGHEST = lax.Precision.HIGHEST
FRAME = (
    (0, 0),
    (1, 0),
    (2, 0),
    (3, 0),
    (4, 0),
    (1, 1),
    (2, 1),
    (3, 1),
    (4, 1),
    (1, -1),
    (2, -1),
    (3, -1),
    (4, -1),
    (2, 2),
    (3, 2),
    (4, 2),
    (2, -2),
    (3, -2),
    (4, -2),
)


def gain_rows(gain):
    pieces = [
        jnp.broadcast_to(gain[degree : degree + 1], (2 * degree + 1, gain.shape[1]))
        for degree in range(5)
    ]
    return jnp.concatenate(pieces, axis=0)


def product(left, right):
    return jnp.dot(left, right, preferred_element_type=jnp.float32)


def across(left, right):
    return lax.dot_general(
        left, right, (((0,), (0,)), ((), ())), preferred_element_type=jnp.float32
    )


def contract(left, right):
    return lax.dot_general(left, right, (((2,), (1,)), ((), ())), preferred_element_type=jnp.float32)


def frames_kernel(*refs):
    pairs, (rotations, scale, out) = refs[:-3], refs[-3:]
    count, width = pairs[0].shape[0], pairs[0].shape[1]
    total = None
    for values, picks in zip(pairs[0::2], pairs[1::2]):
        part = product(values[...].reshape(count * width, values.shape[2]), picks[...])
        total = part if total is None else total + part
    total = total.reshape(count, width, total.shape[1])
    for row, (degree, _) in enumerate(FRAME):
        first = degree * degree
        entry = row * count + first
        line = rotations[entry : entry + 1, :] * total[first]
        for step in range(1, 2 * degree + 1):
            entry = row * count + first + step
            line = line + rotations[entry : entry + 1, :] * total[first + step]
        out[row] = (line * scale[...]).astype(out.dtype)


def to_frames(pairs, rotations, scale):
    count, local = pairs[0][0].shape[0], pairs[0][0].shape[1]
    edges = scale.shape[1]
    block = min(64, local)
    operands, specs = [], []
    for values, picks in pairs:
        operands += [values, picks]
        specs.append(pl.BlockSpec((count, block, values.shape[2]), lambda i: (0, i, 0)))
        specs.append(pl.BlockSpec(picks.shape, lambda i: (0, 0)))
    for whole in (rotations, scale):
        operands.append(whole)
        specs.append(pl.BlockSpec(whole.shape, lambda i: (0, 0)))
    return pl.pallas_call(
        frames_kernel,
        grid=(local // block,),
        in_specs=specs,
        out_specs=pl.BlockSpec((len(FRAME), block, edges), lambda i: (0, i, 0)),
        out_shape=jax.ShapeDtypeStruct((len(FRAME), local, edges), jnp.bfloat16),
        compiler_params=pltpu.CompilerParams(dimension_semantics=("arbitrary",)),
    )(*operands)


def atoms_kernel(count, values, rotations, scale, *refs):
    picks, outs, held = refs[: len(refs) // 2], refs[len(refs) // 2 : -1], refs[-1]
    width, edges = values.shape[1], values.shape[2]
    for degree in range(5):
        members = [row for row, pair in enumerate(FRAME) if pair[0] == degree]
        lines = [values[row].astype(jnp.float32) * scale[...] for row in members]
        for column in range(degree * degree, (degree + 1) * (degree + 1)):
            total = None
            for row, line in zip(members, lines):
                entry = row * count + column
                term = rotations[entry : entry + 1, :] * line
                total = term if total is None else total + term
            held[column] = total.astype(held.dtype)
    flat = held[...].reshape(count * width, edges)
    for pick, out in zip(picks, outs):
        out[...] = product(flat, pick[...]).reshape(out.shape).astype(out.dtype)


def to_atoms(values, rotations, scale, picks, kinds):
    rows, local, edges = values.shape
    count = rotations.shape[0] // rows
    block = min(64, local)
    whole = lambda i: (0, 0)
    return pl.pallas_call(
        functools.partial(atoms_kernel, count),
        grid=(local // block,),
        in_specs=[
            pl.BlockSpec((rows, block, edges), lambda i: (0, i, 0)),
            pl.BlockSpec(rotations.shape, whole),
            pl.BlockSpec(scale.shape, whole),
        ]
        + [pl.BlockSpec(pick.shape, whole) for pick in picks],
        out_specs=[
            pl.BlockSpec((count, block, pick.shape[1]), lambda i: (0, i, 0)) for pick in picks
        ],
        out_shape=[
            jax.ShapeDtypeStruct((count, local, pick.shape[1]), kind)
            for pick, kind in zip(picks, kinds)
        ],
        scratch_shapes=[pltpu.VMEM((count, block, edges), jnp.bfloat16)],
        compiler_params=pltpu.CompilerParams(dimension_semantics=("arbitrary",)),
    )(values, rotations, scale, *picks)


def swap(block, bit):
    count = lax.axis_size("graph")
    return lax.ppermute(block, "graph", [(i, i ^ bit) for i in range(count)])


def from_beside(faces, width):
    count = lax.axis_size("graph")
    forward = [(i, (i + 1) % count) for i in range(count)]
    backward = [(target, source) for source, target in forward]
    low = lax.ppermute(faces[:, :, width:], "graph", forward)
    high = lax.ppermute(faces[:, :, :width], "graph", backward)
    return jnp.concatenate([low, high], axis=2)


def hot_rows(size, codes):
    return (jnp.arange(size, dtype=jnp.int32)[:, None] == codes[None, :]).astype(jnp.bfloat16)


def hot_columns(codes, size):
    return (codes[:, None] == jnp.arange(size, dtype=jnp.int32)[None, :]).astype(jnp.bfloat16)


def beside(plus, minus, axis=-1):
    return jnp.concatenate([plus, minus], axis=axis)


def mix_forward(weights, frame):
    w_zero, w_one, w_two = weights
    edges = frame.shape[2]
    local = w_zero.shape[1]
    mixed = [
        product(w_zero.reshape(-1, w_zero.shape[2]), frame[:5].reshape(-1, edges)).reshape(
            5, local, edges
        )
    ]
    for weight, first, blocks in ((w_one, 5, 4), (w_two, 13, 3)):
        plus = frame[first : first + blocks].reshape(-1, edges)
        minus = frame[first + blocks : first + 2 * blocks].reshape(-1, edges)
        both = product(weight.reshape(-1, weight.shape[-1]), beside(plus, minus))
        both = both.reshape(2, blocks, local, 2 * edges)
        mixed.append(both[0, :, :, :edges] - both[1, :, :, edges:])
        mixed.append(both[0, :, :, edges:] + both[1, :, :, :edges])
    return jnp.concatenate(mixed, axis=0)


def mix_back(weights, grads, shares):
    w_zero, w_one, w_two = weights
    edges = grads.shape[2]

    def shared(block, blocks):
        shaped = block.reshape(blocks, shares, -1, edges).astype(jnp.bfloat16)
        return jnp.transpose(shaped, (1, 0, 2, 3))

    back = [
        shared(across(w_zero.reshape(-1, w_zero.shape[2]), grads[:5].reshape(-1, edges)), 5)
    ]
    for weight, first, blocks in ((w_one, 5, 4), (w_two, 13, 3)):
        plus = grads[first : first + blocks].reshape(-1, edges)
        minus = grads[first + blocks : first + 2 * blocks].reshape(-1, edges)
        sides = jnp.concatenate([beside(plus, minus), beside(minus, -plus)], axis=0)
        both = across(weight.reshape(-1, weight.shape[-1]), sides)
        back.append(shared(both[:, :edges], blocks))
        back.append(shared(both[:, edges:], blocks))
    return jnp.concatenate(back, axis=1)


def column_frames(frame):
    count = lax.axis_size("graph")
    near = 4
    far = count // near
    edges = frame.shape[2]
    cuts = ((0, 5), (5, 4), (9, 4), (13, 3), (16, 3))
    parts = [
        frame[first : first + blocks].reshape(far, near, -1, edges) for first, blocks in cuts
    ]
    widths = [part.shape[2] for part in parts]
    packed = jnp.concatenate(parts, axis=2)
    mine = lax.axis_index("graph") % near
    frames = []
    for bit in (0, 2, 1, 3):
        target = mine ^ bit
        chunk = lax.dynamic_index_in_dim(packed, target, axis=1, keepdims=False)
        frames.append(swap(chunk, bit) if bit else chunk)
    return frames, widths


def weight_grads(frames, widths, grads_all, local):
    count = lax.axis_size("graph")
    near = 4
    far = count // near
    edges = frames[0].shape[2]
    starts = [sum(widths[:i]) for i in range(5)]
    groups = [[z * near + q for z in range(far)] for q in range(near)]

    def settle(partial):
        return lax.psum_scatter(
            partial.astype(jnp.bfloat16),
            "graph",
            scatter_dimension=0,
            axis_index_groups=groups,
            tiled=False,
        ).astype(jnp.float32)

    def settle_direct(partial):
        partial = partial.astype(jnp.bfloat16)
        place = lax.axis_index("graph") // near
        total = lax.dynamic_index_in_dim(partial, place, axis=0, keepdims=False)
        total = total.astype(jnp.float32)
        for step in range(1, far):
            chunk = lax.dynamic_index_in_dim(partial, (place + step) % far, axis=0, keepdims=False)
            shift = [(i, (i + step * near) % count) for i in range(count)]
            total = total + lax.ppermute(chunk, "graph", shift).astype(jnp.float32)
        return total

    def columns(index):
        return [chunk[:, starts[index] : starts[index] + widths[index]] for chunk in frames]

    left = jnp.concatenate(columns(0), axis=2)
    right = jnp.concatenate([g[:5].reshape(-1, edges) for g in grads_all], axis=1)
    done = settle_direct(contract(left, right))
    results = [jnp.transpose(done).reshape(5, local, widths[0])]
    for index, first, blocks in ((1, 5, 4), (3, 13, 3)):
        plus, minus = columns(index), columns(index + 1)
        real_part = jnp.concatenate([x for pair in zip(plus, minus) for x in pair], axis=2)
        imag_part = jnp.concatenate([x for pair in zip(minus, plus) for x in (-pair[0], pair[1])], axis=2)
        left = jnp.concatenate([real_part, imag_part], axis=1)
        right = jnp.concatenate(
            [
                g[start : start + blocks].reshape(-1, edges)
                for g in grads_all
                for start in (first, first + blocks)
            ],
            axis=1,
        )
        done = settle(contract(left, right))
        done = done.reshape(2, widths[index], blocks * local)
        results.append(jnp.transpose(done, (0, 2, 1)).reshape(2, blocks, local, widths[index]))
    return results


NEAR = 4


def lanes(start, size):
    return pl.ds(pl.multiple_of(start, 128), size)


def turned(left, right):
    return lax.dot_general(
        left, right, (((1,), (1,)), ((), ())), preferred_element_type=jnp.float32
    )


class Links:
    def __init__(self, sends, recvs):
        self.sends, self.recvs, self.count, self.started = sends, recvs, 0, []

    def make(self, source, target, device):
        index = self.count
        self.count += 1
        return pltpu.make_async_remote_copy(
            src_ref=source,
            dst_ref=target,
            send_sem=self.sends.at[index],
            recv_sem=self.recvs.at[index],
            device_id=device,
            device_id_type=pl.DeviceIdType.MESH,
        )

    def start(self, source, target, device):
        copy = self.make(source, target, device)
        copy.start()
        self.started.append(copy)
        return copy

    def finish(self):
        for copy in self.started:
            copy.wait_send()


def core_kernel(shares, *refs):
    (own, grads, w_zero, w_one, w_two) = refs[:5]
    (mixed, back, out_zero, out_one, out_two) = refs[5:10]
    (v_zero, v_one, v_two, fa_zero, fa_one, fa_two, g_zero, g_one, g_two) = refs[10:19]
    (gr_one, gr_two, f_zero, f_one, f_two) = refs[19:24]
    (bs_zero, bs_one, bs_two, br_zero, br_one, br_two) = refs[24:30]
    (pk_zero, pk_one, pk_two, ps_zero, ps_one, ps_two) = refs[30:36]
    (pr_zero, pr_one, pr_two, zs_zero, zs_one, zs_two, zr_zero, zr_one, zr_two) = refs[36:45]
    sends, recvs, local_sems = refs[45:48]
    width, edges = own.shape[1], own.shape[2]
    channels = width * shares
    me = lax.axis_index("graph")
    share = lax.axis_index("chan")
    low = me % 2
    side = (me // 2) % 2
    pair = (me // 4) % 2
    far = (me // 8) % 2
    slot = pair * 2 + low

    def flip(bit):
        parts = {1: low, 2: side, 4: pair, 8: far}
        place = me
        for one in (1, 2, 4, 8):
            if bit & one:
                place = place + one - 2 * one * parts[one]
        return (place, share)

    peers = [(share + step) % shares for step in range(1, shares)]
    copies = []

    def bring(source, target):
        copy = pltpu.make_async_copy(source, target, local_sems.at[len(copies)])
        copy.start()
        copies.append(copy)
        return copy

    sets = (
        (fa_one, g_one, gr_one, f_one, bs_one, br_one, pk_one, ps_one, pr_one, zs_one, zr_one, v_one, out_one, 5, 4),
        (fa_zero, g_zero, None, f_zero, bs_zero, br_zero, pk_zero, ps_zero, pr_zero, zs_zero, zr_zero, v_zero, out_zero, 0, 5),
        (fa_two, g_two, gr_two, f_two, bs_two, br_two, pk_two, ps_two, pr_two, zs_two, zr_two, v_two, out_two, 13, 3),
    )
    loads = []
    for fa, g, gr, f, bs, br, pk, ps, pr, zs, zr, v, out, first, blocks in sets:
        parts = 1 if gr is None else 2
        ours = fa.reshape(blocks, shares, width, parts * edges)
        for part in range(parts):
            rows = pl.ds(first + part * blocks, blocks)
            loads.append(bring(own.at[rows], ours.at[:, share, :, pl.ds(part * edges, edges)]))
            spot = g.reshape(blocks, width, parts * NEAR * edges)
            loads.append(
                bring(grads.at[rows], spot.at[:, :, lanes((part * NEAR + slot) * edges, edges)])
            )
    held = [bring(w_one, v_one), bring(w_zero, v_zero), bring(w_two, v_two)]

    barrier = pltpu.get_barrier_semaphore()
    others = [flip(bit) for bit in (1, 2, 4, 5, 8)] + [(me, peer) for peer in peers]
    for other in others:
        pl.semaphore_signal(
            barrier, inc=1, device_id=other, device_id_type=pl.DeviceIdType.MESH
        )
    pl.semaphore_wait(barrier, len(others))

    links = Links(sends, recvs)
    for load in loads:
        load.wait()

    gathered = []
    for fa, g, gr, f, bs, br, pk, ps, pr, zs, zr, v, out, first, blocks in sets:
        parts = 1 if gr is None else 2
        ours = fa.reshape(blocks, shares, width, parts * edges).at[:, share]
        gathered.append([links.start(ours, ours, (me, peer)) for peer in peers])

    near = []
    for fa, g, gr, f, bs, br, pk, ps, pr, zs, zr, v, out, first, blocks in sets:
        parts = 1 if gr is None else 2
        spots = [g.at[:, lanes((part * NEAR + slot) * edges, edges)] for part in range(parts)]
        near.append(
            [[links.start(spot, spot, flip(4)) for spot in spots]]
            + [[links.start(spot, spot, flip(1)) for spot in spots]]
        )

    scattered = []
    for at, (fa, g, gr, f, bs, br, pk, ps, pr, zs, zr, v, out, first, blocks) in enumerate(sets):
        if gr is not None:
            tall = blocks * width
            plus = g[:, lanes(slot * edges, edges)]
            minus = g[:, lanes((NEAR + slot) * edges, edges)]
            gr[:tall, :edges] = plus
            gr[:tall, edges:] = minus
            gr[tall:, :edges] = minus
            gr[tall:, edges:] = -plus
            rights = lambda: gr[...]
        else:
            rights = lambda: g[:, lanes(slot * edges, edges)]
        held[at].wait()

        def backed(row, share_at):
            start = lanes(row * channels + share_at * width, width)
            left = v[..., start]
            return across(left.reshape(-1, width), rights())

        group = []
        for index, peer in enumerate(peers):

            def one(row, unused):
                bs[index, row] = backed(row, peer).astype(bs.dtype)
                return unused

            lax.fori_loop(0, blocks, one, 0)
            group.append(links.start(bs.at[index], br.at[index], (me, peer)))
        scattered.append(group)
        relays = []
        for part, copy in enumerate(near[at][0]):
            copy.wait_recv()
            parts = len(near[at][0])
            spot = g.at[:, lanes((part * NEAR + (1 - pair) * 2 + low) * edges, edges)]
            relays.append(links.start(spot, spot, flip(1)))
        near[at].append(relays)

        def kept(row, unused):
            value = backed(row, share)
            back[first + row] = value[:, :edges]
            if gr is not None:
                back[first + blocks + row] = value[:, edges:]
            return unused

        lax.fori_loop(0, blocks, kept, 0)

    aside = []
    for at, (fa, g, gr, f, bs, br, pk, ps, pr, zs, zr, v, out, first, blocks) in enumerate(sets):
        for copy in gathered[at]:
            copy.wait_recv()
        parts = 1 if gr is None else 2
        tall = f.shape[2] // parts
        cut = fa.reshape(2, 2, 2, 2, tall, parts * edges)
        arrivals = []
        for part in range(parts):
            here = f.at[:, :, pl.ds(0, tall), lanes((part * NEAR + slot) * edges, edges)]
            arrivals.append(
                bring(cut.at[:, pair, :, low, :, pl.ds(part * edges, edges)], here).wait
            )
            for bit in (4, 5, 1):
                its_pair = 1 - pair if bit & 4 else pair
                its_low = 1 - low if bit & 1 else low
                arrivals.append(
                    links.start(
                        cut.at[:, its_pair, :, its_low, :, pl.ds(part * edges, edges)],
                        here,
                        flip(bit),
                    ).wait_recv
                )

        if gr is None:

            def mix(row, unused):
                mixed[first + row] = product(v[row], fa[...])
                return unused

        else:

            def mix(row, unused):
                real = product(v[0, row], fa[...])
                imag = product(v[1, row], fa[...])
                mixed[first + row] = real[:, :edges] - imag[:, edges:]
                mixed[first + blocks + row] = real[:, edges:] + imag[:, :edges]
                return unused

        lax.fori_loop(0, blocks, mix, 0)
        for arrive in arrivals:
            arrive()
        for copies_of in near[at][1:]:
            for copy in copies_of:
                copy.wait_recv()
        span = NEAR * edges
        if parts == 2:
            for one_far in range(2):
                for one_side in range(2):
                    f[one_far, one_side, tall:, :span] = -f[one_far, one_side, :tall, span:]
                    f[one_far, one_side, tall:, span:] = f[one_far, one_side, :tall, :span]
        tile = min(256, g.shape[0])

        def grown(step, one_side):
            left = f[:, one_side].reshape(-1, f.shape[3])
            value = turned(left, g[pl.ds(pl.multiple_of(step * tile, tile), tile), :])
            return value.reshape(2, -1, tile)

        def leave(step, unused):
            ps[:, :, lanes(step * tile, tile)] = grown(step, 1 - side).astype(ps.dtype)
            return unused

        def stay(step, unused):
            pk[:, :, lanes(step * tile, tile)] = grown(step, side)
            return unused

        lax.fori_loop(0, g.shape[0] // tile, leave, 0)
        aside.append(
            [
                links.start(ps.at[1 - far], pr.at[1 - far], flip(2)),
                links.start(ps.at[far], pr.at[far], flip(2)),
            ]
        )
        lax.fori_loop(0, g.shape[0] // tile, stay, 0)

    away = []
    for at, (fa, g, gr, f, bs, br, pk, ps, pr, zs, zr, v, out, first, blocks) in enumerate(sets):
        aside[at][0].wait_recv()
        zs[...] = (pk[1 - far] + pr[1 - far].astype(jnp.float32)).astype(zs.dtype)
        away.append(links.start(zs, zr, flip(8)))
        for index, copy in enumerate(scattered[at]):
            copy.wait_recv()
            for row in range(blocks):
                arrived = br[index, row].astype(jnp.float32)
                back[first + row] += arrived[:, :edges]
                if gr is not None:
                    back[first + blocks + row] += arrived[:, edges:]
    for at, (fa, g, gr, f, bs, br, pk, ps, pr, zs, zr, v, out, first, blocks) in enumerate(sets):
        aside[at][1].wait_recv()
        total = pk[far] + pr[far].astype(jnp.float32)
        away[at].wait_recv()
        out[...] = total + zr[...].astype(jnp.float32)
    links.finish()


def run_core(own, grads, weights, shares):
    w_zero, w_one, w_two = weights
    rows, width, edges = own.shape
    channels = width * shares
    count = lax.axis_size("graph")
    cuts = (w_zero.shape[2] // count, w_one.shape[3] // count, w_two.shape[3] // count)
    bf16, f32 = jnp.bfloat16, jnp.float32
    tall = (5 * width, 4 * width, 3 * width)
    wide = (cuts[0], 2 * cuts[1], 2 * cuts[2])
    near = (NEAR * edges, 2 * NEAR * edges, 2 * NEAR * edges)
    scratch = [(w_zero.shape, bf16), (w_one.shape, bf16), (w_two.shape, bf16)]
    scratch += [((blocks * channels, parts * edges), bf16) for blocks, parts in ((5, 1), (4, 2), (3, 2))]
    scratch += [((tall[i], near[i]), bf16) for i in range(3)]
    scratch += [((2 * tall[i], 2 * edges), bf16) for i in (1, 2)]
    scratch += [((2, 2, wide[i], near[i]), bf16) for i in range(3)]
    for _ in range(2):
        scratch += [
            ((shares - 1, blocks, width, parts * edges), bf16)
            for blocks, parts in ((5, 1), (4, 2), (3, 2))
        ]
    scratch += [((2, wide[i], tall[i]), f32) for i in range(3)]
    scratch += [((2, wide[i], tall[i]), bf16) for i in range(3)]
    scratch += [((2, wide[i], tall[i]), bf16) for i in range(3)]
    scratch += [((wide[i], tall[i]), bf16) for i in range(3)]
    scratch += [((wide[i], tall[i]), bf16) for i in range(3)]
    number = 3 * 2 * (shares - 1) + 15 + 15 + 9
    anywhere = pl.BlockSpec(memory_space=pl.ANY)
    inside = pl.BlockSpec(memory_space=pltpu.VMEM)
    return pl.pallas_call(
        functools.partial(core_kernel, shares),
        in_specs=[anywhere] * 5,
        out_specs=[inside] * 5,
        out_shape=[
            jax.ShapeDtypeStruct((rows, width, edges), f32),
            jax.ShapeDtypeStruct((rows, width, edges), f32),
        ]
        + [jax.ShapeDtypeStruct((wide[i], tall[i]), f32) for i in range(3)],
        scratch_shapes=[pltpu.VMEM(shape, kind) for shape, kind in scratch]
        + [
            pltpu.SemaphoreType.DMA((number,)),
            pltpu.SemaphoreType.DMA((number,)),
            pltpu.SemaphoreType.DMA((32,)),
        ],
        compiler_params=pltpu.CompilerParams(
            collective_id=0, has_side_effects=True, vmem_limit_bytes=66000000
        ),
    )(own, grads, w_zero, w_one, w_two)


def shards(
    embed,
    gain,
    w_zero,
    w_one,
    w_two,
    rot_table,
    face_atoms,
    edge_source,
    edge_target,
    rot_index,
    edge_weight,
    cotangent,
):
    atoms = embed.shape[2]
    local = embed.shape[1]
    halo = face_atoms.shape[0] // 2
    shares = lax.axis_size("chan")
    channels = local * shares
    weights = (w_zero, w_one, w_two)
    values = embed.astype(jnp.float32)
    gains = gain_rows(gain)
    rows, coefficients, rots = rot_table.shape
    which = (jnp.arange(rots, dtype=jnp.int32)[:, None] == rot_index[None, :]).astype(jnp.float32)
    rotations = jnp.dot(
        rot_table.reshape(rows * coefficients, rots),
        which,
        precision=HIGHEST,
        preferred_element_type=jnp.float32,
    )
    weight_row = edge_weight[None, :]
    ones = jnp.ones_like(weight_row)

    squares = lax.psum(jnp.sum(values * values, axis=(0, 1)), "chan")
    inverse = lax.rsqrt(squares / (25 * channels) + EPSILON)
    normed = (values * inverse[None, None, :] * gains[:, :, None]).astype(jnp.bfloat16)
    flat = normed.reshape(25 * local, atoms)
    faces = product(flat, hot_rows(atoms, face_atoms)).astype(jnp.bfloat16)
    table_end = from_beside(faces.reshape(25, local, 2 * halo), halo)

    grads = to_frames([(cotangent, hot_rows(atoms, edge_target))], rotations, weight_row)
    picks = hot_rows(atoms + 2 * halo, edge_source)
    own = to_frames([(normed, picks[:atoms]), (table_end, picks[atoms:])], rotations, ones)
    own, grads = lax.optimization_barrier((own, grads))
    piece = lax.all_gather(own, "chan", axis=1, tiled=True)

    grads_side = swap(grads, 2)
    pair = swap(jnp.stack([grads, grads_side]), 1)
    grads_all = [grads, grads_side, pair[0], pair[1]]

    back = lax.psum_scatter(
        mix_back(weights, grads, shares), "chan", scatter_dimension=0, tiled=False
    )
    frames, widths = column_frames(piece)
    mixed = mix_forward(weights, piece)
    mixed, frames = lax.optimization_barrier((mixed, frames))
    (update,) = to_atoms(
        mixed, rotations, weight_row, [hot_columns(edge_target, atoms)], [jnp.bfloat16]
    )
    leaving = hot_columns(edge_source, atoms + 2 * halo)
    mine, outward = to_atoms(
        back,
        rotations,
        ones,
        [leaving[:, :atoms], leaving[:, atoms:]],
        [jnp.float32, jnp.bfloat16],
    )
    incoming = from_beside(outward, halo)
    settled = product(incoming.reshape(25 * local, 2 * halo), hot_columns(face_atoms, atoms))
    grad_normed = mine + settled.reshape(25, local, atoms)
    scaled = inverse[None, None, :] * gains[:, :, None] * grad_normed
    tally = lax.psum(jnp.sum(values * scaled, axis=(0, 1)), "chan")
    grad_embed = (
        scaled
        - values * (inverse**2 * tally / (25 * channels))[None, None, :]
    ).astype(jnp.bfloat16)
    grad_zero, grad_one, grad_two = weight_grads(frames, widths, grads_all, local)
    return (update, grad_embed, grad_zero, grad_one, grad_two)


def shards_linked(
    embed,
    gain,
    w_zero,
    w_one,
    w_two,
    rot_table,
    face_atoms,
    edge_source,
    edge_target,
    rot_index,
    edge_weight,
    cotangent,
):
    atoms = embed.shape[2]
    local = embed.shape[1]
    halo = face_atoms.shape[0] // 2
    shares = lax.axis_size("chan")
    channels = local * shares
    weights = (w_zero, w_one, w_two)
    values = embed.astype(jnp.float32)
    gains = gain_rows(gain)
    rows, coefficients, rots = rot_table.shape
    which = (jnp.arange(rots, dtype=jnp.int32)[:, None] == rot_index[None, :]).astype(jnp.float32)
    rotations = jnp.dot(
        rot_table.reshape(rows * coefficients, rots),
        which,
        precision=HIGHEST,
        preferred_element_type=jnp.float32,
    )
    weight_row = edge_weight[None, :]
    ones = jnp.ones_like(weight_row)

    squares = lax.psum(jnp.sum(values * values, axis=(0, 1)), "chan")
    inverse = lax.rsqrt(squares / (25 * channels) + EPSILON)
    normed = (values * inverse[None, None, :] * gains[:, :, None]).astype(jnp.bfloat16)
    flat = normed.reshape(25 * local, atoms)
    faces = product(flat, hot_rows(atoms, face_atoms)).astype(jnp.bfloat16)
    table_end = from_beside(faces.reshape(25, local, 2 * halo), halo)

    grads = to_frames([(cotangent, hot_rows(atoms, edge_target))], rotations, weight_row)
    picks = hot_rows(atoms + 2 * halo, edge_source)
    own = to_frames([(normed, picks[:atoms]), (table_end, picks[atoms:])], rotations, ones)
    mixed, back, done_zero, done_one, done_two = run_core(own, grads, weights, shares)
    (update,) = to_atoms(
        mixed, rotations, weight_row, [hot_columns(edge_target, atoms)], [jnp.bfloat16]
    )
    leaving = hot_columns(edge_source, atoms + 2 * halo)
    mine, outward = to_atoms(
        back,
        rotations,
        ones,
        [leaving[:, :atoms], leaving[:, atoms:]],
        [jnp.float32, jnp.bfloat16],
    )
    incoming = from_beside(outward, halo)
    settled = product(incoming.reshape(25 * local, 2 * halo), hot_columns(face_atoms, atoms))
    grad_normed = mine + settled.reshape(25, local, atoms)
    scaled = inverse[None, None, :] * gains[:, :, None] * grad_normed
    tally = lax.psum(jnp.sum(values * scaled, axis=(0, 1)), "chan")
    grad_embed = (
        scaled
        - values * (inverse**2 * tally / (25 * channels))[None, None, :]
    ).astype(jnp.bfloat16)
    grad_zero = jnp.transpose(done_zero).reshape(5, local, -1)
    grad_one, grad_two = [
        jnp.transpose(done.reshape(2, -1, done.shape[1]), (0, 2, 1)).reshape(2, blocks, local, -1)
        for done, blocks in ((done_one, 4), (done_two, 3))
    ]
    return (update, grad_embed, grad_zero, grad_one, grad_two)


def solution(mesh):
    placed = (
        P(None, "chan", "graph"),
        P(None, "chan"),
        P(None, "chan", None),
        P(None, None, "chan", None),
        P(None, None, "chan", None),
        P(),
        P("graph"),
        P("graph"),
        P("graph"),
        P("graph"),
        P("graph"),
        P(None, "chan", "graph"),
    )
    linked = mesh.shape["graph"] == 16 and mesh.shape["chan"] == 2
    return jax.shard_map(
        shards_linked if linked else shards,
        mesh=mesh,
        in_specs=placed,
        out_specs=(
            P(None, "chan", "graph"),
            P(None, "chan", "graph"),
            P(None, "chan", "graph"),
            P(None, None, "chan", "graph"),
            P(None, None, "chan", "graph"),
        ),
        check_vma=False,
    )
```

```python
import functools

import jax
import jax.numpy as jnp
from jax import lax
from jax.experimental import pallas as pl
from jax.experimental.pallas import tpu as pltpu
from jax.sharding import PartitionSpec as P


EPSILON = 1e-06
HIGHEST = lax.Precision.HIGHEST
FRAME = (
    (0, 0),
    (1, 0),
    (2, 0),
    (3, 0),
    (4, 0),
    (1, 1),
    (2, 1),
    (3, 1),
    (4, 1),
    (1, -1),
    (2, -1),
    (3, -1),
    (4, -1),
    (2, 2),
    (3, 2),
    (4, 2),
    (2, -2),
    (3, -2),
    (4, -2),
)


def gain_rows(gain):
    pieces = [
        jnp.broadcast_to(gain[degree : degree + 1], (2 * degree + 1, gain.shape[1]))
        for degree in range(5)
    ]
    return jnp.concatenate(pieces, axis=0)


def product(left, right):
    return jnp.dot(left, right, preferred_element_type=jnp.float32)


def across(left, right):
    return lax.dot_general(
        left, right, (((0,), (0,)), ((), ())), preferred_element_type=jnp.float32
    )


def contract(left, right):
    return lax.dot_general(left, right, (((2,), (1,)), ((), ())), preferred_element_type=jnp.float32)


def frames_kernel(*refs):
    pairs, (rotations, scale, out) = refs[:-3], refs[-3:]
    count, width = pairs[0].shape[0], pairs[0].shape[1]
    total = None
    for values, picks in zip(pairs[0::2], pairs[1::2]):
        part = product(values[...].reshape(count * width, values.shape[2]), picks[...])
        total = part if total is None else total + part
    total = total.reshape(count, width, total.shape[1])
    for row, (degree, _) in enumerate(FRAME):
        first = degree * degree
        entry = row * count + first
        line = rotations[entry : entry + 1, :] * total[first]
        for step in range(1, 2 * degree + 1):
            entry = row * count + first + step
            line = line + rotations[entry : entry + 1, :] * total[first + step]
        out[row] = (line * scale[...]).astype(out.dtype)


def to_frames(pairs, rotations, scale):
    count, local = pairs[0][0].shape[0], pairs[0][0].shape[1]
    edges = scale.shape[1]
    block = min(64, local)
    operands, specs = [], []
    for values, picks in pairs:
        operands += [values, picks]
        specs.append(pl.BlockSpec((count, block, values.shape[2]), lambda i: (0, i, 0)))
        specs.append(pl.BlockSpec(picks.shape, lambda i: (0, 0)))
    for whole in (rotations, scale):
        operands.append(whole)
        specs.append(pl.BlockSpec(whole.shape, lambda i: (0, 0)))
    return pl.pallas_call(
        frames_kernel,
        grid=(local // block,),
        in_specs=specs,
        out_specs=pl.BlockSpec((len(FRAME), block, edges), lambda i: (0, i, 0)),
        out_shape=jax.ShapeDtypeStruct((len(FRAME), local, edges), jnp.bfloat16),
        compiler_params=pltpu.CompilerParams(dimension_semantics=("arbitrary",)),
    )(*operands)


def atoms_kernel(count, values, rotations, scale, *refs):
    picks, outs, held = refs[: len(refs) // 2], refs[len(refs) // 2 : -1], refs[-1]
    width, edges = values.shape[1], values.shape[2]
    for degree in range(5):
        members = [row for row, pair in enumerate(FRAME) if pair[0] == degree]
        lines = [values[row].astype(jnp.float32) * scale[...] for row in members]
        for column in range(degree * degree, (degree + 1) * (degree + 1)):
            total = None
            for row, line in zip(members, lines):
                entry = row * count + column
                term = rotations[entry : entry + 1, :] * line
                total = term if total is None else total + term
            held[column] = total.astype(held.dtype)
    flat = held[...].reshape(count * width, edges)
    for pick, out in zip(picks, outs):
        out[...] = product(flat, pick[...]).reshape(out.shape).astype(out.dtype)


def to_atoms(values, rotations, scale, picks, kinds):
    rows, local, edges = values.shape
    count = rotations.shape[0] // rows
    block = min(64, local)
    whole = lambda i: (0, 0)
    return pl.pallas_call(
        functools.partial(atoms_kernel, count),
        grid=(local // block,),
        in_specs=[
            pl.BlockSpec((rows, block, edges), lambda i: (0, i, 0)),
            pl.BlockSpec(rotations.shape, whole),
            pl.BlockSpec(scale.shape, whole),
        ]
        + [pl.BlockSpec(pick.shape, whole) for pick in picks],
        out_specs=[
            pl.BlockSpec((count, block, pick.shape[1]), lambda i: (0, i, 0)) for pick in picks
        ],
        out_shape=[
            jax.ShapeDtypeStruct((count, local, pick.shape[1]), kind)
            for pick, kind in zip(picks, kinds)
        ],
        scratch_shapes=[pltpu.VMEM((count, block, edges), jnp.bfloat16)],
        compiler_params=pltpu.CompilerParams(dimension_semantics=("arbitrary",)),
    )(values, rotations, scale, *picks)


def swap(block, bit):
    count = lax.axis_size("graph")
    return lax.ppermute(block, "graph", [(i, i ^ bit) for i in range(count)])


def from_beside(faces, width):
    count = lax.axis_size("graph")
    forward = [(i, (i + 1) % count) for i in range(count)]
    backward = [(target, source) for source, target in forward]
    low = lax.ppermute(faces[:, :, width:], "graph", forward)
    high = lax.ppermute(faces[:, :, :width], "graph", backward)
    return jnp.concatenate([low, high], axis=2)


def hot_rows(size, codes):
    return (jnp.arange(size, dtype=jnp.int32)[:, None] == codes[None, :]).astype(jnp.bfloat16)


def hot_columns(codes, size):
    return (codes[:, None] == jnp.arange(size, dtype=jnp.int32)[None, :]).astype(jnp.bfloat16)


def beside(plus, minus, axis=-1):
    return jnp.concatenate([plus, minus], axis=axis)


def mix_forward(weights, frame):
    w_zero, w_one, w_two = weights
    edges = frame.shape[2]
    local = w_zero.shape[1]
    mixed = [
        product(w_zero.reshape(-1, w_zero.shape[2]), frame[:5].reshape(-1, edges)).reshape(
            5, local, edges
        )
    ]
    for weight, first, blocks in ((w_one, 5, 4), (w_two, 13, 3)):
        plus = frame[first : first + blocks].reshape(-1, edges)
        minus = frame[first + blocks : first + 2 * blocks].reshape(-1, edges)
        both = product(weight.reshape(-1, weight.shape[-1]), beside(plus, minus))
        both = both.reshape(2, blocks, local, 2 * edges)
        mixed.append(both[0, :, :, :edges] - both[1, :, :, edges:])
        mixed.append(both[0, :, :, edges:] + both[1, :, :, :edges])
    return jnp.concatenate(mixed, axis=0)


def mix_back(weights, grads, shares):
    w_zero, w_one, w_two = weights
    edges = grads.shape[2]

    def shared(block, blocks):
        shaped = block.reshape(blocks, shares, -1, edges).astype(jnp.bfloat16)
        return jnp.transpose(shaped, (1, 0, 2, 3))

    back = [
        shared(across(w_zero.reshape(-1, w_zero.shape[2]), grads[:5].reshape(-1, edges)), 5)
    ]
    for weight, first, blocks in ((w_one, 5, 4), (w_two, 13, 3)):
        plus = grads[first : first + blocks].reshape(-1, edges)
        minus = grads[first + blocks : first + 2 * blocks].reshape(-1, edges)
        sides = jnp.concatenate([beside(plus, minus), beside(minus, -plus)], axis=0)
        both = across(weight.reshape(-1, weight.shape[-1]), sides)
        back.append(shared(both[:, :edges], blocks))
        back.append(shared(both[:, edges:], blocks))
    return jnp.concatenate(back, axis=1)


def column_frames(frame):
    count = lax.axis_size("graph")
    near = 4
    far = count // near
    edges = frame.shape[2]
    cuts = ((0, 5), (5, 4), (9, 4), (13, 3), (16, 3))
    parts = [
        frame[first : first + blocks].reshape(far, near, -1, edges) for first, blocks in cuts
    ]
    widths = [part.shape[2] for part in parts]
    packed = jnp.concatenate(parts, axis=2)
    mine = lax.axis_index("graph") % near
    frames = []
    for bit in (0, 2, 1, 3):
        target = mine ^ bit
        chunk = lax.dynamic_index_in_dim(packed, target, axis=1, keepdims=False)
        frames.append(swap(chunk, bit) if bit else chunk)
    return frames, widths


def weight_grads(frames, widths, grads_all, local):
    count = lax.axis_size("graph")
    near = 4
    far = count // near
    edges = frames[0].shape[2]
    starts = [sum(widths[:i]) for i in range(5)]
    groups = [[z * near + q for z in range(far)] for q in range(near)]

    def settle(partial):
        return lax.psum_scatter(
            partial.astype(jnp.bfloat16),
            "graph",
            scatter_dimension=0,
            axis_index_groups=groups,
            tiled=False,
        ).astype(jnp.float32)

    def settle_direct(partial):
        partial = partial.astype(jnp.bfloat16)
        place = lax.axis_index("graph") // near
        total = lax.dynamic_index_in_dim(partial, place, axis=0, keepdims=False)
        total = total.astype(jnp.float32)
        for step in range(1, far):
            chunk = lax.dynamic_index_in_dim(partial, (place + step) % far, axis=0, keepdims=False)
            shift = [(i, (i + step * near) % count) for i in range(count)]
            total = total + lax.ppermute(chunk, "graph", shift).astype(jnp.float32)
        return total

    def columns(index):
        return [chunk[:, starts[index] : starts[index] + widths[index]] for chunk in frames]

    left = jnp.concatenate(columns(0), axis=2)
    right = jnp.concatenate([g[:5].reshape(-1, edges) for g in grads_all], axis=1)
    done = settle_direct(contract(left, right))
    results = [jnp.transpose(done).reshape(5, local, widths[0])]
    for index, first, blocks in ((1, 5, 4), (3, 13, 3)):
        plus, minus = columns(index), columns(index + 1)
        real_part = jnp.concatenate([x for pair in zip(plus, minus) for x in pair], axis=2)
        imag_part = jnp.concatenate([x for pair in zip(minus, plus) for x in (-pair[0], pair[1])], axis=2)
        left = jnp.concatenate([real_part, imag_part], axis=1)
        right = jnp.concatenate(
            [
                g[start : start + blocks].reshape(-1, edges)
                for g in grads_all
                for start in (first, first + blocks)
            ],
            axis=1,
        )
        done = settle(contract(left, right))
        done = done.reshape(2, widths[index], blocks * local)
        results.append(jnp.transpose(done, (0, 2, 1)).reshape(2, blocks, local, widths[index]))
    return results


NEAR = 4
PARTS = ((5, 1), (4, 2), (3, 2))
FIRSTS = (0, 5, 13)


def lanes(start, size):
    return pl.ds(pl.multiple_of(start, 128), size)


def turned(left, right):
    return lax.dot_general(
        left, right, (((1,), (1,)), ((), ())), preferred_element_type=jnp.float32
    )


def hot(size, codes, first=0):
    places = lax.broadcasted_iota(jnp.int32, (size, codes.shape[1]), 0) + first
    return (places == codes).astype(jnp.bfloat16)


class Links:
    def __init__(self, sends, recvs):
        self.sends, self.recvs, self.count, self.started = sends, recvs, 0, []

    def start(self, source, target, device):
        index = self.count
        self.count += 1
        copy = pltpu.make_async_remote_copy(
            src_ref=source,
            dst_ref=target,
            send_sem=self.sends.at[index],
            recv_sem=self.recvs.at[index],
            device_id=device,
            device_id_type=pl.DeviceIdType.MESH,
        )
        copy.start()
        self.started.append(copy)
        return copy

    def settle(self, copy):
        copy.wait_send()
        self.started = [one for one in self.started if one is not copy]

    def finish(self):
        for copy in self.started:
            copy.wait_send()


def layer_kernel(shares, count, *refs):
    (embed, cotangent, gain, w_zero, w_one, w_two, table) = refs[:7]
    (face_row, source_row, target_row, which_row, weight_row) = refs[7:12]
    (update, grad_embed, out_zero, out_one, out_two) = refs[12:17]
    weights = refs[17:20]
    frames = refs[20:23]
    grads = refs[23:26]
    doubled = (None,) + tuple(refs[26:28])
    nears = refs[28:31]
    back_out, back_in = refs[31:34], refs[34:37]
    kept, leaving, arriving, final = refs[37:40], refs[40:43], refs[43:46], refs[46:49]
    (work, back, arrow, values, normed, rot, gains) = refs[49:56]
    (face_out, face_in, ends_out, ends_in) = refs[56:60]
    (square_out, square_in, tally_out, tally_in) = refs[60:64]
    sends, recvs, local_sems = refs[64:67]
    outs = (out_zero, out_one, out_two)
    f32, bf16 = jnp.float32, jnp.bfloat16
    terms, width, atoms = values.shape
    edges = source_row.shape[1]
    halo = face_row.shape[1] // 2
    channels = width * shares
    me = lax.axis_index("graph")
    share = lax.axis_index("chan")
    low, side, pair, far = me % 2, (me // 2) % 2, (me // 4) % 2, (me // 8) % 2
    slot = pair * 2 + low

    def flip(bit):
        digits = {1: low, 2: side, 4: pair, 8: far}
        place = me
        for one in (1, 2, 4, 8):
            if bit & one:
                place = place + one - 2 * one * digits[one]
        return (place, share)

    after, before = (lax.rem(me + 1, count), share), (lax.rem(me + count - 1, count), share)
    peers = [lax.rem(share + step, shares) for step in range(1, shares)]
    copies = []

    def bring(origin, target):
        copy = pltpu.make_async_copy(origin, target, local_sems.at[len(copies)])
        copy.start()
        copies.append(copy)
        return copy

    load_embed = bring(embed, values)
    load_cotangent = bring(cotangent, arrow)
    order = (1, 0, 2)
    loads = {at: bring((w_zero, w_one, w_two)[at], weights[at]) for at in order}

    barrier = pltpu.get_barrier_semaphore()
    others = [flip(bit) for bit in (1, 2, 4, 5, 8)] + [after, before]
    others += [(me, peer) for peer in peers]
    for other in others:
        pl.semaphore_signal(
            barrier, inc=1, device_id=other, device_id_type=pl.DeviceIdType.MESH
        )
    links = Links(sends, recvs)

    which = hot(table.shape[2], which_row[...]).astype(f32)

    def turn(row, unused):
        rot[row] = jnp.dot(
            table[row], which, precision=HIGHEST, preferred_element_type=f32
        )
        return unused

    lax.fori_loop(0, len(FRAME), turn, 0)
    degrees = lax.broadcasted_iota(jnp.int32, (5, atoms), 0)
    for degree in range(5):
        gains[degree] = lax.dot_general(
            gain[...],
            (degrees == degree).astype(f32),
            (((0,), (0,)), ((), ())),
            precision=HIGHEST,
            preferred_element_type=f32,
        )
    to_target = hot(atoms, target_row[...])
    to_source = hot(atoms, source_row[...])
    to_halo = hot(2 * halo, source_row[...], atoms)
    faces = hot(atoms, face_row[...])
    square = lax.broadcasted_iota(jnp.int32, (2 * halo, 2 * halo), 0)
    unit = (square == lax.broadcasted_iota(jnp.int32, square.shape, 1)).astype(bf16)
    to_face = turned(unit, faces).astype(bf16)
    scale = weight_row[...]

    load_embed.wait()

    def squared(term, total):
        value = values[term].astype(f32)
        return total + value * value

    total = lax.fori_loop(0, terms, squared, jnp.zeros((width, atoms), f32))
    own_squares = jnp.sum(total, axis=0, keepdims=True)
    square_out[...] = jnp.broadcast_to(own_squares, square_out.shape)
    pl.semaphore_wait(barrier, len(others))
    summed = [
        links.start(square_out, square_in.at[index], (me, peer))
        for index, peer in enumerate(peers)
    ]

    def spread(values_ref, picks):
        def one(term, unused):
            work[term] = product(values_ref[term], picks)
            return unused

        lax.fori_loop(0, terms, one, 0)

    tall = min(32, width)

    def rotate(at, put):
        first, (blocks, parts) = FIRSTS[at], PARTS[at]

        def one(step, unused):
            rows = pl.ds(pl.multiple_of(step * tall, tall), tall)
            for degree in range(5):
                base = degree * degree
                members = [
                    row
                    for row in range(first, first + blocks * parts)
                    if FRAME[row][0] == degree
                ]
                if not members:
                    continue
                lines = [work[base + index, rows, :] for index in range(2 * degree + 1)]
                for row in members:
                    line = None
                    for index, entry in enumerate(lines):
                        term = rot[row, base + index : base + index + 1, :] * entry
                        line = term if line is None else line + term
                    part, block = divmod(row - first, blocks)
                    put(block, part, step * tall, line)
            return unused

        lax.fori_loop(0, width // tall, one, 0)

    load_cotangent.wait()
    spread(arrow, to_target)
    near = [None] * 3
    for at in order:
        parts = PARTS[at][1]

        def put_grad(block, part, start, line):
            rows = pl.ds(pl.multiple_of(block * width + start, tall), tall)
            grads[at][rows, lanes((part * NEAR + slot) * edges, edges)] = (line * scale).astype(bf16)

        rotate(at, put_grad)
        spots = [
            grads[at].at[:, lanes((part * NEAR + slot) * edges, edges)] for part in range(parts)
        ]
        near[at] = [
            [links.start(spot, spot, flip(4)) for spot in spots],
            [links.start(spot, spot, flip(1)) for spot in spots],
        ]

    whole = own_squares
    for index, copy in enumerate(summed):
        copy.wait_recv()
        whole = whole + square_in[index, :1, :]
    inverse = lax.rsqrt(whole / (terms * channels) + EPSILON)
    for degree in range(5):

        def normal(term, unused):
            normed[term] = (values[term].astype(f32) * inverse * gains[degree]).astype(bf16)
            return unused

        lax.fori_loop(degree * degree, (degree + 1) * (degree + 1), normal, 0)

    def edge_of(term, unused):
        value = turned(to_face, normed[term]).astype(bf16)
        face_out[:, :, lanes(term * width, width)] = value.reshape(2, halo, width)
        return unused

    lax.fori_loop(0, terms, edge_of, 0)
    halos = [
        links.start(face_out.at[1], face_in.at[0], after),
        links.start(face_out.at[0], face_in.at[1], before),
    ]
    spread(normed, to_source)

    for at in (1, 2):
        blocks = PARTS[at][0]
        height = blocks * width
        g = grads[at]
        plus = g[:, lanes(slot * edges, edges)]
        minus = g[:, lanes((NEAR + slot) * edges, edges)]
        doubled[at][:height, :edges] = plus
        doubled[at][:height, edges:] = minus
        doubled[at][height:, :edges] = minus
        doubled[at][height:, edges:] = -plus

    def backed(at, row, share_at):
        if at == 0:
            right = grads[0][:, lanes(slot * edges, edges)]
        else:
            right = doubled[at][...]
        left = weights[at][..., lanes(row * channels + share_at * width, width)]
        return across(left.reshape(-1, width), right)

    def back_leave(at):
        loads[at].wait()
        for index, peer in enumerate(peers):

            def one(row, unused):
                back_out[at][index, row] = backed(at, row, peer).astype(bf16)
                return unused

            lax.fori_loop(0, PARTS[at][0], one, 0)

    def back_send(at):
        return [
            links.start(back_out[at].at[index], back_in[at].at[index], (me, peer))
            for index, peer in enumerate(peers)
        ]

    def back_keep(at):
        first, (blocks, parts) = FIRSTS[at], PARTS[at]

        def one(row, unused):
            value = backed(at, row, share)
            for part in range(parts):
                back[first + part * blocks + row] = value[:, part * edges : (part + 1) * edges]
            return unused

        lax.fori_loop(0, blocks, one, 0)

    back_leave(1)
    for copy in halos:
        copy.wait_recv()

    def joined(term, unused):
        value = face_in[:, :, lanes(term * width, width)].reshape(2 * halo, width)
        work[term] += across(value, to_halo)
        return unused

    lax.fori_loop(0, terms, joined, 0)
    gathered = [None] * 3
    scattered = [None] * 3
    for at in order:
        blocks, parts = PARTS[at]

        def put_frame(block, part, start, line):
            rows = pl.ds(pl.multiple_of(block * channels + share * width + start, tall), tall)
            frames[at][rows, part * edges : (part + 1) * edges] = line.astype(bf16)

        rotate(at, put_frame)
        ours = frames[at].reshape(blocks, shares, width, parts * edges).at[:, share]
        gathered[at] = [links.start(ours, ours, (me, peer)) for peer in peers]

    def relay(at):
        relays = []
        for part, copy in enumerate(near[at][0]):
            copy.wait_recv()
            spot = grads[at].at[:, lanes((part * NEAR + (1 - pair) * 2 + low) * edges, edges)]
            relays.append(links.start(spot, spot, flip(1)))
        near[at].append(relays)

    scattered[1] = back_send(1)
    relay(1)
    back_leave(0)
    scattered[0] = back_send(0)
    relay(0)
    arrivals = [None] * 3

    def scatter_frames(at):
        for copy in gathered[at]:
            copy.wait_recv()
        parts = PARTS[at][1]
        short = nears[at].shape[2] // parts
        cut = frames[at].reshape(2, 2, 2, 2, short, parts * edges)
        waits = []
        for part in range(parts):
            here = nears[at].at[:, :, pl.ds(0, short), lanes((part * NEAR + slot) * edges, edges)]
            spread_lanes = pl.ds(part * edges, edges)
            for bit in (4, 5, 1):
                its_pair = 1 - pair if bit & 4 else pair
                its_low = 1 - low if bit & 1 else low
                piece = cut.at[:, its_pair, :, its_low, :, spread_lanes]
                waits.append(links.start(piece, here, flip(bit)).wait_recv)
            waits.append(bring(cut.at[:, pair, :, low, :, spread_lanes], here).wait)
        arrivals[at] = waits

    def mix(at):
        first, (blocks, parts) = FIRSTS[at], PARTS[at]

        def one(row, unused):
            if parts == 1:
                work[first + row] = product(weights[at][row], frames[at][...])
            else:
                real = product(weights[at][0, row], frames[at][...])
                imag = product(weights[at][1, row], frames[at][...])
                work[first + row] = real[:, :edges] - imag[:, edges:]
                work[first + blocks + row] = real[:, edges:] + imag[:, :edges]
            return unused

        lax.fori_loop(0, blocks, one, 0)

    def grown(at, step, one_side):
        tile = min(256, grads[at].shape[0])
        left = nears[at][:, one_side].reshape(-1, nears[at].shape[3])
        right = grads[at][pl.ds(pl.multiple_of(step * tile, tile), tile), :]
        return turned(left, right).reshape(2, -1, tile), lanes(step * tile, tile)

    aside = [None] * 3
    away = [None] * 3

    def grow_leave(at):
        for arrive in arrivals[at]:
            arrive()
        for group in near[at][1:]:
            for copy in group:
                copy.wait_recv()
        parts = PARTS[at][1]
        f, span = nears[at], NEAR * edges
        short = f.shape[2] // parts
        if parts == 2:
            for one_far in range(2):
                for one_side in range(2):
                    f[one_far, one_side, short:, :span] = -f[one_far, one_side, :short, span:]
                    f[one_far, one_side, short:, span:] = f[one_far, one_side, :short, :span]

        def leave(step, unused):
            value, columns = grown(at, step, 1 - side)
            leaving[at][:, :, columns] = value.astype(bf16)
            return unused

        lax.fori_loop(0, grads[at].shape[0] // min(256, grads[at].shape[0]), leave, 0)
        aside[at] = [
            links.start(leaving[at].at[1 - far], arriving[at].at[1 - far], flip(2))
        ]

    def grow_later(at):
        aside[at].append(links.start(leaving[at].at[far], arriving[at].at[far], flip(2)))

    def grow_keep(at):
        def stay(step, unused):
            value, columns = grown(at, step, side)
            kept[at][:, :, columns] = value
            return unused

        lax.fori_loop(0, grads[at].shape[0] // min(256, grads[at].shape[0]), stay, 0)

    def pass_on(at):
        aside[at][0].wait_recv()
        links.settle(aside[at][0])
        total = kept[at][1 - far] + arriving[at][1 - far].astype(f32)
        leaving[at][1 - far] = total.astype(bf16)
        away[at] = links.start(leaving[at].at[1 - far], final[at], flip(8))

    scatter_frames(1)
    back_leave(2)
    scattered[2] = back_send(2)
    relay(2)
    scatter_frames(0)
    grow_leave(1)
    scatter_frames(2)
    grow_keep(1)
    back_keep(1)
    mix(1)
    grow_leave(0)
    pass_on(1)
    grow_keep(0)
    mix(0)
    grow_leave(2)
    for at in order:
        grow_later(at)
    grow_keep(2)
    pass_on(0)
    mix(2)
    back_keep(0)
    back_keep(2)

    def unturn(origin, factor, put):
        def one(step, unused):
            rows = pl.ds(pl.multiple_of(step * tall, tall), tall)
            for degree in range(5):
                members = [row for row, entry in enumerate(FRAME) if entry[0] == degree]
                lines = [origin[row, rows, :] for row in members]
                if factor is not None:
                    lines = [line * factor for line in lines]
                for column in range(degree * degree, (degree + 1) * (degree + 1)):
                    value = None
                    for row, line in zip(members, lines):
                        term = rot[row, column : column + 1, :] * line
                        value = term if value is None else value + term
                    put(column, rows, value)
            return unused

        lax.fori_loop(0, width // tall, one, 0)

    def put_normed(column, rows, value):
        normed[column, rows, :] = value.astype(bf16)

    unturn(work, scale, put_normed)

    def updated(term, unused):
        arrow[term] = turned(normed[term], to_target).astype(bf16)
        return unused

    lax.fori_loop(0, terms, updated, 0)
    stored = [bring(arrow, update)]
    pass_on(2)

    for at in order:
        first, (blocks, parts) = FIRSTS[at], PARTS[at]
        for index, copy in enumerate(scattered[at]):
            copy.wait_recv()

            def add(row, unused):
                arrived = back_in[at][index, row].astype(f32)
                for part in range(parts):
                    back[first + part * blocks + row] += arrived[
                        :, part * edges : (part + 1) * edges
                    ]
                return unused

            lax.fori_loop(0, blocks, add, 0)
    unturn(back, None, put_normed)

    def end_of(term, unused):
        value = turned(to_halo, normed[term]).astype(bf16)
        ends_out[:, :, lanes(term * width, width)] = value.reshape(2, halo, width)
        return unused

    lax.fori_loop(0, terms, end_of, 0)
    ends = [
        links.start(ends_out.at[1], ends_in.at[0], after),
        links.start(ends_out.at[0], ends_in.at[1], before),
    ]

    def owned(term, unused):
        work[term] = turned(normed[term], to_source)
        return unused

    lax.fori_loop(0, terms, owned, 0)
    for copy in ends:
        copy.wait_recv()
    total = jnp.zeros((width, atoms), f32)
    for degree in range(5):

        def scaled(term, total):
            value = ends_in[:, :, lanes(term * width, width)].reshape(2 * halo, width)
            result = (work[term] + across(value, to_face)) * inverse * gains[degree]
            work[term] = result
            return total + result * values[term].astype(f32)

        total = lax.fori_loop(degree * degree, (degree + 1) * (degree + 1), scaled, total)
    whole = jnp.sum(total, axis=0, keepdims=True)
    tally_out[...] = jnp.broadcast_to(whole, tally_out.shape)
    tallies = [
        links.start(tally_out, tally_in.at[index], (me, peer))
        for index, peer in enumerate(peers)
    ]
    for index, copy in enumerate(tallies):
        copy.wait_recv()
        whole = whole + tally_in[index, :1, :]
    factor = inverse * inverse * whole / (terms * channels)

    def finished(term, unused):
        normed[term] = (work[term] - values[term].astype(f32) * factor).astype(bf16)
        return unused

    lax.fori_loop(0, terms, finished, 0)
    stored.append(bring(normed, grad_embed))
    for at in order:
        aside[at][1].wait_recv()
        total = kept[at][far] + arriving[at][far].astype(f32)
        away[at].wait_recv()
        kept[at][far] = total + final[at][...].astype(f32)
        stored.append(bring(kept[at].at[far], outs[at]))
    links.finish()
    for copy in stored:
        copy.wait()


def run_layer(arrays, sizes):
    embed, w_zero, w_one, w_two = arrays[0], arrays[3], arrays[4], arrays[5]
    shares, count = sizes
    terms, width, atoms = embed.shape
    edges, halo = arrays[8].shape[1], arrays[7].shape[1] // 2
    channels = width * shares
    cuts = (w_zero.shape[2] // count, w_one.shape[3] // count, w_two.shape[3] // count)
    bf16, f32 = jnp.bfloat16, jnp.float32
    three = range(3)
    tall = [blocks * width for blocks, parts in PARTS]
    wide = [parts * cut for (blocks, parts), cut in zip(PARTS, cuts)]
    near = [NEAR * parts * edges for blocks, parts in PARTS]
    scratch = [(w.shape, bf16) for w in (w_zero, w_one, w_two)]
    scratch += [((blocks * channels, parts * edges), bf16) for blocks, parts in PARTS]
    scratch += [((tall[i], near[i]), bf16) for i in three]
    scratch += [((2 * tall[i], 2 * edges), bf16) for i in (1, 2)]
    scratch += [((2, 2, wide[i], near[i]), bf16) for i in three]
    scratch += 2 * [
        ((shares - 1, blocks, width, parts * edges), bf16) for blocks, parts in PARTS
    ]
    scratch += [((2, wide[i], tall[i]), f32) for i in three]
    scratch += 2 * [((2, wide[i], tall[i]), bf16) for i in three]
    scratch += [((wide[i], tall[i]), bf16) for i in three]
    scratch += [
        ((terms, width, edges), f32),
        ((len(FRAME), width, edges), f32),
        ((terms, width, atoms), bf16),
        ((terms, width, atoms), bf16),
        ((terms, width, atoms), bf16),
        ((len(FRAME), terms, edges), f32),
        ((5, width, atoms), f32),
    ]
    scratch += 4 * [((2, halo, terms * width), bf16)]
    scratch += 2 * [((8, atoms), f32), ((shares - 1, 8, atoms), f32)]
    number = 8 * (shares - 1) + 15 + 15 + 9 + 4
    anywhere = pl.BlockSpec(memory_space=pl.ANY)
    inside = pl.BlockSpec(memory_space=pltpu.VMEM)
    return pl.pallas_call(
        functools.partial(layer_kernel, shares, count),
        in_specs=[anywhere] * 2 + [inside] + [anywhere] * 3 + [inside] * 6,
        out_specs=[anywhere] * 5,
        out_shape=[jax.ShapeDtypeStruct(embed.shape, bf16)] * 2
        + [jax.ShapeDtypeStruct((wide[i], tall[i]), f32) for i in three],
        scratch_shapes=[pltpu.VMEM(shape, kind) for shape, kind in scratch]
        + [
            pltpu.SemaphoreType.DMA((number,)),
            pltpu.SemaphoreType.DMA((number,)),
            pltpu.SemaphoreType.DMA((24,)),
        ],
        compiler_params=pltpu.CompilerParams(
            collective_id=0, has_side_effects=True, vmem_limit_bytes=67043328
        ),
    )(*arrays)


def shards(
    embed,
    gain,
    w_zero,
    w_one,
    w_two,
    rot_table,
    face_atoms,
    edge_source,
    edge_target,
    rot_index,
    edge_weight,
    cotangent,
):
    atoms = embed.shape[2]
    local = embed.shape[1]
    halo = face_atoms.shape[0] // 2
    shares = lax.axis_size("chan")
    channels = local * shares
    weights = (w_zero, w_one, w_two)
    values = embed.astype(jnp.float32)
    gains = gain_rows(gain)
    rows, coefficients, rots = rot_table.shape
    which = (jnp.arange(rots, dtype=jnp.int32)[:, None] == rot_index[None, :]).astype(jnp.float32)
    rotations = jnp.dot(
        rot_table.reshape(rows * coefficients, rots),
        which,
        precision=HIGHEST,
        preferred_element_type=jnp.float32,
    )
    weight_row = edge_weight[None, :]
    ones = jnp.ones_like(weight_row)

    squares = lax.psum(jnp.sum(values * values, axis=(0, 1)), "chan")
    inverse = lax.rsqrt(squares / (25 * channels) + EPSILON)
    normed = (values * inverse[None, None, :] * gains[:, :, None]).astype(jnp.bfloat16)
    flat = normed.reshape(25 * local, atoms)
    faces = product(flat, hot_rows(atoms, face_atoms)).astype(jnp.bfloat16)
    table_end = from_beside(faces.reshape(25, local, 2 * halo), halo)

    grads = to_frames([(cotangent, hot_rows(atoms, edge_target))], rotations, weight_row)
    picks = hot_rows(atoms + 2 * halo, edge_source)
    own = to_frames([(normed, picks[:atoms]), (table_end, picks[atoms:])], rotations, ones)
    own, grads = lax.optimization_barrier((own, grads))
    piece = lax.all_gather(own, "chan", axis=1, tiled=True)

    grads_side = swap(grads, 2)
    pair = swap(jnp.stack([grads, grads_side]), 1)
    grads_all = [grads, grads_side, pair[0], pair[1]]

    back = lax.psum_scatter(
        mix_back(weights, grads, shares), "chan", scatter_dimension=0, tiled=False
    )
    frames, widths = column_frames(piece)
    mixed = mix_forward(weights, piece)
    mixed, frames = lax.optimization_barrier((mixed, frames))
    (update,) = to_atoms(
        mixed, rotations, weight_row, [hot_columns(edge_target, atoms)], [jnp.bfloat16]
    )
    leaving = hot_columns(edge_source, atoms + 2 * halo)
    mine, outward = to_atoms(
        back,
        rotations,
        ones,
        [leaving[:, :atoms], leaving[:, atoms:]],
        [jnp.float32, jnp.bfloat16],
    )
    incoming = from_beside(outward, halo)
    settled = product(incoming.reshape(25 * local, 2 * halo), hot_columns(face_atoms, atoms))
    grad_normed = mine + settled.reshape(25, local, atoms)
    scaled = inverse[None, None, :] * gains[:, :, None] * grad_normed
    tally = lax.psum(jnp.sum(values * scaled, axis=(0, 1)), "chan")
    grad_embed = (
        scaled
        - values * (inverse**2 * tally / (25 * channels))[None, None, :]
    ).astype(jnp.bfloat16)
    grad_zero, grad_one, grad_two = weight_grads(frames, widths, grads_all, local)
    return (update, grad_embed, grad_zero, grad_one, grad_two)


def shards_linked(
    embed,
    gain,
    w_zero,
    w_one,
    w_two,
    rot_table,
    face_atoms,
    edge_source,
    edge_target,
    rot_index,
    edge_weight,
    cotangent,
):
    local = embed.shape[1]
    arrays = (
        embed,
        cotangent,
        gain,
        w_zero,
        w_one,
        w_two,
        rot_table,
        face_atoms[None, :],
        edge_source[None, :],
        edge_target[None, :],
        rot_index[None, :],
        edge_weight[None, :],
    )
    sizes = (lax.axis_size("chan"), lax.axis_size("graph"))
    update, grad_embed, done_zero, done_one, done_two = run_layer(arrays, sizes)
    grad_zero = jnp.transpose(done_zero).reshape(5, local, -1)
    grad_one, grad_two = [
        jnp.transpose(done.reshape(2, -1, done.shape[1]), (0, 2, 1)).reshape(2, blocks, local, -1)
        for done, blocks in ((done_one, 4), (done_two, 3))
    ]
    return (update, grad_embed, grad_zero, grad_one, grad_two)


def solution(mesh):
    placed = (
        P(None, "chan", "graph"),
        P(None, "chan"),
        P(None, "chan", None),
        P(None, None, "chan", None),
        P(None, None, "chan", None),
        P(),
        P("graph"),
        P("graph"),
        P("graph"),
        P("graph"),
        P("graph"),
        P(None, "chan", "graph"),
    )
    linked = mesh.shape["graph"] == 16 and mesh.shape["chan"] == 2
    return jax.shard_map(
        shards_linked if linked else shards,
        mesh=mesh,
        in_specs=placed,
        out_specs=(
            P(None, "chan", "graph"),
            P(None, "chan", "graph"),
            P(None, "chan", "graph"),
            P(None, None, "chan", "graph"),
            P(None, None, "chan", "graph"),
        ),
        check_vma=False,
    )
```

```python
import functools

import jax
import jax.numpy as jnp
from jax import lax
from jax.experimental import pallas as pl
from jax.experimental.pallas import tpu as pltpu
from jax.sharding import PartitionSpec as P


EPSILON = 1e-06
HIGHEST = lax.Precision.HIGHEST
FRAME = (
    (0, 0),
    (1, 0),
    (2, 0),
    (3, 0),
    (4, 0),
    (1, 1),
    (2, 1),
    (3, 1),
    (4, 1),
    (1, -1),
    (2, -1),
    (3, -1),
    (4, -1),
    (2, 2),
    (3, 2),
    (4, 2),
    (2, -2),
    (3, -2),
    (4, -2),
)


def gain_rows(gain):
    pieces = [
        jnp.broadcast_to(gain[degree : degree + 1], (2 * degree + 1, gain.shape[1]))
        for degree in range(5)
    ]
    return jnp.concatenate(pieces, axis=0)


def product(left, right):
    return jnp.dot(left, right, preferred_element_type=jnp.float32)


def across(left, right):
    return lax.dot_general(
        left, right, (((0,), (0,)), ((), ())), preferred_element_type=jnp.float32
    )


def contract(left, right):
    return lax.dot_general(left, right, (((2,), (1,)), ((), ())), preferred_element_type=jnp.float32)


def frames_kernel(*refs):
    pairs, (rotations, scale, out) = refs[:-3], refs[-3:]
    count, width = pairs[0].shape[0], pairs[0].shape[1]
    total = None
    for values, picks in zip(pairs[0::2], pairs[1::2]):
        part = product(values[...].reshape(count * width, values.shape[2]), picks[...])
        total = part if total is None else total + part
    total = total.reshape(count, width, total.shape[1])
    for row, (degree, _) in enumerate(FRAME):
        first = degree * degree
        entry = row * count + first
        line = rotations[entry : entry + 1, :] * total[first]
        for step in range(1, 2 * degree + 1):
            entry = row * count + first + step
            line = line + rotations[entry : entry + 1, :] * total[first + step]
        out[row] = (line * scale[...]).astype(out.dtype)


def to_frames(pairs, rotations, scale):
    count, local = pairs[0][0].shape[0], pairs[0][0].shape[1]
    edges = scale.shape[1]
    block = min(64, local)
    operands, specs = [], []
    for values, picks in pairs:
        operands += [values, picks]
        specs.append(pl.BlockSpec((count, block, values.shape[2]), lambda i: (0, i, 0)))
        specs.append(pl.BlockSpec(picks.shape, lambda i: (0, 0)))
    for whole in (rotations, scale):
        operands.append(whole)
        specs.append(pl.BlockSpec(whole.shape, lambda i: (0, 0)))
    return pl.pallas_call(
        frames_kernel,
        grid=(local // block,),
        in_specs=specs,
        out_specs=pl.BlockSpec((len(FRAME), block, edges), lambda i: (0, i, 0)),
        out_shape=jax.ShapeDtypeStruct((len(FRAME), local, edges), jnp.bfloat16),
        compiler_params=pltpu.CompilerParams(dimension_semantics=("arbitrary",)),
    )(*operands)


def atoms_kernel(count, values, rotations, scale, *refs):
    picks, outs, held = refs[: len(refs) // 2], refs[len(refs) // 2 : -1], refs[-1]
    width, edges = values.shape[1], values.shape[2]
    for degree in range(5):
        members = [row for row, pair in enumerate(FRAME) if pair[0] == degree]
        lines = [values[row].astype(jnp.float32) * scale[...] for row in members]
        for column in range(degree * degree, (degree + 1) * (degree + 1)):
            total = None
            for row, line in zip(members, lines):
                entry = row * count + column
                term = rotations[entry : entry + 1, :] * line
                total = term if total is None else total + term
            held[column] = total.astype(held.dtype)
    flat = held[...].reshape(count * width, edges)
    for pick, out in zip(picks, outs):
        out[...] = product(flat, pick[...]).reshape(out.shape).astype(out.dtype)


def to_atoms(values, rotations, scale, picks, kinds):
    rows, local, edges = values.shape
    count = rotations.shape[0] // rows
    block = min(64, local)
    whole = lambda i: (0, 0)
    return pl.pallas_call(
        functools.partial(atoms_kernel, count),
        grid=(local // block,),
        in_specs=[
            pl.BlockSpec((rows, block, edges), lambda i: (0, i, 0)),
            pl.BlockSpec(rotations.shape, whole),
            pl.BlockSpec(scale.shape, whole),
        ]
        + [pl.BlockSpec(pick.shape, whole) for pick in picks],
        out_specs=[
            pl.BlockSpec((count, block, pick.shape[1]), lambda i: (0, i, 0)) for pick in picks
        ],
        out_shape=[
            jax.ShapeDtypeStruct((count, local, pick.shape[1]), kind)
            for pick, kind in zip(picks, kinds)
        ],
        scratch_shapes=[pltpu.VMEM((count, block, edges), jnp.bfloat16)],
        compiler_params=pltpu.CompilerParams(dimension_semantics=("arbitrary",)),
    )(values, rotations, scale, *picks)


def swap(block, bit):
    count = lax.axis_size("graph")
    return lax.ppermute(block, "graph", [(i, i ^ bit) for i in range(count)])


def from_beside(faces, width):
    count = lax.axis_size("graph")
    forward = [(i, (i + 1) % count) for i in range(count)]
    backward = [(target, source) for source, target in forward]
    low = lax.ppermute(faces[:, :, width:], "graph", forward)
    high = lax.ppermute(faces[:, :, :width], "graph", backward)
    return jnp.concatenate([low, high], axis=2)


def hot_rows(size, codes):
    return (jnp.arange(size, dtype=jnp.int32)[:, None] == codes[None, :]).astype(jnp.bfloat16)


def hot_columns(codes, size):
    return (codes[:, None] == jnp.arange(size, dtype=jnp.int32)[None, :]).astype(jnp.bfloat16)


def beside(plus, minus, axis=-1):
    return jnp.concatenate([plus, minus], axis=axis)


def mix_forward(weights, frame):
    w_zero, w_one, w_two = weights
    edges = frame.shape[2]
    local = w_zero.shape[1]
    mixed = [
        product(w_zero.reshape(-1, w_zero.shape[2]), frame[:5].reshape(-1, edges)).reshape(
            5, local, edges
        )
    ]
    for weight, first, blocks in ((w_one, 5, 4), (w_two, 13, 3)):
        plus = frame[first : first + blocks].reshape(-1, edges)
        minus = frame[first + blocks : first + 2 * blocks].reshape(-1, edges)
        both = product(weight.reshape(-1, weight.shape[-1]), beside(plus, minus))
        both = both.reshape(2, blocks, local, 2 * edges)
        mixed.append(both[0, :, :, :edges] - both[1, :, :, edges:])
        mixed.append(both[0, :, :, edges:] + both[1, :, :, :edges])
    return jnp.concatenate(mixed, axis=0)


def mix_back(weights, grads, shares):
    w_zero, w_one, w_two = weights
    edges = grads.shape[2]

    def shared(block, blocks):
        shaped = block.reshape(blocks, shares, -1, edges).astype(jnp.bfloat16)
        return jnp.transpose(shaped, (1, 0, 2, 3))

    back = [
        shared(across(w_zero.reshape(-1, w_zero.shape[2]), grads[:5].reshape(-1, edges)), 5)
    ]
    for weight, first, blocks in ((w_one, 5, 4), (w_two, 13, 3)):
        plus = grads[first : first + blocks].reshape(-1, edges)
        minus = grads[first + blocks : first + 2 * blocks].reshape(-1, edges)
        sides = jnp.concatenate([beside(plus, minus), beside(minus, -plus)], axis=0)
        both = across(weight.reshape(-1, weight.shape[-1]), sides)
        back.append(shared(both[:, :edges], blocks))
        back.append(shared(both[:, edges:], blocks))
    return jnp.concatenate(back, axis=1)


def column_frames(frame):
    count = lax.axis_size("graph")
    near = 4
    far = count // near
    edges = frame.shape[2]
    cuts = ((0, 5), (5, 4), (9, 4), (13, 3), (16, 3))
    parts = [
        frame[first : first + blocks].reshape(far, near, -1, edges) for first, blocks in cuts
    ]
    widths = [part.shape[2] for part in parts]
    packed = jnp.concatenate(parts, axis=2)
    mine = lax.axis_index("graph") % near
    frames = []
    for bit in (0, 2, 1, 3):
        target = mine ^ bit
        chunk = lax.dynamic_index_in_dim(packed, target, axis=1, keepdims=False)
        frames.append(swap(chunk, bit) if bit else chunk)
    return frames, widths


def weight_grads(frames, widths, grads_all, local):
    count = lax.axis_size("graph")
    near = 4
    far = count // near
    edges = frames[0].shape[2]
    starts = [sum(widths[:i]) for i in range(5)]
    groups = [[z * near + q for z in range(far)] for q in range(near)]

    def settle(partial):
        return lax.psum_scatter(
            partial.astype(jnp.bfloat16),
            "graph",
            scatter_dimension=0,
            axis_index_groups=groups,
            tiled=False,
        ).astype(jnp.float32)

    def settle_direct(partial):
        partial = partial.astype(jnp.bfloat16)
        place = lax.axis_index("graph") // near
        total = lax.dynamic_index_in_dim(partial, place, axis=0, keepdims=False)
        total = total.astype(jnp.float32)
        for step in range(1, far):
            chunk = lax.dynamic_index_in_dim(partial, (place + step) % far, axis=0, keepdims=False)
            shift = [(i, (i + step * near) % count) for i in range(count)]
            total = total + lax.ppermute(chunk, "graph", shift).astype(jnp.float32)
        return total

    def columns(index):
        return [chunk[:, starts[index] : starts[index] + widths[index]] for chunk in frames]

    left = jnp.concatenate(columns(0), axis=2)
    right = jnp.concatenate([g[:5].reshape(-1, edges) for g in grads_all], axis=1)
    done = settle_direct(contract(left, right))
    results = [jnp.transpose(done).reshape(5, local, widths[0])]
    for index, first, blocks in ((1, 5, 4), (3, 13, 3)):
        plus, minus = columns(index), columns(index + 1)
        real_part = jnp.concatenate([x for pair in zip(plus, minus) for x in pair], axis=2)
        imag_part = jnp.concatenate([x for pair in zip(minus, plus) for x in (-pair[0], pair[1])], axis=2)
        left = jnp.concatenate([real_part, imag_part], axis=1)
        right = jnp.concatenate(
            [
                g[start : start + blocks].reshape(-1, edges)
                for g in grads_all
                for start in (first, first + blocks)
            ],
            axis=1,
        )
        done = settle(contract(left, right))
        done = done.reshape(2, widths[index], blocks * local)
        results.append(jnp.transpose(done, (0, 2, 1)).reshape(2, blocks, local, widths[index]))
    return results


NEAR = 4
PARTS = ((5, 1), (4, 2), (3, 2))
FIRSTS = (0, 5, 13)


def lanes(start, size):
    return pl.ds(pl.multiple_of(start, 128), size)


def turned(left, right):
    return lax.dot_general(
        left, right, (((1,), (1,)), ((), ())), preferred_element_type=jnp.float32
    )


def hot(size, codes, first=0):
    places = lax.broadcasted_iota(jnp.int32, (size, codes.shape[1]), 0) + first
    return (places == codes).astype(jnp.bfloat16)


class Links:
    def __init__(self, sends, recvs):
        self.sends, self.recvs, self.count, self.started = sends, recvs, 0, []

    def start(self, source, target, device):
        index = self.count
        self.count += 1
        copy = pltpu.make_async_remote_copy(
            src_ref=source,
            dst_ref=target,
            send_sem=self.sends.at[index],
            recv_sem=self.recvs.at[index],
            device_id=device,
            device_id_type=pl.DeviceIdType.MESH,
        )
        copy.start()
        self.started.append(copy)
        return copy

    def settle(self, copy):
        copy.wait_send()
        self.started = [one for one in self.started if one is not copy]

    def finish(self):
        for copy in self.started:
            copy.wait_send()


def layer_kernel(shares, count, *refs):
    (embed, cotangent, gain, w_zero, w_one, w_two, table) = refs[:7]
    (face_row, source_row, target_row, which_row, weight_row) = refs[7:12]
    (update, grad_embed, out_zero, out_one, out_two) = refs[12:17]
    weights = refs[17:20]
    frames = refs[20:23]
    grads = refs[23:26]
    doubled = (None,) + tuple(refs[26:28])
    nears = refs[28:31]
    back_out, back_in = refs[31:34], refs[34:37]
    kept, leaving, arriving, final = refs[37:40], refs[40:43], refs[43:46], refs[46:49]
    (work, back, arrow, values, normed, rot, gains) = refs[49:56]
    (face_out, face_in, ends_out, ends_in) = refs[56:60]
    (square_out, square_in, tally_out, tally_in) = refs[60:64]
    sends, recvs, local_sems = refs[64:67]
    outs = (out_zero, out_one, out_two)
    f32, bf16 = jnp.float32, jnp.bfloat16
    terms, width, atoms = values.shape
    edges = source_row.shape[1]
    halo = face_row.shape[1] // 2
    channels = width * shares
    me = lax.axis_index("graph")
    share = lax.axis_index("chan")
    low, side, pair, far = me % 2, (me // 2) % 2, (me // 4) % 2, (me // 8) % 2
    slot = pair * 2 + low
    batch = 5

    def flip(bit):
        digits = {1: low, 2: side, 4: pair, 8: far}
        place = me
        for one in (1, 2, 4, 8):
            if bit & one:
                place = place + one - 2 * one * digits[one]
        return (place, share)

    after, before = (lax.rem(me + 1, count), share), (lax.rem(me + count - 1, count), share)
    peers = [lax.rem(share + step, shares) for step in range(1, shares)]
    copies = []

    def bring(origin, target):
        copy = pltpu.make_async_copy(origin, target, local_sems.at[len(copies)])
        copy.start()
        copies.append(copy)
        return copy

    load_embed = bring(embed, values)
    load_cotangent = bring(cotangent, arrow)
    order = (1, 0, 2)
    loads = {at: bring((w_zero, w_one, w_two)[at], weights[at]) for at in order}

    barrier = pltpu.get_barrier_semaphore()
    others = [flip(bit) for bit in (1, 2, 4, 5, 8)] + [after, before]
    others += [(me, peer) for peer in peers]
    for other in others:
        pl.semaphore_signal(
            barrier, inc=1, device_id=other, device_id_type=pl.DeviceIdType.MESH
        )
    links = Links(sends, recvs)
    load_embed.wait()

    def squared(term, total):
        value = values[term].astype(f32)
        return total + value * value

    total = lax.fori_loop(0, terms, squared, jnp.zeros((width, atoms), f32))
    own_squares = jnp.sum(total, axis=0, keepdims=True)
    square_out[...] = jnp.broadcast_to(own_squares, square_out.shape)
    pl.semaphore_wait(barrier, len(others))
    summed = [
        links.start(square_out, square_in.at[index], (me, peer))
        for index, peer in enumerate(peers)
    ]

    which = hot(table.shape[2], which_row[...])

    def turn(term, unused):
        rest, total = table[term], None
        for _ in range(3):
            part = rest.astype(bf16)
            rest = rest - part.astype(f32)
            value = product(part, which)
            total = value if total is None else total + value
        rot[term] = total
        return unused

    lax.fori_loop(0, terms, turn, 0, unroll=5)
    degrees = lax.broadcasted_iota(jnp.int32, (5, atoms), 0)
    for degree in range(5):
        gains[degree] = lax.dot_general(
            gain[...],
            (degrees == degree).astype(f32),
            (((0,), (0,)), ((), ())),
            precision=HIGHEST,
            preferred_element_type=f32,
        )
    to_target = hot(atoms, target_row[...])
    to_source = hot(atoms, source_row[...])
    to_halo = hot(2 * halo, source_row[...], atoms)
    faces = hot(atoms, face_row[...])
    square = lax.broadcasted_iota(jnp.int32, (2 * halo, 2 * halo), 0)
    unit = (square == lax.broadcasted_iota(jnp.int32, square.shape, 1)).astype(bf16)
    to_face = turned(unit, faces).astype(bf16)
    scale = weight_row[...]

    whole = own_squares
    for index, copy in enumerate(summed):
        copy.wait_recv()
        whole = whole + square_in[index, :1, :]
    inverse = lax.rsqrt(whole / (terms * channels) + EPSILON)
    for degree in range(5):

        def normal(term, unused):
            normed[term] = (values[term].astype(f32) * inverse * gains[degree]).astype(bf16)
            return unused

        lax.fori_loop(degree * degree, (degree + 1) * (degree + 1), normal, 0)

    def fold(picks, target):
        def one(step, unused):
            value = normed[pl.ds(step * batch, batch)].reshape(batch * width, atoms)
            value = turned(picks, value).astype(bf16).reshape(2, halo, batch * width)
            target[:, :, lanes(step * batch * width, batch * width)] = value
            return unused

        lax.fori_loop(0, terms // batch, one, 0)

    def unfold(origin, picks):
        def one(step, unused):
            some = pl.ds(step * batch, batch)
            value = origin[:, :, lanes(step * batch * width, batch * width)]
            value = across(value.reshape(2 * halo, batch * width), picks)
            work[some] += value.reshape(batch, width, atoms)
            return unused

        lax.fori_loop(0, terms // batch, one, 0)

    fold(to_face, face_out)
    halos = [
        links.start(face_out.at[1], face_in.at[0], after),
        links.start(face_out.at[0], face_in.at[1], before),
    ]

    def spread(values_ref, picks):
        def one(step, unused):
            some = pl.ds(step * batch, batch)
            value = values_ref[some].reshape(batch * width, atoms)
            work[some] = product(value, picks).reshape(batch, width, edges)
            return unused

        lax.fori_loop(0, terms // batch, one, 0)

    tall = min(32, width)

    def rotate(at, put):
        first, (blocks, parts) = FIRSTS[at], PARTS[at]

        def one(step, unused):
            rows = pl.ds(pl.multiple_of(step * tall, tall), tall)
            for degree in range(5):
                base = degree * degree
                members = [
                    row
                    for row in range(first, first + blocks * parts)
                    if FRAME[row][0] == degree
                ]
                if not members:
                    continue
                lines = [work[base + index, rows, :] for index in range(2 * degree + 1)]
                for row in members:
                    line = None
                    for index, entry in enumerate(lines):
                        term = rot[base + index, row : row + 1, :] * entry
                        line = term if line is None else line + term
                    part, block = divmod(row - first, blocks)
                    put(block, part, step * tall, line)
            return unused

        lax.fori_loop(0, width // tall, one, 0)

    load_cotangent.wait()
    spread(arrow, to_target)
    near = [None] * 3

    def near_send(at):
        spots = [
            grads[at].at[:, lanes((part * NEAR + slot) * edges, edges)]
            for part in range(PARTS[at][1])
        ]
        near[at] = [
            [links.start(spot, spot, flip(4)) for spot in spots],
            [links.start(spot, spot, flip(1)) for spot in spots],
        ]

    for at in order:

        def put_grad(block, part, start, line):
            rows = pl.ds(pl.multiple_of(block * width + start, tall), tall)
            grads[at][rows, lanes((part * NEAR + slot) * edges, edges)] = (line * scale).astype(bf16)

        rotate(at, put_grad)
        if at == 1:
            near_send(1)
    spread(normed, to_source)
    for at in (1, 2):
        blocks = PARTS[at][0]
        height = blocks * width
        g = grads[at]
        plus = g[:, lanes(slot * edges, edges)]
        minus = g[:, lanes((NEAR + slot) * edges, edges)]
        doubled[at][:height, :edges] = plus
        doubled[at][:height, edges:] = minus
        doubled[at][height:, :edges] = minus
        doubled[at][height:, edges:] = -plus

    def backed(at, row, share_at):
        if at == 0:
            right = grads[0][:, lanes(slot * edges, edges)]
        else:
            right = doubled[at][...]
        left = weights[at][..., lanes(row * channels + share_at * width, width)]
        return across(left.reshape(-1, width), right)

    def back_leave(at):
        loads[at].wait()
        for index, peer in enumerate(peers):

            def one(row, unused):
                back_out[at][index, row] = backed(at, row, peer).astype(bf16)
                return unused

            lax.fori_loop(0, PARTS[at][0], one, 0)

    scattered = [None] * 3

    def back_send(at):
        scattered[at] = [
            links.start(back_out[at].at[index], back_in[at].at[index], (me, peer))
            for index, peer in enumerate(peers)
        ]

    def back_keep(at):
        first, (blocks, parts) = FIRSTS[at], PARTS[at]

        def one(row, unused):
            value = backed(at, row, share)
            for part in range(parts):
                back[first + part * blocks + row] = value[:, part * edges : (part + 1) * edges]
            return unused

        lax.fori_loop(0, blocks, one, 0)

    def relay(at):
        relays = []
        for part, copy in enumerate(near[at][0]):
            copy.wait_recv()
            spot = grads[at].at[:, lanes((part * NEAR + (1 - pair) * 2 + low) * edges, edges)]
            relays.append(links.start(spot, spot, flip(1)))
        near[at].append(relays)

    gathered = {}

    def share_frames(at, turn_at):
        blocks, parts = PARTS[at]
        size = (blocks + 1) // 2
        if turn_at == 0:
            start = (1 - far) * (blocks - size)
        else:
            start, size = far * size, blocks - size
        ours = frames[at].reshape(blocks, shares, width, parts * edges)
        ours = ours.at[pl.ds(start, size), share]
        gathered[at, turn_at] = [links.start(ours, ours, (me, peer)) for peer in peers]

    arrivals = {}
    places = (1 - far, far)

    def scatter(at, turn_at):
        for copy in gathered[at, turn_at]:
            copy.wait_recv()
        parts = PARTS[at][1]
        place = places[turn_at]
        short = nears[at].shape[2] // parts
        cut = frames[at].reshape(2, 2, 2, 2, short, parts * edges)
        waits = []
        for part in range(parts):
            here = nears[at].at[
                place, :, pl.ds(0, short), lanes((part * NEAR + slot) * edges, edges)
            ]
            spread_lanes = pl.ds(part * edges, edges)
            for bit in (4, 5, 1):
                its_pair = 1 - pair if bit & 4 else pair
                its_low = 1 - low if bit & 1 else low
                piece = cut.at[place, its_pair, :, its_low, :, spread_lanes]
                waits.append(links.start(piece, here, flip(bit)).wait_recv)
            waits.append(bring(cut.at[place, pair, :, low, :, spread_lanes], here).wait)
        arrivals[at, turn_at] = waits

    def mix(at):
        first, (blocks, parts) = FIRSTS[at], PARTS[at]

        def one(row, unused):
            if parts == 1:
                work[first + row] = product(weights[at][row], frames[at][...])
            else:
                real = product(weights[at][0, row], frames[at][...])
                imag = product(weights[at][1, row], frames[at][...])
                work[first + row] = real[:, :edges] - imag[:, edges:]
                work[first + blocks + row] = real[:, edges:] + imag[:, :edges]
            return unused

        lax.fori_loop(0, blocks, one, 0)

    def grown(at, place, step, one_side):
        columns = nears[at][place, one_side]
        rows = grads[at][pl.ds(pl.multiple_of(step * width, width), width), :]
        return turned(rows, columns) if at == 1 else turned(columns, rows)

    aside = {}
    away = {}
    pieces = {1: ((0, 2), (2, 4)), 0: ((0, 5),), 2: ((0, 3),)}

    def grow_leave(at, turn_at):
        for arrive in arrivals[at, turn_at]:
            arrive()
        if turn_at == 0:
            for group in near[at][1:]:
                for copy in group:
                    copy.wait_recv()
        parts = PARTS[at][1]
        place = places[turn_at]
        f, span = nears[at], NEAR * edges
        short = f.shape[2] // parts
        if parts == 2:
            for one_side in range(2):
                f[place, one_side, short:, :span] = -f[place, one_side, :short, span:]
                f[place, one_side, short:, span:] = f[place, one_side, :short, :span]

        def leave(step, unused):
            leaving[at][place, step] = grown(at, place, step, 1 - side).astype(bf16)
            return unused

        for index, (start, stop) in enumerate(pieces[at]):
            lax.fori_loop(start, stop, leave, 0)
            steps = pl.ds(start, stop - start)
            aside[at, turn_at, index] = links.start(
                leaving[at].at[place, steps], arriving[at].at[place, steps], flip(2)
            )

    def grow_keep(at, turn_at):
        place = places[turn_at]

        def stay(step, unused):
            kept[at][place, step] = grown(at, place, step, side)
            return unused

        lax.fori_loop(0, PARTS[at][0], stay, 0)

    def pass_on(at, index):
        start, stop = pieces[at][index]
        aside[at, 0, index].wait_recv()
        links.settle(aside[at, 0, index])
        place = places[0]

        def one(step, unused):
            total = kept[at][place, step] + arriving[at][place, step].astype(f32)
            leaving[at][place, step] = total.astype(bf16)
            return unused

        lax.fori_loop(start, stop, one, 0)
        steps = pl.ds(start, stop - start)
        away[at, index] = links.start(
            leaving[at].at[place, steps], final[at].at[steps], flip(8)
        )

    back_leave(1)
    for copy in halos:
        copy.wait_recv()
    unfold(face_in, to_halo)
    for at in order:
        blocks, parts = PARTS[at]

        def put_frame(block, part, start, line):
            rows = pl.ds(pl.multiple_of(block * channels + share * width + start, tall), tall)
            frames[at][rows, part * edges : (part + 1) * edges] = line.astype(bf16)

        rotate(at, put_frame)
        share_frames(at, 0)
    for at in order:
        share_frames(at, 1)
    back_send(1)
    back_leave(0)
    back_send(0)
    relay(1)
    scatter(1, 0)
    near_send(0)
    back_leave(2)
    back_send(2)
    back_keep(1)
    scatter(0, 0)
    near_send(2)
    grow_leave(1, 0)
    grow_keep(1, 0)
    scatter(2, 0)
    relay(0)
    back_keep(0)
    back_keep(2)
    scatter(1, 1)
    pass_on(1, 0)
    pass_on(1, 1)
    relay(2)
    scatter(0, 1)
    grow_leave(0, 0)
    grow_keep(0, 0)
    scatter(2, 1)
    mix(1)
    grow_leave(2, 0)
    grow_keep(2, 0)
    pass_on(0, 0)
    mix(0)
    grow_leave(1, 1)
    mix(2)
    pass_on(2, 0)
    grow_leave(0, 1)
    grow_leave(2, 1)

    def unturn(origin, factor, put):
        def one(step, unused):
            rows = pl.ds(pl.multiple_of(step * tall, tall), tall)
            for degree in range(5):
                members = [row for row, entry in enumerate(FRAME) if entry[0] == degree]
                lines = [origin[row, rows, :] for row in members]
                if factor is not None:
                    lines = [line * factor for line in lines]
                for column in range(degree * degree, (degree + 1) * (degree + 1)):
                    value = None
                    for row, line in zip(members, lines):
                        term = rot[column, row : row + 1, :] * line
                        value = term if value is None else value + term
                    put(column, rows, value)
            return unused

        lax.fori_loop(0, width // tall, one, 0)

    def put_normed(column, rows, value):
        normed[column, rows, :] = value.astype(bf16)

    unturn(work, scale, put_normed)

    def gather(picks, target):
        def one(step, unused):
            some = pl.ds(step * batch, batch)
            value = turned(normed[some].reshape(batch * width, edges), picks)
            target[some] = value.reshape(batch, width, atoms).astype(target.dtype)
            return unused

        lax.fori_loop(0, terms // batch, one, 0)

    gather(to_target, arrow)
    stored = [bring(arrow, update)]
    for at in order:
        grow_keep(at, 1)
    for at in order:
        first, (blocks, parts) = FIRSTS[at], PARTS[at]
        for index, copy in enumerate(scattered[at]):
            copy.wait_recv()

            def add(row, unused):
                arrived = back_in[at][index, row].astype(f32)
                for part in range(parts):
                    back[first + part * blocks + row] += arrived[
                        :, part * edges : (part + 1) * edges
                    ]
                return unused

            lax.fori_loop(0, blocks, add, 0)
    unturn(back, None, put_normed)

    fold(to_halo, ends_out)
    ends = [
        links.start(ends_out.at[1], ends_in.at[0], after),
        links.start(ends_out.at[0], ends_in.at[1], before),
    ]

    gather(to_source, work)
    for copy in ends:
        copy.wait_recv()
    unfold(ends_in, to_face)
    total = jnp.zeros((width, atoms), f32)
    for degree in range(5):

        def scaled(term, total):
            result = work[term] * inverse * gains[degree]
            work[term] = result
            return total + result * values[term].astype(f32)

        total = lax.fori_loop(degree * degree, (degree + 1) * (degree + 1), scaled, total)
    whole = jnp.sum(total, axis=0, keepdims=True)
    tally_out[...] = jnp.broadcast_to(whole, tally_out.shape)
    tallies = [
        links.start(tally_out, tally_in.at[index], (me, peer))
        for index, peer in enumerate(peers)
    ]
    for index, copy in enumerate(tallies):
        copy.wait_recv()
        whole = whole + tally_in[index, :1, :]
    factor = inverse * inverse * whole / (terms * channels)

    def finished(term, unused):
        normed[term] = (work[term] - values[term].astype(f32) * factor).astype(bf16)
        return unused

    lax.fori_loop(0, terms, finished, 0)
    stored.append(bring(normed, grad_embed))
    for at in order:
        for index in range(len(pieces[at])):
            aside[at, 1, index].wait_recv()
            away[at, index].wait_recv()

        def settled(step, unused):
            total = kept[at][far, step] + arriving[at][far, step].astype(f32)
            kept[at][far, step] = total + final[at][step].astype(f32)
            return unused

        lax.fori_loop(0, PARTS[at][0], settled, 0)
        ready = kept[at].at[far]
        if at == 0:
            stored.append(bring(ready, outs[at]))
        else:
            for part in range(2):
                short = outs[at].shape[-1 if at == 1 else -2]
                some = pl.ds(part * short, short)
                piece = ready.at[:, :, some] if at == 1 else ready.at[:, some]
                stored.append(bring(piece, outs[at].at[part]))
    links.finish()
    for copy in stored:
        copy.wait()


def run_layer(arrays, sizes):
    embed, w_zero, w_one, w_two = arrays[0], arrays[3], arrays[4], arrays[5]
    shares, count = sizes
    terms, width, atoms = embed.shape
    edges, halo = arrays[8].shape[1], arrays[7].shape[1] // 2
    channels = width * shares
    cuts = (w_zero.shape[2] // count, w_one.shape[3] // count, w_two.shape[3] // count)
    bf16, f32 = jnp.bfloat16, jnp.float32
    three = range(3)
    tall = [blocks * width for blocks, parts in PARTS]
    wide = [parts * cut for (blocks, parts), cut in zip(PARTS, cuts)]
    near = [NEAR * parts * edges for blocks, parts in PARTS]
    scratch = [(w.shape, bf16) for w in (w_zero, w_one, w_two)]
    scratch += [((blocks * channels, parts * edges), bf16) for blocks, parts in PARTS]
    scratch += [((tall[i], near[i]), bf16) for i in three]
    scratch += [((2 * tall[i], 2 * edges), bf16) for i in (1, 2)]
    scratch += [((2, 2, wide[i], near[i]), bf16) for i in three]
    scratch += 2 * [
        ((shares - 1, blocks, width, parts * edges), bf16) for blocks, parts in PARTS
    ]
    slabs = [
        (5, wide[0], width),
        (4, width, wide[1]),
        (3, wide[2], width),
    ]
    scratch += [((2,) + slab, f32) for slab in slabs]
    scratch += 2 * [((2,) + slab, bf16) for slab in slabs]
    scratch += [(slab, bf16) for slab in slabs]
    scratch += [
        ((terms, width, edges), f32),
        ((len(FRAME), width, edges), f32),
        ((terms, width, atoms), bf16),
        ((terms, width, atoms), bf16),
        ((terms, width, atoms), bf16),
        ((terms, len(FRAME), edges), f32),
        ((5, width, atoms), f32),
    ]
    scratch += 4 * [((2, halo, terms * width), bf16)]
    scratch += 2 * [((8, atoms), f32), ((shares - 1, 8, atoms), f32)]
    number = 11 * (shares - 1) + 15 + 30 + 12 + 4
    anywhere = pl.BlockSpec(memory_space=pl.ANY)
    inside = pl.BlockSpec(memory_space=pltpu.VMEM)
    return pl.pallas_call(
        functools.partial(layer_kernel, shares, count),
        in_specs=[anywhere] * 2 + [inside] + [anywhere] * 3 + [inside] * 6,
        out_specs=[anywhere] * 5,
        out_shape=[jax.ShapeDtypeStruct(embed.shape, bf16)] * 2
        + [
            jax.ShapeDtypeStruct((5, cuts[0], width), f32),
            jax.ShapeDtypeStruct((2, 4, width, cuts[1]), f32),
            jax.ShapeDtypeStruct((2, 3, cuts[2], width), f32),
        ],
        scratch_shapes=[pltpu.VMEM(shape, kind) for shape, kind in scratch]
        + [
            pltpu.SemaphoreType.DMA((number,)),
            pltpu.SemaphoreType.DMA((number,)),
            pltpu.SemaphoreType.DMA((32,)),
        ],
        compiler_params=pltpu.CompilerParams(
            collective_id=0, has_side_effects=True, vmem_limit_bytes=67043328
        ),
    )(*arrays)


def shards(
    embed,
    gain,
    w_zero,
    w_one,
    w_two,
    rot_table,
    face_atoms,
    edge_source,
    edge_target,
    rot_index,
    edge_weight,
    cotangent,
):
    atoms = embed.shape[2]
    local = embed.shape[1]
    halo = face_atoms.shape[0] // 2
    shares = lax.axis_size("chan")
    channels = local * shares
    weights = (w_zero, w_one, w_two)
    values = embed.astype(jnp.float32)
    gains = gain_rows(gain)
    rows, coefficients, rots = rot_table.shape
    which = (jnp.arange(rots, dtype=jnp.int32)[:, None] == rot_index[None, :]).astype(jnp.float32)
    rotations = jnp.dot(
        rot_table.reshape(rows * coefficients, rots),
        which,
        precision=HIGHEST,
        preferred_element_type=jnp.float32,
    )
    weight_row = edge_weight[None, :]
    ones = jnp.ones_like(weight_row)

    squares = lax.psum(jnp.sum(values * values, axis=(0, 1)), "chan")
    inverse = lax.rsqrt(squares / (25 * channels) + EPSILON)
    normed = (values * inverse[None, None, :] * gains[:, :, None]).astype(jnp.bfloat16)
    flat = normed.reshape(25 * local, atoms)
    faces = product(flat, hot_rows(atoms, face_atoms)).astype(jnp.bfloat16)
    table_end = from_beside(faces.reshape(25, local, 2 * halo), halo)

    grads = to_frames([(cotangent, hot_rows(atoms, edge_target))], rotations, weight_row)
    picks = hot_rows(atoms + 2 * halo, edge_source)
    own = to_frames([(normed, picks[:atoms]), (table_end, picks[atoms:])], rotations, ones)
    own, grads = lax.optimization_barrier((own, grads))
    piece = lax.all_gather(own, "chan", axis=1, tiled=True)

    grads_side = swap(grads, 2)
    pair = swap(jnp.stack([grads, grads_side]), 1)
    grads_all = [grads, grads_side, pair[0], pair[1]]

    back = lax.psum_scatter(
        mix_back(weights, grads, shares), "chan", scatter_dimension=0, tiled=False
    )
    frames, widths = column_frames(piece)
    mixed = mix_forward(weights, piece)
    mixed, frames = lax.optimization_barrier((mixed, frames))
    (update,) = to_atoms(
        mixed, rotations, weight_row, [hot_columns(edge_target, atoms)], [jnp.bfloat16]
    )
    leaving = hot_columns(edge_source, atoms + 2 * halo)
    mine, outward = to_atoms(
        back,
        rotations,
        ones,
        [leaving[:, :atoms], leaving[:, atoms:]],
        [jnp.float32, jnp.bfloat16],
    )
    incoming = from_beside(outward, halo)
    settled = product(incoming.reshape(25 * local, 2 * halo), hot_columns(face_atoms, atoms))
    grad_normed = mine + settled.reshape(25, local, atoms)
    scaled = inverse[None, None, :] * gains[:, :, None] * grad_normed
    tally = lax.psum(jnp.sum(values * scaled, axis=(0, 1)), "chan")
    grad_embed = (
        scaled
        - values * (inverse**2 * tally / (25 * channels))[None, None, :]
    ).astype(jnp.bfloat16)
    grad_zero, grad_one, grad_two = weight_grads(frames, widths, grads_all, local)
    return (update, grad_embed, grad_zero, grad_one, grad_two)


def shards_linked(
    embed,
    gain,
    w_zero,
    w_one,
    w_two,
    rot_table,
    face_atoms,
    edge_source,
    edge_target,
    rot_index,
    edge_weight,
    cotangent,
):
    arrays = (
        embed,
        cotangent,
        gain,
        w_zero,
        w_one,
        w_two,
        jnp.transpose(rot_table, (1, 0, 2)),
        face_atoms[None, :],
        edge_source[None, :],
        edge_target[None, :],
        rot_index[None, :],
        edge_weight[None, :],
    )
    sizes = (lax.axis_size("chan"), lax.axis_size("graph"))
    update, grad_embed, done_zero, done_one, done_two = run_layer(arrays, sizes)
    grad_zero = jnp.transpose(done_zero, (0, 2, 1))
    grad_two = jnp.transpose(done_two, (0, 1, 3, 2))
    return (update, grad_embed, grad_zero, done_one, grad_two)


def solution(mesh):
    placed = (
        P(None, "chan", "graph"),
        P(None, "chan"),
        P(None, "chan", None),
        P(None, None, "chan", None),
        P(None, None, "chan", None),
        P(),
        P("graph"),
        P("graph"),
        P("graph"),
        P("graph"),
        P("graph"),
        P(None, "chan", "graph"),
    )
    linked = mesh.shape["graph"] == 16 and mesh.shape["chan"] == 2
    return jax.shard_map(
        shards_linked if linked else shards,
        mesh=mesh,
        in_specs=placed,
        out_specs=(
            P(None, "chan", "graph"),
            P(None, "chan", "graph"),
            P(None, "chan", "graph"),
            P(None, None, "chan", "graph"),
            P(None, None, "chan", "graph"),
        ),
        check_vma=False,
    )
```

```python
import functools

import jax
import jax.numpy as jnp
from jax import lax
from jax.experimental import pallas as pl
from jax.experimental.pallas import tpu as pltpu
from jax.sharding import PartitionSpec as P


EPSILON = 1e-06
HIGHEST = lax.Precision.HIGHEST
FRAME = (
    (0, 0),
    (1, 0),
    (2, 0),
    (3, 0),
    (4, 0),
    (1, 1),
    (2, 1),
    (3, 1),
    (4, 1),
    (1, -1),
    (2, -1),
    (3, -1),
    (4, -1),
    (2, 2),
    (3, 2),
    (4, 2),
    (2, -2),
    (3, -2),
    (4, -2),
)


def gain_rows(gain):
    pieces = [
        jnp.broadcast_to(gain[degree : degree + 1], (2 * degree + 1, gain.shape[1]))
        for degree in range(5)
    ]
    return jnp.concatenate(pieces, axis=0)


def product(left, right):
    return jnp.dot(left, right, preferred_element_type=jnp.float32)


def across(left, right):
    return lax.dot_general(
        left, right, (((0,), (0,)), ((), ())), preferred_element_type=jnp.float32
    )


def contract(left, right):
    return lax.dot_general(left, right, (((2,), (1,)), ((), ())), preferred_element_type=jnp.float32)


def frames_kernel(*refs):
    pairs, (rotations, scale, out) = refs[:-3], refs[-3:]
    count, width = pairs[0].shape[0], pairs[0].shape[1]
    total = None
    for values, picks in zip(pairs[0::2], pairs[1::2]):
        part = product(values[...].reshape(count * width, values.shape[2]), picks[...])
        total = part if total is None else total + part
    total = total.reshape(count, width, total.shape[1])
    for row, (degree, _) in enumerate(FRAME):
        first = degree * degree
        entry = row * count + first
        line = rotations[entry : entry + 1, :] * total[first]
        for step in range(1, 2 * degree + 1):
            entry = row * count + first + step
            line = line + rotations[entry : entry + 1, :] * total[first + step]
        out[row] = (line * scale[...]).astype(out.dtype)


def to_frames(pairs, rotations, scale):
    count, local = pairs[0][0].shape[0], pairs[0][0].shape[1]
    edges = scale.shape[1]
    block = min(64, local)
    operands, specs = [], []
    for values, picks in pairs:
        operands += [values, picks]
        specs.append(pl.BlockSpec((count, block, values.shape[2]), lambda i: (0, i, 0)))
        specs.append(pl.BlockSpec(picks.shape, lambda i: (0, 0)))
    for whole in (rotations, scale):
        operands.append(whole)
        specs.append(pl.BlockSpec(whole.shape, lambda i: (0, 0)))
    return pl.pallas_call(
        frames_kernel,
        grid=(local // block,),
        in_specs=specs,
        out_specs=pl.BlockSpec((len(FRAME), block, edges), lambda i: (0, i, 0)),
        out_shape=jax.ShapeDtypeStruct((len(FRAME), local, edges), jnp.bfloat16),
        compiler_params=pltpu.CompilerParams(dimension_semantics=("arbitrary",)),
    )(*operands)


def atoms_kernel(count, values, rotations, scale, *refs):
    picks, outs, held = refs[: len(refs) // 2], refs[len(refs) // 2 : -1], refs[-1]
    width, edges = values.shape[1], values.shape[2]
    for degree in range(5):
        members = [row for row, pair in enumerate(FRAME) if pair[0] == degree]
        lines = [values[row].astype(jnp.float32) * scale[...] for row in members]
        for column in range(degree * degree, (degree + 1) * (degree + 1)):
            total = None
            for row, line in zip(members, lines):
                entry = row * count + column
                term = rotations[entry : entry + 1, :] * line
                total = term if total is None else total + term
            held[column] = total.astype(held.dtype)
    flat = held[...].reshape(count * width, edges)
    for pick, out in zip(picks, outs):
        out[...] = product(flat, pick[...]).reshape(out.shape).astype(out.dtype)


def to_atoms(values, rotations, scale, picks, kinds):
    rows, local, edges = values.shape
    count = rotations.shape[0] // rows
    block = min(64, local)
    whole = lambda i: (0, 0)
    return pl.pallas_call(
        functools.partial(atoms_kernel, count),
        grid=(local // block,),
        in_specs=[
            pl.BlockSpec((rows, block, edges), lambda i: (0, i, 0)),
            pl.BlockSpec(rotations.shape, whole),
            pl.BlockSpec(scale.shape, whole),
        ]
        + [pl.BlockSpec(pick.shape, whole) for pick in picks],
        out_specs=[
            pl.BlockSpec((count, block, pick.shape[1]), lambda i: (0, i, 0)) for pick in picks
        ],
        out_shape=[
            jax.ShapeDtypeStruct((count, local, pick.shape[1]), kind)
            for pick, kind in zip(picks, kinds)
        ],
        scratch_shapes=[pltpu.VMEM((count, block, edges), jnp.bfloat16)],
        compiler_params=pltpu.CompilerParams(dimension_semantics=("arbitrary",)),
    )(values, rotations, scale, *picks)


def swap(block, bit):
    count = lax.axis_size("graph")
    return lax.ppermute(block, "graph", [(i, i ^ bit) for i in range(count)])


def from_beside(faces, width):
    count = lax.axis_size("graph")
    forward = [(i, (i + 1) % count) for i in range(count)]
    backward = [(target, source) for source, target in forward]
    low = lax.ppermute(faces[:, :, width:], "graph", forward)
    high = lax.ppermute(faces[:, :, :width], "graph", backward)
    return jnp.concatenate([low, high], axis=2)


def hot_rows(size, codes):
    return (jnp.arange(size, dtype=jnp.int32)[:, None] == codes[None, :]).astype(jnp.bfloat16)


def hot_columns(codes, size):
    return (codes[:, None] == jnp.arange(size, dtype=jnp.int32)[None, :]).astype(jnp.bfloat16)


def beside(plus, minus, axis=-1):
    return jnp.concatenate([plus, minus], axis=axis)


def mix_forward(weights, frame):
    w_zero, w_one, w_two = weights
    edges = frame.shape[2]
    local = w_zero.shape[1]
    mixed = [
        product(w_zero.reshape(-1, w_zero.shape[2]), frame[:5].reshape(-1, edges)).reshape(
            5, local, edges
        )
    ]
    for weight, first, blocks in ((w_one, 5, 4), (w_two, 13, 3)):
        plus = frame[first : first + blocks].reshape(-1, edges)
        minus = frame[first + blocks : first + 2 * blocks].reshape(-1, edges)
        both = product(weight.reshape(-1, weight.shape[-1]), beside(plus, minus))
        both = both.reshape(2, blocks, local, 2 * edges)
        mixed.append(both[0, :, :, :edges] - both[1, :, :, edges:])
        mixed.append(both[0, :, :, edges:] + both[1, :, :, :edges])
    return jnp.concatenate(mixed, axis=0)


def mix_back(weights, grads, shares):
    w_zero, w_one, w_two = weights
    edges = grads.shape[2]

    def shared(block, blocks):
        shaped = block.reshape(blocks, shares, -1, edges).astype(jnp.bfloat16)
        return jnp.transpose(shaped, (1, 0, 2, 3))

    back = [
        shared(across(w_zero.reshape(-1, w_zero.shape[2]), grads[:5].reshape(-1, edges)), 5)
    ]
    for weight, first, blocks in ((w_one, 5, 4), (w_two, 13, 3)):
        plus = grads[first : first + blocks].reshape(-1, edges)
        minus = grads[first + blocks : first + 2 * blocks].reshape(-1, edges)
        sides = jnp.concatenate([beside(plus, minus), beside(minus, -plus)], axis=0)
        both = across(weight.reshape(-1, weight.shape[-1]), sides)
        back.append(shared(both[:, :edges], blocks))
        back.append(shared(both[:, edges:], blocks))
    return jnp.concatenate(back, axis=1)


def column_frames(frame):
    count = lax.axis_size("graph")
    near = 4
    far = count // near
    edges = frame.shape[2]
    cuts = ((0, 5), (5, 4), (9, 4), (13, 3), (16, 3))
    parts = [
        frame[first : first + blocks].reshape(far, near, -1, edges) for first, blocks in cuts
    ]
    widths = [part.shape[2] for part in parts]
    packed = jnp.concatenate(parts, axis=2)
    mine = lax.axis_index("graph") % near
    frames = []
    for bit in (0, 2, 1, 3):
        target = mine ^ bit
        chunk = lax.dynamic_index_in_dim(packed, target, axis=1, keepdims=False)
        frames.append(swap(chunk, bit) if bit else chunk)
    return frames, widths


def weight_grads(frames, widths, grads_all, local):
    count = lax.axis_size("graph")
    near = 4
    far = count // near
    edges = frames[0].shape[2]
    starts = [sum(widths[:i]) for i in range(5)]
    groups = [[z * near + q for z in range(far)] for q in range(near)]

    def settle(partial):
        return lax.psum_scatter(
            partial.astype(jnp.bfloat16),
            "graph",
            scatter_dimension=0,
            axis_index_groups=groups,
            tiled=False,
        ).astype(jnp.float32)

    def settle_direct(partial):
        partial = partial.astype(jnp.bfloat16)
        place = lax.axis_index("graph") // near
        total = lax.dynamic_index_in_dim(partial, place, axis=0, keepdims=False)
        total = total.astype(jnp.float32)
        for step in range(1, far):
            chunk = lax.dynamic_index_in_dim(partial, (place + step) % far, axis=0, keepdims=False)
            shift = [(i, (i + step * near) % count) for i in range(count)]
            total = total + lax.ppermute(chunk, "graph", shift).astype(jnp.float32)
        return total

    def columns(index):
        return [chunk[:, starts[index] : starts[index] + widths[index]] for chunk in frames]

    left = jnp.concatenate(columns(0), axis=2)
    right = jnp.concatenate([g[:5].reshape(-1, edges) for g in grads_all], axis=1)
    done = settle_direct(contract(left, right))
    results = [jnp.transpose(done).reshape(5, local, widths[0])]
    for index, first, blocks in ((1, 5, 4), (3, 13, 3)):
        plus, minus = columns(index), columns(index + 1)
        real_part = jnp.concatenate([x for pair in zip(plus, minus) for x in pair], axis=2)
        imag_part = jnp.concatenate([x for pair in zip(minus, plus) for x in (-pair[0], pair[1])], axis=2)
        left = jnp.concatenate([real_part, imag_part], axis=1)
        right = jnp.concatenate(
            [
                g[start : start + blocks].reshape(-1, edges)
                for g in grads_all
                for start in (first, first + blocks)
            ],
            axis=1,
        )
        done = settle(contract(left, right))
        done = done.reshape(2, widths[index], blocks * local)
        results.append(jnp.transpose(done, (0, 2, 1)).reshape(2, blocks, local, widths[index]))
    return results


NEAR = 4
PARTS = ((5, 1), (4, 2), (3, 2))
FIRSTS = (0, 5, 13)


def lanes(start, size):
    return pl.ds(pl.multiple_of(start, 128), size)


def turned(left, right):
    return lax.dot_general(
        left, right, (((1,), (1,)), ((), ())), preferred_element_type=jnp.float32
    )


def hot(size, codes, first=0):
    places = lax.broadcasted_iota(jnp.int32, (size, codes.shape[1]), 0) + first
    return (places == codes).astype(jnp.bfloat16)


class Links:
    def __init__(self, sends, recvs):
        self.sends, self.recvs, self.count, self.started = sends, recvs, 0, []

    def start(self, source, target, device):
        index = self.count
        self.count += 1
        copy = pltpu.make_async_remote_copy(
            src_ref=source,
            dst_ref=target,
            send_sem=self.sends.at[index],
            recv_sem=self.recvs.at[index],
            device_id=device,
            device_id_type=pl.DeviceIdType.MESH,
        )
        copy.start()
        self.started.append(copy)
        return copy

    def settle(self, copy):
        copy.wait_send()
        self.started = [one for one in self.started if one is not copy]

    def finish(self):
        for copy in self.started:
            copy.wait_send()


def layer_kernel(shares, count, *refs):
    (embed, cotangent, gain, w_zero, w_one, w_two, table) = refs[:7]
    (face_row, source_row, target_row, which_row, weight_row) = refs[7:12]
    (update, grad_embed, out_zero, out_one, out_two) = refs[12:17]
    weights = refs[17:20]
    frames = refs[20:23]
    grads = refs[23:26]
    doubled = (None,) + tuple(refs[26:28])
    nears = refs[28:31]
    back_out, back_in = refs[31:34], refs[34:37]
    kept, leaving, arriving, final = refs[37:40], refs[40:43], refs[43:46], refs[46:49]
    (work, back, arrow, values, normed, rot, gains) = refs[49:56]
    (face_out, face_in, ends_out, ends_in) = refs[56:60]
    (square_out, square_in, tally_out, tally_in) = refs[60:64]
    sends, recvs, local_sems = refs[64:67]
    outs = (out_zero, out_one, out_two)
    f32, bf16 = jnp.float32, jnp.bfloat16
    terms, width, atoms = values.shape
    edges = source_row.shape[1]
    halo = face_row.shape[1] // 2
    channels = width * shares
    me = lax.axis_index("graph")
    share = lax.axis_index("chan")
    low, side, pair, far = me % 2, (me // 2) % 2, (me // 4) % 2, (me // 8) % 2
    slot = pair * 2 + low
    batch = 5

    def flip(bit):
        digits = {1: low, 2: side, 4: pair, 8: far}
        place = me
        for one in (1, 2, 4, 8):
            if bit & one:
                place = place + one - 2 * one * digits[one]
        return (place, share)

    after, before = (lax.rem(me + 1, count), share), (lax.rem(me + count - 1, count), share)
    peers = [lax.rem(share + step, shares) for step in range(1, shares)]
    copies = []

    def bring(origin, target):
        copy = pltpu.make_async_copy(origin, target, local_sems.at[len(copies)])
        copy.start()
        copies.append(copy)
        return copy

    load_embed = bring(embed, values)
    load_cotangent = bring(cotangent, arrow)
    order = (1, 0, 2)
    loads = {at: bring((w_zero, w_one, w_two)[at], weights[at]) for at in order}

    barrier = pltpu.get_barrier_semaphore()
    others = [flip(bit) for bit in (1, 2, 4, 5, 8)] + [after, before]
    others += [(me, peer) for peer in peers]
    for other in others:
        pl.semaphore_signal(
            barrier, inc=1, device_id=other, device_id_type=pl.DeviceIdType.MESH
        )
    links = Links(sends, recvs)
    which = hot(table.shape[2], which_row[...])

    def turn(term, unused):
        rest, total = table[term], None
        for _ in range(3):
            part = rest.astype(bf16)
            rest = rest - part.astype(f32)
            value = product(part, which)
            total = value if total is None else total + value
        rot[term] = total
        return unused

    lax.fori_loop(0, terms, turn, 0, unroll=5)
    degrees = lax.broadcasted_iota(jnp.int32, (5, atoms), 0)
    for degree in range(5):
        gains[degree] = lax.dot_general(
            gain[...],
            (degrees == degree).astype(f32),
            (((0,), (0,)), ((), ())),
            precision=HIGHEST,
            preferred_element_type=f32,
        )
    to_target = hot(atoms, target_row[...])
    to_source = hot(atoms, source_row[...])
    to_halo = hot(2 * halo, source_row[...], atoms)
    faces = hot(atoms, face_row[...])
    square = lax.broadcasted_iota(jnp.int32, (2 * halo, 2 * halo), 0)
    unit = (square == lax.broadcasted_iota(jnp.int32, square.shape, 1)).astype(bf16)
    to_face = turned(unit, faces).astype(bf16)
    scale = weight_row[...]

    load_embed.wait()

    def squared(term, total):
        value = values[term].astype(f32)
        return total + value * value

    total = lax.fori_loop(0, terms, squared, jnp.zeros((width, atoms), f32))
    own_squares = jnp.sum(total, axis=0, keepdims=True)
    square_out[...] = jnp.broadcast_to(own_squares, square_out.shape)
    pl.semaphore_wait(barrier, len(others))
    summed = [
        links.start(square_out, square_in.at[index], (me, peer))
        for index, peer in enumerate(peers)
    ]

    whole = own_squares
    for index, copy in enumerate(summed):
        copy.wait_recv()
        whole = whole + square_in[index, :1, :]
    inverse = lax.rsqrt(whole / (terms * channels) + EPSILON)
    for degree in range(5):

        def normal(term, unused):
            normed[term] = (values[term].astype(f32) * inverse * gains[degree]).astype(bf16)
            return unused

        lax.fori_loop(degree * degree, (degree + 1) * (degree + 1), normal, 0)

    def fold(picks, target):
        def one(step, unused):
            value = normed[pl.ds(step * batch, batch)].reshape(batch * width, atoms)
            value = turned(picks, value).astype(bf16).reshape(2, halo, batch * width)
            target[:, :, lanes(step * batch * width, batch * width)] = value
            return unused

        lax.fori_loop(0, terms // batch, one, 0)

    def unfold(origin, picks):
        def one(step, unused):
            some = pl.ds(step * batch, batch)
            value = origin[:, :, lanes(step * batch * width, batch * width)]
            value = across(value.reshape(2 * halo, batch * width), picks)
            work[some] += value.reshape(batch, width, atoms)
            return unused

        lax.fori_loop(0, terms // batch, one, 0)

    fold(to_face, face_out)
    halos = [
        links.start(face_out.at[1], face_in.at[0], after),
        links.start(face_out.at[0], face_in.at[1], before),
    ]

    def spread(values_ref, picks):
        def one(step, unused):
            some = pl.ds(step * batch, batch)
            value = values_ref[some].reshape(batch * width, atoms)
            work[some] = product(value, picks).reshape(batch, width, edges)
            return unused

        lax.fori_loop(0, terms // batch, one, 0)

    tall = min(32, width)

    def rotate(at, put):
        first, (blocks, parts) = FIRSTS[at], PARTS[at]

        def one(step, unused):
            rows = pl.ds(pl.multiple_of(step * tall, tall), tall)
            for degree in range(5):
                base = degree * degree
                members = [
                    row
                    for row in range(first, first + blocks * parts)
                    if FRAME[row][0] == degree
                ]
                if not members:
                    continue
                lines = [work[base + index, rows, :] for index in range(2 * degree + 1)]
                for row in members:
                    line = None
                    for index, entry in enumerate(lines):
                        term = rot[base + index, row : row + 1, :] * entry
                        line = term if line is None else line + term
                    part, block = divmod(row - first, blocks)
                    put(block, part, step * tall, line)
            return unused

        lax.fori_loop(0, width // tall, one, 0)

    load_cotangent.wait()
    spread(arrow, to_target)
    near = [None] * 3

    def near_send(at):
        spots = [
            grads[at].at[:, lanes((part * NEAR + slot) * edges, edges)]
            for part in range(PARTS[at][1])
        ]
        near[at] = [
            [links.start(spot, spot, flip(4)) for spot in spots],
            [links.start(spot, spot, flip(1)) for spot in spots],
        ]

    for at in order:

        def put_grad(block, part, start, line):
            rows = pl.ds(pl.multiple_of(block * width + start, tall), tall)
            grads[at][rows, lanes((part * NEAR + slot) * edges, edges)] = (line * scale).astype(bf16)

        rotate(at, put_grad)
        if at == 1:
            near_send(1)
    for at in (1, 2):
        blocks = PARTS[at][0]
        height = blocks * width
        g = grads[at]
        plus = g[:, lanes(slot * edges, edges)]
        minus = g[:, lanes((NEAR + slot) * edges, edges)]
        doubled[at][:height, :edges] = plus
        doubled[at][:height, edges:] = minus
        doubled[at][height:, :edges] = minus
        doubled[at][height:, edges:] = -plus

    def backed(at, row, share_at):
        if at == 0:
            right = grads[0][:, lanes(slot * edges, edges)]
        else:
            right = doubled[at][...]
        left = weights[at][..., lanes(row * channels + share_at * width, width)]
        return across(left.reshape(-1, width), right)

    scattered = {at: [] for at in order}

    def back_leave(at, start, stop):
        if start == 0:
            loads[at].wait()
        for index, peer in enumerate(peers):

            def one(row, unused):
                back_out[at][index, row] = backed(at, row, peer).astype(bf16)
                return unused

            lax.fori_loop(start, stop, one, 0)

    def back_send(at, start, stop):
        rows = pl.ds(start, stop - start)
        scattered[at] += [
            links.start(back_out[at].at[index, rows], back_in[at].at[index, rows], (me, peer))
            for index, peer in enumerate(peers)
        ]

    def back_keep(at):
        first, (blocks, parts) = FIRSTS[at], PARTS[at]

        def one(row, unused):
            value = backed(at, row, share)
            for part in range(parts):
                back[first + part * blocks + row] = value[:, part * edges : (part + 1) * edges]
            return unused

        lax.fori_loop(0, blocks, one, 0)

    def relay(at):
        relays = []
        for part, copy in enumerate(near[at][0]):
            copy.wait_recv()
            spot = grads[at].at[:, lanes((part * NEAR + (1 - pair) * 2 + low) * edges, edges)]
            relays.append(links.start(spot, spot, flip(1)))
        near[at].append(relays)

    gathered = {}

    def share_frames(at, turn_at):
        blocks, parts = PARTS[at]
        size = (blocks + 1) // 2
        if turn_at == 0:
            start = (1 - far) * (blocks - size)
        else:
            start, size = far * size, blocks - size
        ours = frames[at].reshape(blocks, shares, width, parts * edges)
        ours = ours.at[pl.ds(start, size), share]
        gathered[at, turn_at] = [links.start(ours, ours, (me, peer)) for peer in peers]

    arrivals, passing, through = {}, {}, {}
    places = (1 - far, far)

    def scatter(at, turn_at, own):
        parts = PARTS[at][1]
        place = places[turn_at]
        short = nears[at].shape[2] // parts
        cut = frames[at].reshape(2, 2, 2, 2, short, parts * edges)
        one_side = share if own else 1 - share
        if not own:
            for copy in gathered[at, turn_at]:
                copy.wait_recv()
        waits = arrivals.setdefault((at, turn_at), [])
        for part in range(parts):
            spread_lanes = pl.ds(part * edges, edges)

            def here(first_slot, slots):
                start = (part * NEAR + first_slot) * edges
                return nears[at].at[
                    place, one_side, pl.ds(0, short), lanes(start, slots * edges)
                ]

            for bit in (4, 5, 1) if own else (1,):
                its_pair = 1 - pair if bit & 4 else pair
                its_low = 1 - low if bit & 1 else low
                piece = cut.at[place, its_pair, one_side, its_low, :, spread_lanes]
                copy = links.start(piece, here(slot, 1), flip(bit))
                if bit & 4:
                    passing.setdefault((at, turn_at, part), []).append(copy)
                else:
                    waits.append(copy.wait_recv)
            piece = cut.at[place, pair, one_side, low, :, spread_lanes]
            waits.append(bring(piece, here(slot, 1)).wait)
            if own:
                through[at, turn_at, part] = here((1 - pair) * 2, 2)

    def forward(at, turn_at):
        for part in range(PARTS[at][1]):
            for copy in passing[at, turn_at, part]:
                copy.wait_recv()
            spot = through[at, turn_at, part]
            arrivals[at, turn_at].append(links.start(spot, spot, (me, peers[0])).wait_recv)

    def scatter_both(at, turn_at):
        for copy in gathered[at, turn_at]:
            copy.wait_recv()
        parts = PARTS[at][1]
        place = places[turn_at]
        short = nears[at].shape[2] // parts
        cut = frames[at].reshape(2, 2, 2, 2, short, parts * edges)
        waits = []
        for part in range(parts):
            here = nears[at].at[
                place, :, pl.ds(0, short), lanes((part * NEAR + slot) * edges, edges)
            ]
            spread_lanes = pl.ds(part * edges, edges)
            for bit in (4, 5, 1):
                its_pair = 1 - pair if bit & 4 else pair
                its_low = 1 - low if bit & 1 else low
                piece = cut.at[place, its_pair, :, its_low, :, spread_lanes]
                waits.append(links.start(piece, here, flip(bit)).wait_recv)
            waits.append(bring(cut.at[place, pair, :, low, :, spread_lanes], here).wait)
        arrivals[at, turn_at] = waits

    def mix(at):
        first, (blocks, parts) = FIRSTS[at], PARTS[at]

        def one(row, unused):
            if parts == 1:
                work[first + row] = product(weights[at][row], frames[at][...])
            else:
                real = product(weights[at][0, row], frames[at][...])
                imag = product(weights[at][1, row], frames[at][...])
                work[first + row] = real[:, :edges] - imag[:, edges:]
                work[first + blocks + row] = real[:, edges:] + imag[:, :edges]
            return unused

        lax.fori_loop(0, blocks, one, 0)

    def grown(at, place, step, one_side):
        columns = nears[at][place, one_side]
        rows = grads[at][pl.ds(pl.multiple_of(step * width, width), width), :]
        return turned(rows, columns) if at == 1 else turned(columns, rows)

    aside = {}
    away = {}
    pieces = {1: ((0, 1), (1, 2), (2, 3), (3, 4)), 0: ((0, 3), (3, 5)), 2: ((0, 3),)}

    def grow_leave(at, turn_at):
        for arrive in arrivals[at, turn_at]:
            arrive()
        if turn_at == 0:
            for group in near[at][1:]:
                for copy in group:
                    copy.wait_recv()
        parts = PARTS[at][1]
        place = places[turn_at]
        f, span = nears[at], NEAR * edges
        short = f.shape[2] // parts
        if parts == 2:
            for one_side in range(2):
                f[place, one_side, short:, :span] = -f[place, one_side, :short, span:]
                f[place, one_side, short:, span:] = f[place, one_side, :short, :span]

        def leave(step, unused):
            leaving[at][place, step] = grown(at, place, step, 1 - side).astype(bf16)
            return unused

        for index, (start, stop) in enumerate(pieces[at]):
            lax.fori_loop(start, stop, leave, 0)
            steps = pl.ds(start, stop - start)
            aside[at, turn_at, index] = links.start(
                leaving[at].at[place, steps], arriving[at].at[place, steps], flip(2)
            )

    def grow_keep(at, turn_at):
        place = places[turn_at]

        def stay(step, unused):
            kept[at][place, step] = grown(at, place, step, side)
            return unused

        lax.fori_loop(0, PARTS[at][0], stay, 0)

    def pass_on(at, index):
        start, stop = pieces[at][index]
        aside[at, 0, index].wait_recv()
        links.settle(aside[at, 0, index])
        place = places[0]

        def one(step, unused):
            total = kept[at][place, step] + arriving[at][place, step].astype(f32)
            leaving[at][place, step] = total.astype(bf16)
            return unused

        lax.fori_loop(start, stop, one, 0)
        steps = pl.ds(start, stop - start)
        away[at, index] = links.start(
            leaving[at].at[place, steps], final[at].at[steps], flip(8)
        )

    back_leave(1, 0, 2)
    back_send(1, 0, 2)
    spread(normed, to_source)
    back_leave(1, 2, 4)
    for copy in halos:
        copy.wait_recv()
    unfold(face_in, to_halo)
    for at in order:
        blocks, _ = PARTS[at]

        def put_frame(block, part, start, line):
            rows = pl.ds(pl.multiple_of(block * channels + share * width + start, tall), tall)
            frames[at][rows, part * edges : (part + 1) * edges] = line.astype(bf16)

        rotate(at, put_frame)
        if at == 1:
            share_frames(1, 0)
            scatter(1, 0, True)
            scatter(1, 1, True)

    def unturn(origin, factor, put):
        def one(step, unused):
            rows = pl.ds(pl.multiple_of(step * tall, tall), tall)
            for degree in range(5):
                members = [row for row, entry in enumerate(FRAME) if entry[0] == degree]
                lines = [origin[row, rows, :] for row in members]
                if factor is not None:
                    lines = [line * factor for line in lines]
                for column in range(degree * degree, (degree + 1) * (degree + 1)):
                    value = None
                    for row, line in zip(members, lines):
                        term = rot[column, row : row + 1, :] * line
                        value = term if value is None else value + term
                    put(column, rows, value)
            return unused

        lax.fori_loop(0, width // tall, one, 0)

    def put_normed(column, rows, value):
        normed[column, rows, :] = value.astype(bf16)

    def gather(picks, target):
        def one(step, unused):
            some = pl.ds(step * batch, batch)
            value = turned(normed[some].reshape(batch * width, edges), picks)
            target[some] = value.reshape(batch, width, atoms).astype(target.dtype)
            return unused

        lax.fori_loop(0, terms // batch, one, 0)

    def back_add():
        for at in order:
            first, (blocks, parts) = FIRSTS[at], PARTS[at]
            for copy in scattered[at]:
                copy.wait_recv()
            for index in range(shares - 1):

                def add(row, unused):
                    arrived = back_in[at][index, row].astype(f32)
                    for part in range(parts):
                        back[first + part * blocks + row] += arrived[
                            :, part * edges : (part + 1) * edges
                        ]
                    return unused

                lax.fori_loop(0, blocks, add, 0)

    share_frames(0, 0)
    near_send(0)
    back_leave(0, 0, 5)
    relay(1)
    forward(1, 0)
    scatter(1, 0, False)
    share_frames(2, 0)
    share_frames(1, 1)
    back_leave(2, 0, 3)
    forward(1, 1)
    share_frames(0, 1)
    share_frames(2, 1)
    scatter_both(0, 0)
    near_send(2)
    grow_leave(1, 0)
    grow_keep(1, 0)
    back_send(1, 2, 4)
    back_send(0, 0, 5)
    back_keep(1)
    pass_on(1, 0)
    pass_on(1, 1)
    scatter_both(2, 0)
    back_keep(0)
    pass_on(1, 2)
    pass_on(1, 3)
    scatter(1, 1, False)
    relay(0)
    back_send(2, 0, 3)
    grow_leave(0, 0)
    grow_keep(0, 0)
    scatter_both(0, 1)
    scatter_both(2, 1)
    back_keep(2)
    mix(1)
    grow_leave(1, 1)
    grow_keep(1, 1)
    pass_on(0, 0)
    pass_on(0, 1)
    relay(2)
    grow_leave(2, 0)
    grow_keep(2, 0)
    mix(0)
    mix(2)
    unturn(work, scale, put_normed)
    gather(to_target, arrow)
    stored = [bring(arrow, update)]
    back_add()
    unturn(back, None, put_normed)
    fold(to_halo, ends_out)
    ends = [
        links.start(ends_out.at[1], ends_in.at[0], after),
        links.start(ends_out.at[0], ends_in.at[1], before),
    ]
    pass_on(2, 0)
    gather(to_source, work)
    grow_leave(0, 1)
    grow_keep(0, 1)
    grow_leave(2, 1)
    grow_keep(2, 1)
    for copy in ends:
        copy.wait_recv()
    unfold(ends_in, to_face)
    total = jnp.zeros((width, atoms), f32)
    for degree in range(5):

        def scaled(term, total):
            result = work[term] * inverse * gains[degree]
            work[term] = result
            return total + result * values[term].astype(f32)

        total = lax.fori_loop(degree * degree, (degree + 1) * (degree + 1), scaled, total)
    whole = jnp.sum(total, axis=0, keepdims=True)
    tally_out[...] = jnp.broadcast_to(whole, tally_out.shape)
    tallies = [
        links.start(tally_out, tally_in.at[index], (me, peer))
        for index, peer in enumerate(peers)
    ]
    for index, copy in enumerate(tallies):
        copy.wait_recv()
        whole = whole + tally_in[index, :1, :]
    factor = inverse * inverse * whole / (terms * channels)

    def finished(term, unused):
        normed[term] = (work[term] - values[term].astype(f32) * factor).astype(bf16)
        return unused

    lax.fori_loop(0, terms, finished, 0)
    stored.append(bring(normed, grad_embed))
    for at in order:
        for index in range(len(pieces[at])):
            aside[at, 1, index].wait_recv()
            away[at, index].wait_recv()

        def settled(step, unused):
            total = kept[at][far, step] + arriving[at][far, step].astype(f32)
            kept[at][far, step] = total + final[at][step].astype(f32)
            return unused

        lax.fori_loop(0, PARTS[at][0], settled, 0)
        ready = kept[at].at[far]
        if at == 0:
            stored.append(bring(ready, outs[at]))
        else:
            for part in range(2):
                short = outs[at].shape[-1 if at == 1 else -2]
                some = pl.ds(part * short, short)
                piece = ready.at[:, :, some] if at == 1 else ready.at[:, some]
                stored.append(bring(piece, outs[at].at[part]))
    links.finish()
    for copy in stored:
        copy.wait()


def run_layer(arrays, sizes):
    embed, w_zero, w_one, w_two = arrays[0], arrays[3], arrays[4], arrays[5]
    shares, count = sizes
    terms, width, atoms = embed.shape
    edges, halo = arrays[8].shape[1], arrays[7].shape[1] // 2
    channels = width * shares
    cuts = (w_zero.shape[2] // count, w_one.shape[3] // count, w_two.shape[3] // count)
    bf16, f32 = jnp.bfloat16, jnp.float32
    three = range(3)
    tall = [blocks * width for blocks, parts in PARTS]
    wide = [parts * cut for (blocks, parts), cut in zip(PARTS, cuts)]
    near = [NEAR * parts * edges for blocks, parts in PARTS]
    scratch = [(w.shape, bf16) for w in (w_zero, w_one, w_two)]
    scratch += [((blocks * channels, parts * edges), bf16) for blocks, parts in PARTS]
    scratch += [((tall[i], near[i]), bf16) for i in three]
    scratch += [((2 * tall[i], 2 * edges), bf16) for i in (1, 2)]
    scratch += [((2, 2, wide[i], near[i]), bf16) for i in three]
    scratch += 2 * [
        ((shares - 1, blocks, width, parts * edges), bf16) for blocks, parts in PARTS
    ]
    slabs = [
        (5, wide[0], width),
        (4, width, wide[1]),
        (3, wide[2], width),
    ]
    scratch += [((2,) + slab, f32) for slab in slabs]
    scratch += 2 * [((2,) + slab, bf16) for slab in slabs]
    scratch += [(slab, bf16) for slab in slabs]
    scratch += [
        ((terms, width, edges), f32),
        ((len(FRAME), width, edges), f32),
        ((terms, width, atoms), bf16),
        ((terms, width, atoms), bf16),
        ((terms, width, atoms), bf16),
        ((terms, len(FRAME), edges), f32),
        ((5, width, atoms), f32),
    ]
    scratch += 4 * [((2, halo, terms * width), bf16)]
    scratch += 2 * [((8, atoms), f32), ((shares - 1, 8, atoms), f32)]
    number = 16 * (shares - 1) + 15 + 50 + 24 + 4
    anywhere = pl.BlockSpec(memory_space=pl.ANY)
    inside = pl.BlockSpec(memory_space=pltpu.VMEM)
    return pl.pallas_call(
        functools.partial(layer_kernel, shares, count),
        in_specs=[anywhere] * 2 + [inside] + [anywhere] * 3 + [inside] * 6,
        out_specs=[anywhere] * 5,
        out_shape=[jax.ShapeDtypeStruct(embed.shape, bf16)] * 2
        + [
            jax.ShapeDtypeStruct((5, cuts[0], width), f32),
            jax.ShapeDtypeStruct((2, 4, width, cuts[1]), f32),
            jax.ShapeDtypeStruct((2, 3, cuts[2], width), f32),
        ],
        scratch_shapes=[pltpu.VMEM(shape, kind) for shape, kind in scratch]
        + [
            pltpu.SemaphoreType.DMA((number,)),
            pltpu.SemaphoreType.DMA((number,)),
            pltpu.SemaphoreType.DMA((48,)),
        ],
        compiler_params=pltpu.CompilerParams(
            collective_id=0, has_side_effects=True, vmem_limit_bytes=67043328
        ),
    )(*arrays)


def carry_kernel(*refs):
    count = (len(refs) - 1) // 3
    sems = refs[-1]
    origins, targets, held = refs[:count], refs[count : 2 * count], refs[2 * count : 3 * count]
    reads = [
        pltpu.make_async_copy(origin, here, sems.at[0, index])
        for index, (origin, here) in enumerate(zip(origins, held))
    ]
    writes = [
        pltpu.make_async_copy(here, target, sems.at[1, index])
        for index, (here, target) in enumerate(zip(held, targets))
    ]
    for read in reads:
        read.start()
    for read, write in zip(reads, writes):
        read.wait()
        write.start()
    for write in writes:
        write.wait()


def carry_out(arrays):
    anywhere = [pl.BlockSpec(memory_space=pl.ANY)] * len(arrays)
    return pl.pallas_call(
        carry_kernel,
        in_specs=anywhere,
        out_specs=anywhere,
        out_shape=[jax.ShapeDtypeStruct(array.shape, array.dtype) for array in arrays],
        scratch_shapes=[pltpu.VMEM(array.shape, array.dtype) for array in arrays]
        + [pltpu.SemaphoreType.DMA((2, len(arrays)))],
        compiler_params=pltpu.CompilerParams(vmem_limit_bytes=67043328),
    )(*arrays)


def shards(
    embed,
    gain,
    w_zero,
    w_one,
    w_two,
    rot_table,
    face_atoms,
    edge_source,
    edge_target,
    rot_index,
    edge_weight,
    cotangent,
):
    atoms = embed.shape[2]
    local = embed.shape[1]
    halo = face_atoms.shape[0] // 2
    shares = lax.axis_size("chan")
    channels = local * shares
    weights = (w_zero, w_one, w_two)
    values = embed.astype(jnp.float32)
    gains = gain_rows(gain)
    rows, coefficients, rots = rot_table.shape
    which = (jnp.arange(rots, dtype=jnp.int32)[:, None] == rot_index[None, :]).astype(jnp.float32)
    rotations = jnp.dot(
        rot_table.reshape(rows * coefficients, rots),
        which,
        precision=HIGHEST,
        preferred_element_type=jnp.float32,
    )
    weight_row = edge_weight[None, :]
    ones = jnp.ones_like(weight_row)

    squares = lax.psum(jnp.sum(values * values, axis=(0, 1)), "chan")
    inverse = lax.rsqrt(squares / (25 * channels) + EPSILON)
    normed = (values * inverse[None, None, :] * gains[:, :, None]).astype(jnp.bfloat16)
    flat = normed.reshape(25 * local, atoms)
    faces = product(flat, hot_rows(atoms, face_atoms)).astype(jnp.bfloat16)
    table_end = from_beside(faces.reshape(25, local, 2 * halo), halo)

    grads = to_frames([(cotangent, hot_rows(atoms, edge_target))], rotations, weight_row)
    picks = hot_rows(atoms + 2 * halo, edge_source)
    own = to_frames([(normed, picks[:atoms]), (table_end, picks[atoms:])], rotations, ones)
    own, grads = lax.optimization_barrier((own, grads))
    piece = lax.all_gather(own, "chan", axis=1, tiled=True)

    grads_side = swap(grads, 2)
    pair = swap(jnp.stack([grads, grads_side]), 1)
    grads_all = [grads, grads_side, pair[0], pair[1]]

    back = lax.psum_scatter(
        mix_back(weights, grads, shares), "chan", scatter_dimension=0, tiled=False
    )
    frames, widths = column_frames(piece)
    mixed = mix_forward(weights, piece)
    mixed, frames = lax.optimization_barrier((mixed, frames))
    (update,) = to_atoms(
        mixed, rotations, weight_row, [hot_columns(edge_target, atoms)], [jnp.bfloat16]
    )
    leaving = hot_columns(edge_source, atoms + 2 * halo)
    mine, outward = to_atoms(
        back,
        rotations,
        ones,
        [leaving[:, :atoms], leaving[:, atoms:]],
        [jnp.float32, jnp.bfloat16],
    )
    incoming = from_beside(outward, halo)
    settled = product(incoming.reshape(25 * local, 2 * halo), hot_columns(face_atoms, atoms))
    grad_normed = mine + settled.reshape(25, local, atoms)
    scaled = inverse[None, None, :] * gains[:, :, None] * grad_normed
    tally = lax.psum(jnp.sum(values * scaled, axis=(0, 1)), "chan")
    grad_embed = (
        scaled
        - values * (inverse**2 * tally / (25 * channels))[None, None, :]
    ).astype(jnp.bfloat16)
    grad_zero, grad_one, grad_two = weight_grads(frames, widths, grads_all, local)
    return (update, grad_embed, grad_zero, grad_one, grad_two)


def shards_linked(
    embed,
    gain,
    w_zero,
    w_one,
    w_two,
    rot_table,
    face_atoms,
    edge_source,
    edge_target,
    rot_index,
    edge_weight,
    cotangent,
):
    arrays = (
        embed,
        cotangent,
        gain,
        w_zero,
        w_one,
        w_two,
        jnp.transpose(rot_table, (1, 0, 2)),
        face_atoms[None, :],
        edge_source[None, :],
        edge_target[None, :],
        rot_index[None, :],
        edge_weight[None, :],
    )
    sizes = (lax.axis_size("chan"), lax.axis_size("graph"))
    update, grad_embed, done_zero, done_one, done_two = carry_out(run_layer(arrays, sizes))
    grad_zero = jnp.transpose(done_zero, (0, 2, 1))
    grad_two = jnp.transpose(done_two, (0, 1, 3, 2))
    return (update, grad_embed, grad_zero, done_one, grad_two)


def solution(mesh):
    placed = (
        P(None, "chan", "graph"),
        P(None, "chan"),
        P(None, "chan", None),
        P(None, None, "chan", None),
        P(None, None, "chan", None),
        P(),
        P("graph"),
        P("graph"),
        P("graph"),
        P("graph"),
        P("graph"),
        P(None, "chan", "graph"),
    )
    linked = mesh.shape["graph"] == 16 and mesh.shape["chan"] == 2
    return jax.shard_map(
        shards_linked if linked else shards,
        mesh=mesh,
        in_specs=placed,
        out_specs=(
            P(None, "chan", "graph"),
            P(None, "chan", "graph"),
            P(None, "chan", "graph"),
            P(None, None, "chan", "graph"),
            P(None, None, "chan", "graph"),
        ),
        check_vma=False,
    )
```

```python
import functools

import jax
import jax.numpy as jnp
from jax import lax
from jax.experimental import pallas as pl
from jax.experimental.pallas import tpu as pltpu
from jax.sharding import PartitionSpec as P


EPSILON = 1e-06
HIGHEST = lax.Precision.HIGHEST
FRAME = (
    (0, 0),
    (1, 0),
    (2, 0),
    (3, 0),
    (4, 0),
    (1, 1),
    (2, 1),
    (3, 1),
    (4, 1),
    (1, -1),
    (2, -1),
    (3, -1),
    (4, -1),
    (2, 2),
    (3, 2),
    (4, 2),
    (2, -2),
    (3, -2),
    (4, -2),
)


def gain_rows(gain):
    pieces = [
        jnp.broadcast_to(gain[degree : degree + 1], (2 * degree + 1, gain.shape[1]))
        for degree in range(5)
    ]
    return jnp.concatenate(pieces, axis=0)


def product(left, right):
    return jnp.dot(left, right, preferred_element_type=jnp.float32)


def across(left, right):
    return lax.dot_general(
        left, right, (((0,), (0,)), ((), ())), preferred_element_type=jnp.float32
    )


def contract(left, right):
    return lax.dot_general(left, right, (((2,), (1,)), ((), ())), preferred_element_type=jnp.float32)


def frames_kernel(*refs):
    pairs, (rotations, scale, out) = refs[:-3], refs[-3:]
    count, width = pairs[0].shape[0], pairs[0].shape[1]
    total = None
    for values, picks in zip(pairs[0::2], pairs[1::2]):
        part = product(values[...].reshape(count * width, values.shape[2]), picks[...])
        total = part if total is None else total + part
    total = total.reshape(count, width, total.shape[1])
    for row, (degree, _) in enumerate(FRAME):
        first = degree * degree
        entry = row * count + first
        line = rotations[entry : entry + 1, :] * total[first]
        for step in range(1, 2 * degree + 1):
            entry = row * count + first + step
            line = line + rotations[entry : entry + 1, :] * total[first + step]
        out[row] = (line * scale[...]).astype(out.dtype)


def to_frames(pairs, rotations, scale):
    count, local = pairs[0][0].shape[0], pairs[0][0].shape[1]
    edges = scale.shape[1]
    block = min(64, local)
    operands, specs = [], []
    for values, picks in pairs:
        operands += [values, picks]
        specs.append(pl.BlockSpec((count, block, values.shape[2]), lambda i: (0, i, 0)))
        specs.append(pl.BlockSpec(picks.shape, lambda i: (0, 0)))
    for whole in (rotations, scale):
        operands.append(whole)
        specs.append(pl.BlockSpec(whole.shape, lambda i: (0, 0)))
    return pl.pallas_call(
        frames_kernel,
        grid=(local // block,),
        in_specs=specs,
        out_specs=pl.BlockSpec((len(FRAME), block, edges), lambda i: (0, i, 0)),
        out_shape=jax.ShapeDtypeStruct((len(FRAME), local, edges), jnp.bfloat16),
        compiler_params=pltpu.CompilerParams(dimension_semantics=("arbitrary",)),
    )(*operands)


def atoms_kernel(count, values, rotations, scale, *refs):
    picks, outs, held = refs[: len(refs) // 2], refs[len(refs) // 2 : -1], refs[-1]
    width, edges = values.shape[1], values.shape[2]
    for degree in range(5):
        members = [row for row, pair in enumerate(FRAME) if pair[0] == degree]
        lines = [values[row].astype(jnp.float32) * scale[...] for row in members]
        for column in range(degree * degree, (degree + 1) * (degree + 1)):
            total = None
            for row, line in zip(members, lines):
                entry = row * count + column
                term = rotations[entry : entry + 1, :] * line
                total = term if total is None else total + term
            held[column] = total.astype(held.dtype)
    flat = held[...].reshape(count * width, edges)
    for pick, out in zip(picks, outs):
        out[...] = product(flat, pick[...]).reshape(out.shape).astype(out.dtype)


def to_atoms(values, rotations, scale, picks, kinds):
    rows, local, edges = values.shape
    count = rotations.shape[0] // rows
    block = min(64, local)
    whole = lambda i: (0, 0)
    return pl.pallas_call(
        functools.partial(atoms_kernel, count),
        grid=(local // block,),
        in_specs=[
            pl.BlockSpec((rows, block, edges), lambda i: (0, i, 0)),
            pl.BlockSpec(rotations.shape, whole),
            pl.BlockSpec(scale.shape, whole),
        ]
        + [pl.BlockSpec(pick.shape, whole) for pick in picks],
        out_specs=[
            pl.BlockSpec((count, block, pick.shape[1]), lambda i: (0, i, 0)) for pick in picks
        ],
        out_shape=[
            jax.ShapeDtypeStruct((count, local, pick.shape[1]), kind)
            for pick, kind in zip(picks, kinds)
        ],
        scratch_shapes=[pltpu.VMEM((count, block, edges), jnp.bfloat16)],
        compiler_params=pltpu.CompilerParams(dimension_semantics=("arbitrary",)),
    )(values, rotations, scale, *picks)


def swap(block, bit):
    count = lax.axis_size("graph")
    return lax.ppermute(block, "graph", [(i, i ^ bit) for i in range(count)])


def from_beside(faces, width):
    count = lax.axis_size("graph")
    forward = [(i, (i + 1) % count) for i in range(count)]
    backward = [(target, source) for source, target in forward]
    low = lax.ppermute(faces[:, :, width:], "graph", forward)
    high = lax.ppermute(faces[:, :, :width], "graph", backward)
    return jnp.concatenate([low, high], axis=2)


def hot_rows(size, codes):
    return (jnp.arange(size, dtype=jnp.int32)[:, None] == codes[None, :]).astype(jnp.bfloat16)


def hot_columns(codes, size):
    return (codes[:, None] == jnp.arange(size, dtype=jnp.int32)[None, :]).astype(jnp.bfloat16)


def beside(plus, minus, axis=-1):
    return jnp.concatenate([plus, minus], axis=axis)


def mix_forward(weights, frame):
    w_zero, w_one, w_two = weights
    edges = frame.shape[2]
    local = w_zero.shape[1]
    mixed = [
        product(w_zero.reshape(-1, w_zero.shape[2]), frame[:5].reshape(-1, edges)).reshape(
            5, local, edges
        )
    ]
    for weight, first, blocks in ((w_one, 5, 4), (w_two, 13, 3)):
        plus = frame[first : first + blocks].reshape(-1, edges)
        minus = frame[first + blocks : first + 2 * blocks].reshape(-1, edges)
        both = product(weight.reshape(-1, weight.shape[-1]), beside(plus, minus))
        both = both.reshape(2, blocks, local, 2 * edges)
        mixed.append(both[0, :, :, :edges] - both[1, :, :, edges:])
        mixed.append(both[0, :, :, edges:] + both[1, :, :, :edges])
    return jnp.concatenate(mixed, axis=0)


def mix_back(weights, grads, shares):
    w_zero, w_one, w_two = weights
    edges = grads.shape[2]

    def shared(block, blocks):
        shaped = block.reshape(blocks, shares, -1, edges).astype(jnp.bfloat16)
        return jnp.transpose(shaped, (1, 0, 2, 3))

    back = [
        shared(across(w_zero.reshape(-1, w_zero.shape[2]), grads[:5].reshape(-1, edges)), 5)
    ]
    for weight, first, blocks in ((w_one, 5, 4), (w_two, 13, 3)):
        plus = grads[first : first + blocks].reshape(-1, edges)
        minus = grads[first + blocks : first + 2 * blocks].reshape(-1, edges)
        sides = jnp.concatenate([beside(plus, minus), beside(minus, -plus)], axis=0)
        both = across(weight.reshape(-1, weight.shape[-1]), sides)
        back.append(shared(both[:, :edges], blocks))
        back.append(shared(both[:, edges:], blocks))
    return jnp.concatenate(back, axis=1)


def column_frames(frame):
    count = lax.axis_size("graph")
    near = 4
    far = count // near
    edges = frame.shape[2]
    cuts = ((0, 5), (5, 4), (9, 4), (13, 3), (16, 3))
    parts = [
        frame[first : first + blocks].reshape(far, near, -1, edges) for first, blocks in cuts
    ]
    widths = [part.shape[2] for part in parts]
    packed = jnp.concatenate(parts, axis=2)
    mine = lax.axis_index("graph") % near
    frames = []
    for bit in (0, 2, 1, 3):
        target = mine ^ bit
        chunk = lax.dynamic_index_in_dim(packed, target, axis=1, keepdims=False)
        frames.append(swap(chunk, bit) if bit else chunk)
    return frames, widths


def weight_grads(frames, widths, grads_all, local):
    count = lax.axis_size("graph")
    near = 4
    far = count // near
    edges = frames[0].shape[2]
    starts = [sum(widths[:i]) for i in range(5)]
    groups = [[z * near + q for z in range(far)] for q in range(near)]

    def settle(partial):
        return lax.psum_scatter(
            partial.astype(jnp.bfloat16),
            "graph",
            scatter_dimension=0,
            axis_index_groups=groups,
            tiled=False,
        ).astype(jnp.float32)

    def settle_direct(partial):
        partial = partial.astype(jnp.bfloat16)
        place = lax.axis_index("graph") // near
        total = lax.dynamic_index_in_dim(partial, place, axis=0, keepdims=False)
        total = total.astype(jnp.float32)
        for step in range(1, far):
            chunk = lax.dynamic_index_in_dim(partial, (place + step) % far, axis=0, keepdims=False)
            shift = [(i, (i + step * near) % count) for i in range(count)]
            total = total + lax.ppermute(chunk, "graph", shift).astype(jnp.float32)
        return total

    def columns(index):
        return [chunk[:, starts[index] : starts[index] + widths[index]] for chunk in frames]

    left = jnp.concatenate(columns(0), axis=2)
    right = jnp.concatenate([g[:5].reshape(-1, edges) for g in grads_all], axis=1)
    done = settle_direct(contract(left, right))
    results = [jnp.transpose(done).reshape(5, local, widths[0])]
    for index, first, blocks in ((1, 5, 4), (3, 13, 3)):
        plus, minus = columns(index), columns(index + 1)
        real_part = jnp.concatenate([x for pair in zip(plus, minus) for x in pair], axis=2)
        imag_part = jnp.concatenate([x for pair in zip(minus, plus) for x in (-pair[0], pair[1])], axis=2)
        left = jnp.concatenate([real_part, imag_part], axis=1)
        right = jnp.concatenate(
            [
                g[start : start + blocks].reshape(-1, edges)
                for g in grads_all
                for start in (first, first + blocks)
            ],
            axis=1,
        )
        done = settle(contract(left, right))
        done = done.reshape(2, widths[index], blocks * local)
        results.append(jnp.transpose(done, (0, 2, 1)).reshape(2, blocks, local, widths[index]))
    return results


NEAR = 4
PARTS = ((5, 1), (4, 2), (3, 2))
FIRSTS = (0, 5, 13)


def lanes(start, size):
    return pl.ds(pl.multiple_of(start, 128), size)


def turned(left, right):
    return lax.dot_general(
        left, right, (((1,), (1,)), ((), ())), preferred_element_type=jnp.float32
    )


def hot(size, codes, first=0):
    places = lax.broadcasted_iota(jnp.int32, (size, codes.shape[1]), 0) + first
    return (places == codes).astype(jnp.bfloat16)


class Links:
    def __init__(self, sends, recvs):
        self.sends, self.recvs, self.count, self.started = sends, recvs, 0, []

    def start(self, source, target, device):
        index = self.count
        self.count += 1
        copy = pltpu.make_async_remote_copy(
            src_ref=source,
            dst_ref=target,
            send_sem=self.sends.at[index],
            recv_sem=self.recvs.at[index],
            device_id=device,
            device_id_type=pl.DeviceIdType.MESH,
        )
        copy.start()
        self.started.append(copy)
        return copy

    def settle(self, copy):
        copy.wait_send()
        self.started = [one for one in self.started if one is not copy]

    def finish(self):
        for copy in self.started:
            copy.wait_send()


def layer_kernel(shares, count, *refs):
    (embed, cotangent, gain, w_zero, w_one, w_two, table) = refs[:7]
    (face_row, source_row, target_row, which_row, weight_row) = refs[7:12]
    (update, grad_embed, out_zero, out_one, out_two) = refs[12:17]
    weights = refs[17:20]
    frames = refs[20:23]
    grads = refs[23:26]
    doubled = (None,) + tuple(refs[26:28])
    nears = refs[28:31]
    back_out, back_in = refs[31:34], refs[34:37]
    kept, leaving, arriving, final = refs[37:40], refs[40:43], refs[43:46], refs[46:49]
    (work, back, arrow, values, normed, rot, gains) = refs[49:56]
    (face_out, face_in, ends_out, ends_in) = refs[56:60]
    (square_out, square_in, tally_out, tally_in) = refs[60:64]
    sends, recvs, local_sems = refs[64:67]
    outs = (out_zero, out_one, out_two)
    f32, bf16 = jnp.float32, jnp.bfloat16
    terms, width, atoms = values.shape
    edges = source_row.shape[1]
    halo = face_row.shape[1] // 2
    channels = width * shares
    me = lax.axis_index("graph")
    share = lax.axis_index("chan")
    low, side, pair, far = me % 2, (me // 2) % 2, (me // 4) % 2, (me // 8) % 2
    slot = pair * 2 + low
    batch = 5

    def flip(bit):
        digits = {1: low, 2: side, 4: pair, 8: far}
        place = me
        for one in (1, 2, 4, 8):
            if bit & one:
                place = place + one - 2 * one * digits[one]
        return (place, share)

    after, before = (lax.rem(me + 1, count), share), (lax.rem(me + count - 1, count), share)
    peers = [lax.rem(share + step, shares) for step in range(1, shares)]
    copies = []

    def bring(origin, target):
        copy = pltpu.make_async_copy(origin, target, local_sems.at[len(copies)])
        copy.start()
        copies.append(copy)
        return copy

    load_embed = bring(embed, values)
    load_cotangent = bring(cotangent, arrow)
    order = (1, 0, 2)
    loads = {at: bring((w_zero, w_one, w_two)[at], weights[at]) for at in order}

    barrier = pltpu.get_barrier_semaphore()
    others = [flip(bit) for bit in (1, 2, 4, 5, 8)] + [after, before]
    others += [(me, peer) for peer in peers]
    for other in others:
        pl.semaphore_signal(
            barrier, inc=1, device_id=other, device_id_type=pl.DeviceIdType.MESH
        )
    links = Links(sends, recvs)
    which = hot(table.shape[2], which_row[...])

    def turn(term, unused):
        rest, total = table[term], None
        for _ in range(3):
            part = rest.astype(bf16)
            rest = rest - part.astype(f32)
            value = product(part, which)
            total = value if total is None else total + value
        rot[term] = total
        return unused

    lax.fori_loop(0, terms, turn, 0, unroll=5)
    degrees = lax.broadcasted_iota(jnp.int32, (5, atoms), 0)
    for degree in range(5):
        gains[degree] = lax.dot_general(
            gain[...],
            (degrees == degree).astype(f32),
            (((0,), (0,)), ((), ())),
            precision=HIGHEST,
            preferred_element_type=f32,
        )
    to_target = hot(atoms, target_row[...])
    to_source = hot(atoms, source_row[...])
    to_halo = hot(2 * halo, source_row[...], atoms)
    faces = hot(atoms, face_row[...])
    square = lax.broadcasted_iota(jnp.int32, (2 * halo, 2 * halo), 0)
    unit = (square == lax.broadcasted_iota(jnp.int32, square.shape, 1)).astype(bf16)
    to_face = turned(unit, faces).astype(bf16)
    scale = weight_row[...]

    load_embed.wait()

    def squared(term, total):
        value = values[term].astype(f32)
        return total + value * value

    total = lax.fori_loop(0, terms, squared, jnp.zeros((width, atoms), f32))
    own_squares = jnp.sum(total, axis=0, keepdims=True)
    square_out[...] = jnp.broadcast_to(own_squares, square_out.shape)
    pl.semaphore_wait(barrier, len(others))
    summed = [
        links.start(square_out, square_in.at[index], (me, peer))
        for index, peer in enumerate(peers)
    ]

    def spread(values_ref, picks):
        def one(step, unused):
            some = pl.ds(step * batch, batch)
            value = values_ref[some].reshape(batch * width, atoms)
            work[some] = product(value, picks).reshape(batch, width, edges)
            return unused

        lax.fori_loop(0, terms // batch, one, 0)

    tall = min(32, width)

    def rotate(at, put):
        first, (blocks, parts) = FIRSTS[at], PARTS[at]

        def one(step, unused):
            rows = pl.ds(pl.multiple_of(step * tall, tall), tall)
            for degree in range(5):
                base = degree * degree
                members = [
                    row
                    for row in range(first, first + blocks * parts)
                    if FRAME[row][0] == degree
                ]
                if not members:
                    continue
                lines = [work[base + index, rows, :] for index in range(2 * degree + 1)]
                for row in members:
                    line = None
                    for index, entry in enumerate(lines):
                        term = rot[base + index, row : row + 1, :] * entry
                        line = term if line is None else line + term
                    part, block = divmod(row - first, blocks)
                    put(block, part, step * tall, line)
            return unused

        lax.fori_loop(0, width // tall, one, 0)

    load_cotangent.wait()
    spread(arrow, to_target)
    near = [None] * 3

    def near_send(at):
        spots = [
            grads[at].at[:, lanes((part * NEAR + slot) * edges, edges)]
            for part in range(PARTS[at][1])
        ]
        near[at] = [
            [links.start(spot, spot, flip(4)) for spot in spots],
            [links.start(spot, spot, flip(1)) for spot in spots],
        ]

    def frame_grad(at):
        def put_grad(block, part, start, line):
            rows = pl.ds(pl.multiple_of(block * width + start, tall), tall)
            grads[at][rows, lanes((part * NEAR + slot) * edges, edges)] = (line * scale).astype(bf16)

        rotate(at, put_grad)

    frame_grad(1)

    whole = own_squares
    for index, copy in enumerate(summed):
        copy.wait_recv()
        whole = whole + square_in[index, :1, :]
    inverse = lax.rsqrt(whole / (terms * channels) + EPSILON)
    for degree in range(5):

        def normal(term, unused):
            normed[term] = (values[term].astype(f32) * inverse * gains[degree]).astype(bf16)
            return unused

        lax.fori_loop(degree * degree, (degree + 1) * (degree + 1), normal, 0)

    def fold(picks, target):
        def one(step, unused):
            value = normed[pl.ds(step * batch, batch)].reshape(batch * width, atoms)
            value = turned(picks, value).astype(bf16).reshape(2, halo, batch * width)
            target[:, :, lanes(step * batch * width, batch * width)] = value
            return unused

        lax.fori_loop(0, terms // batch, one, 0)

    def unfold(origin, picks):
        def one(step, unused):
            some = pl.ds(step * batch, batch)
            value = origin[:, :, lanes(step * batch * width, batch * width)]
            value = across(value.reshape(2 * halo, batch * width), picks)
            work[some] += value.reshape(batch, width, atoms)
            return unused

        lax.fori_loop(0, terms // batch, one, 0)

    fold(to_face, face_out)
    halos = [
        links.start(face_out.at[1], face_in.at[0], after),
        links.start(face_out.at[0], face_in.at[1], before),
    ]

    near_send(1)
    frame_grad(0)
    frame_grad(2)
    for at in (1, 2):
        blocks = PARTS[at][0]
        height = blocks * width
        g = grads[at]
        plus = g[:, lanes(slot * edges, edges)]
        minus = g[:, lanes((NEAR + slot) * edges, edges)]
        doubled[at][:height, :edges] = plus
        doubled[at][:height, edges:] = minus
        doubled[at][height:, :edges] = minus
        doubled[at][height:, edges:] = -plus

    def backed(at, row, share_at):
        if at == 0:
            right = grads[0][:, lanes(slot * edges, edges)]
        else:
            right = doubled[at][...]
        left = weights[at][..., lanes(row * channels + share_at * width, width)]
        return across(left.reshape(-1, width), right)

    scattered = {at: [] for at in order}

    def back_leave(at, start, stop):
        if start == 0:
            loads[at].wait()
        for index, peer in enumerate(peers):

            def one(row, unused):
                back_out[at][index, row] = backed(at, row, peer).astype(bf16)
                return unused

            lax.fori_loop(start, stop, one, 0)

    def back_send(at, start, stop):
        rows = pl.ds(start, stop - start)
        scattered[at] += [
            links.start(back_out[at].at[index, rows], back_in[at].at[index, rows], (me, peer))
            for index, peer in enumerate(peers)
        ]

    def back_keep(at):
        first, (blocks, parts) = FIRSTS[at], PARTS[at]

        def one(row, unused):
            value = backed(at, row, share)
            for part in range(parts):
                back[first + part * blocks + row] = value[:, part * edges : (part + 1) * edges]
            return unused

        lax.fori_loop(0, blocks, one, 0)

    def relay(at):
        relays = []
        for part, copy in enumerate(near[at][0]):
            copy.wait_recv()
            spot = grads[at].at[:, lanes((part * NEAR + (1 - pair) * 2 + low) * edges, edges)]
            relays.append(links.start(spot, spot, flip(1)))
        near[at].append(relays)

    gathered = {}

    def share_frames(at, turn_at):
        blocks, parts = PARTS[at]
        size = (blocks + 1) // 2
        if turn_at == 0:
            start = (1 - far) * (blocks - size)
        else:
            start, size = far * size, blocks - size
        ours = frames[at].reshape(blocks, shares, width, parts * edges)
        ours = ours.at[pl.ds(start, size), share]
        gathered[at, turn_at] = [links.start(ours, ours, (me, peer)) for peer in peers]

    arrivals, passing, through = {}, {}, {}
    places = (1 - far, far)

    def scatter(at, turn_at, own):
        parts = PARTS[at][1]
        place = places[turn_at]
        short = nears[at].shape[2] // parts
        cut = frames[at].reshape(2, 2, 2, 2, short, parts * edges)
        one_side = share if own else 1 - share
        if not own:
            for copy in gathered[at, turn_at]:
                copy.wait_recv()
        waits = arrivals.setdefault((at, turn_at), [])
        for part in range(parts):
            spread_lanes = pl.ds(part * edges, edges)

            def here(first_slot, slots):
                start = (part * NEAR + first_slot) * edges
                return nears[at].at[
                    place, one_side, pl.ds(0, short), lanes(start, slots * edges)
                ]

            for bit in (4, 5, 1) if own else (1,):
                its_pair = 1 - pair if bit & 4 else pair
                its_low = 1 - low if bit & 1 else low
                piece = cut.at[place, its_pair, one_side, its_low, :, spread_lanes]
                copy = links.start(piece, here(slot, 1), flip(bit))
                if bit & 4:
                    passing.setdefault((at, turn_at, part), []).append(copy)
                else:
                    waits.append(copy.wait_recv)
            piece = cut.at[place, pair, one_side, low, :, spread_lanes]
            waits.append(bring(piece, here(slot, 1)).wait)
            if own:
                through[at, turn_at, part] = here((1 - pair) * 2, 2)

    def forward(at, turn_at):
        for part in range(PARTS[at][1]):
            for copy in passing[at, turn_at, part]:
                copy.wait_recv()
            spot = through[at, turn_at, part]
            arrivals[at, turn_at].append(links.start(spot, spot, (me, peers[0])).wait_recv)

    def scatter_both(at, turn_at):
        for copy in gathered[at, turn_at]:
            copy.wait_recv()
        parts = PARTS[at][1]
        place = places[turn_at]
        short = nears[at].shape[2] // parts
        cut = frames[at].reshape(2, 2, 2, 2, short, parts * edges)
        waits = []
        for part in range(parts):
            here = nears[at].at[
                place, :, pl.ds(0, short), lanes((part * NEAR + slot) * edges, edges)
            ]
            spread_lanes = pl.ds(part * edges, edges)
            for bit in (4, 5, 1):
                its_pair = 1 - pair if bit & 4 else pair
                its_low = 1 - low if bit & 1 else low
                piece = cut.at[place, its_pair, :, its_low, :, spread_lanes]
                waits.append(links.start(piece, here, flip(bit)).wait_recv)
            waits.append(bring(cut.at[place, pair, :, low, :, spread_lanes], here).wait)
        arrivals[at, turn_at] = waits

    def mix(at):
        first, (blocks, parts) = FIRSTS[at], PARTS[at]

        def one(row, unused):
            if parts == 1:
                work[first + row] = product(weights[at][row], frames[at][...])
            else:
                real = product(weights[at][0, row], frames[at][...])
                imag = product(weights[at][1, row], frames[at][...])
                work[first + row] = real[:, :edges] - imag[:, edges:]
                work[first + blocks + row] = real[:, edges:] + imag[:, :edges]
            return unused

        lax.fori_loop(0, blocks, one, 0)

    def grown(at, place, step, one_side):
        columns = nears[at][place, one_side]
        rows = grads[at][pl.ds(pl.multiple_of(step * width, width), width), :]
        return turned(rows, columns) if at == 1 else turned(columns, rows)

    aside = {}
    away = {}
    pieces = {1: ((0, 1), (1, 2), (2, 3), (3, 4)), 0: ((0, 3), (3, 5)), 2: ((0, 3),)}

    def grow_leave(at, turn_at):
        for arrive in arrivals[at, turn_at]:
            arrive()
        if turn_at == 0:
            for group in near[at][1:]:
                for copy in group:
                    copy.wait_recv()
        parts = PARTS[at][1]
        place = places[turn_at]
        f, span = nears[at], NEAR * edges
        short = f.shape[2] // parts
        if parts == 2:
            for one_side in range(2):
                f[place, one_side, short:, :span] = -f[place, one_side, :short, span:]
                f[place, one_side, short:, span:] = f[place, one_side, :short, :span]

        def leave(step, unused):
            leaving[at][place, step] = grown(at, place, step, 1 - side).astype(bf16)
            return unused

        for index, (start, stop) in enumerate(pieces[at]):
            lax.fori_loop(start, stop, leave, 0)
            steps = pl.ds(start, stop - start)
            aside[at, turn_at, index] = links.start(
                leaving[at].at[place, steps], arriving[at].at[place, steps], flip(2)
            )

    def grow_keep(at, turn_at):
        place = places[turn_at]

        def stay(step, unused):
            kept[at][place, step] = grown(at, place, step, side)
            return unused

        lax.fori_loop(0, PARTS[at][0], stay, 0)

    def pass_on(at, index):
        start, stop = pieces[at][index]
        aside[at, 0, index].wait_recv()
        links.settle(aside[at, 0, index])
        place = places[0]

        def one(step, unused):
            total = kept[at][place, step] + arriving[at][place, step].astype(f32)
            leaving[at][place, step] = total.astype(bf16)
            return unused

        lax.fori_loop(start, stop, one, 0)
        steps = pl.ds(start, stop - start)
        away[at, index] = links.start(
            leaving[at].at[place, steps], final[at].at[steps], flip(8)
        )

    back_leave(1, 0, 2)
    back_send(1, 0, 2)
    spread(normed, to_source)
    back_leave(1, 2, 4)
    for copy in halos:
        copy.wait_recv()
    unfold(face_in, to_halo)
    for at in order:
        blocks, _ = PARTS[at]

        def put_frame(block, part, start, line):
            rows = pl.ds(pl.multiple_of(block * channels + share * width + start, tall), tall)
            frames[at][rows, part * edges : (part + 1) * edges] = line.astype(bf16)

        rotate(at, put_frame)
        if at == 1:
            share_frames(1, 0)
            scatter(1, 0, True)
            scatter(1, 1, True)

    def unturn(origin, factor, put):
        def one(step, unused):
            rows = pl.ds(pl.multiple_of(step * tall, tall), tall)
            for degree in range(5):
                members = [row for row, entry in enumerate(FRAME) if entry[0] == degree]
                lines = [origin[row, rows, :] for row in members]
                if factor is not None:
                    lines = [line * factor for line in lines]
                for column in range(degree * degree, (degree + 1) * (degree + 1)):
                    value = None
                    for row, line in zip(members, lines):
                        term = rot[column, row : row + 1, :] * line
                        value = term if value is None else value + term
                    put(column, rows, value)
            return unused

        lax.fori_loop(0, width // tall, one, 0)

    def put_normed(column, rows, value):
        normed[column, rows, :] = value.astype(bf16)

    def gather(picks, target):
        def one(step, unused):
            some = pl.ds(step * batch, batch)
            value = turned(normed[some].reshape(batch * width, edges), picks)
            target[some] = value.reshape(batch, width, atoms).astype(target.dtype)
            return unused

        lax.fori_loop(0, terms // batch, one, 0)

    def back_add():
        for at in order:
            first, (blocks, parts) = FIRSTS[at], PARTS[at]
            for copy in scattered[at]:
                copy.wait_recv()
            for index in range(shares - 1):

                def add(row, unused):
                    arrived = back_in[at][index, row].astype(f32)
                    for part in range(parts):
                        back[first + part * blocks + row] += arrived[
                            :, part * edges : (part + 1) * edges
                        ]
                    return unused

                lax.fori_loop(0, blocks, add, 0)

    share_frames(0, 0)
    near_send(0)
    back_leave(0, 0, 5)
    back_leave(2, 0, 3)
    relay(1)
    forward(1, 0)
    scatter(1, 0, False)
    share_frames(2, 0)
    share_frames(1, 1)
    forward(1, 1)
    share_frames(0, 1)
    share_frames(2, 1)
    scatter_both(0, 0)
    near_send(2)
    grow_leave(1, 0)
    grow_keep(1, 0)
    back_send(1, 2, 4)
    back_send(0, 0, 5)
    scatter_both(2, 0)
    pass_on(1, 0)
    back_keep(1)
    pass_on(1, 1)
    back_keep(0)
    pass_on(1, 2)
    pass_on(1, 3)
    scatter(1, 1, False)
    relay(0)
    back_send(2, 0, 3)
    grow_leave(0, 0)
    grow_keep(0, 0)
    scatter_both(0, 1)
    back_keep(2)
    scatter_both(2, 1)
    grow_leave(1, 1)
    grow_keep(1, 1)
    mix(1)
    pass_on(0, 0)
    pass_on(0, 1)
    mix(0)
    relay(2)
    mix(2)
    unturn(work, scale, put_normed)
    gather(to_target, arrow)
    stored = [bring(arrow, update)]
    grow_leave(2, 0)
    grow_keep(2, 0)
    back_add()
    unturn(back, None, put_normed)
    fold(to_halo, ends_out)
    ends = [
        links.start(ends_out.at[1], ends_in.at[0], after),
        links.start(ends_out.at[0], ends_in.at[1], before),
    ]
    grow_leave(0, 1)
    pass_on(2, 0)
    grow_leave(2, 1)
    gather(to_source, work)
    grow_keep(0, 1)
    grow_keep(2, 1)
    for copy in ends:
        copy.wait_recv()
    unfold(ends_in, to_face)
    total = jnp.zeros((width, atoms), f32)
    for degree in range(5):

        def scaled(term, total):
            result = work[term] * inverse * gains[degree]
            work[term] = result
            return total + result * values[term].astype(f32)

        total = lax.fori_loop(degree * degree, (degree + 1) * (degree + 1), scaled, total)
    whole = jnp.sum(total, axis=0, keepdims=True)
    tally_out[...] = jnp.broadcast_to(whole, tally_out.shape)
    tallies = [
        links.start(tally_out, tally_in.at[index], (me, peer))
        for index, peer in enumerate(peers)
    ]
    for index, copy in enumerate(tallies):
        copy.wait_recv()
        whole = whole + tally_in[index, :1, :]
    factor = inverse * inverse * whole / (terms * channels)

    def finished(term, unused):
        normed[term] = (work[term] - values[term].astype(f32) * factor).astype(bf16)
        return unused

    lax.fori_loop(0, terms, finished, 0)
    stored.append(bring(normed, grad_embed))
    for at in order:
        for index in range(len(pieces[at])):
            aside[at, 1, index].wait_recv()
            away[at, index].wait_recv()

        def settled(step, unused):
            total = kept[at][far, step] + arriving[at][far, step].astype(f32)
            kept[at][far, step] = total + final[at][step].astype(f32)
            return unused

        lax.fori_loop(0, PARTS[at][0], settled, 0)
        ready = kept[at].at[far]
        if at == 0:
            stored.append(bring(ready, outs[at]))
        else:
            for part in range(2):
                short = outs[at].shape[-1 if at == 1 else -2]
                some = pl.ds(part * short, short)
                piece = ready.at[:, :, some] if at == 1 else ready.at[:, some]
                stored.append(bring(piece, outs[at].at[part]))
    links.finish()
    for copy in stored:
        copy.wait()


def run_layer(arrays, sizes):
    embed, w_zero, w_one, w_two = arrays[0], arrays[3], arrays[4], arrays[5]
    shares, count = sizes
    terms, width, atoms = embed.shape
    edges, halo = arrays[8].shape[1], arrays[7].shape[1] // 2
    channels = width * shares
    cuts = (w_zero.shape[2] // count, w_one.shape[3] // count, w_two.shape[3] // count)
    bf16, f32 = jnp.bfloat16, jnp.float32
    three = range(3)
    tall = [blocks * width for blocks, parts in PARTS]
    wide = [parts * cut for (blocks, parts), cut in zip(PARTS, cuts)]
    near = [NEAR * parts * edges for blocks, parts in PARTS]
    scratch = [(w.shape, bf16) for w in (w_zero, w_one, w_two)]
    scratch += [((blocks * channels, parts * edges), bf16) for blocks, parts in PARTS]
    scratch += [((tall[i], near[i]), bf16) for i in three]
    scratch += [((2 * tall[i], 2 * edges), bf16) for i in (1, 2)]
    scratch += [((2, 2, wide[i], near[i]), bf16) for i in three]
    scratch += 2 * [
        ((shares - 1, blocks, width, parts * edges), bf16) for blocks, parts in PARTS
    ]
    slabs = [
        (5, wide[0], width),
        (4, width, wide[1]),
        (3, wide[2], width),
    ]
    scratch += [((2,) + slab, f32) for slab in slabs]
    scratch += 2 * [((2,) + slab, bf16) for slab in slabs]
    scratch += [(slab, bf16) for slab in slabs]
    scratch += [
        ((terms, width, edges), f32),
        ((len(FRAME), width, edges), f32),
        ((terms, width, atoms), bf16),
        ((terms, width, atoms), bf16),
        ((terms, width, atoms), bf16),
        ((terms, len(FRAME), edges), f32),
        ((5, width, atoms), f32),
    ]
    scratch += 4 * [((2, halo, terms * width), bf16)]
    scratch += 2 * [((8, atoms), f32), ((shares - 1, 8, atoms), f32)]
    number = 16 * (shares - 1) + 15 + 50 + 24 + 4
    anywhere = pl.BlockSpec(memory_space=pl.ANY)
    inside = pl.BlockSpec(memory_space=pltpu.VMEM)
    return pl.pallas_call(
        functools.partial(layer_kernel, shares, count),
        in_specs=[anywhere] * 2 + [inside] + [anywhere] * 3 + [inside] * 6,
        out_specs=[anywhere] * 5,
        out_shape=[jax.ShapeDtypeStruct(embed.shape, bf16)] * 2
        + [
            jax.ShapeDtypeStruct((5, cuts[0], width), f32),
            jax.ShapeDtypeStruct((2, 4, width, cuts[1]), f32),
            jax.ShapeDtypeStruct((2, 3, cuts[2], width), f32),
        ],
        scratch_shapes=[pltpu.VMEM(shape, kind) for shape, kind in scratch]
        + [
            pltpu.SemaphoreType.DMA((number,)),
            pltpu.SemaphoreType.DMA((number,)),
            pltpu.SemaphoreType.DMA((48,)),
        ],
        compiler_params=pltpu.CompilerParams(
            collective_id=0, has_side_effects=True, vmem_limit_bytes=67043328
        ),
    )(*arrays)


def carry_kernel(*refs):
    count = (len(refs) - 1) // 3
    sems = refs[-1]
    origins, targets, held = refs[:count], refs[count : 2 * count], refs[2 * count : 3 * count]
    reads = [
        pltpu.make_async_copy(origin, here, sems.at[0, index])
        for index, (origin, here) in enumerate(zip(origins, held))
    ]
    writes = [
        pltpu.make_async_copy(here, target, sems.at[1, index])
        for index, (here, target) in enumerate(zip(held, targets))
    ]
    for read in reads:
        read.start()
    for read, write in zip(reads, writes):
        read.wait()
        write.start()
    for write in writes:
        write.wait()


def carry_out(arrays):
    anywhere = [pl.BlockSpec(memory_space=pl.ANY)] * len(arrays)
    return pl.pallas_call(
        carry_kernel,
        in_specs=anywhere,
        out_specs=anywhere,
        out_shape=[jax.ShapeDtypeStruct(array.shape, array.dtype) for array in arrays],
        scratch_shapes=[pltpu.VMEM(array.shape, array.dtype) for array in arrays]
        + [pltpu.SemaphoreType.DMA((2, len(arrays)))],
        compiler_params=pltpu.CompilerParams(vmem_limit_bytes=67043328),
    )(*arrays)


def shards(
    embed,
    gain,
    w_zero,
    w_one,
    w_two,
    rot_table,
    face_atoms,
    edge_source,
    edge_target,
    rot_index,
    edge_weight,
    cotangent,
):
    atoms = embed.shape[2]
    local = embed.shape[1]
    halo = face_atoms.shape[0] // 2
    shares = lax.axis_size("chan")
    channels = local * shares
    weights = (w_zero, w_one, w_two)
    values = embed.astype(jnp.float32)
    gains = gain_rows(gain)
    rows, coefficients, rots = rot_table.shape
    which = (jnp.arange(rots, dtype=jnp.int32)[:, None] == rot_index[None, :]).astype(jnp.float32)
    rotations = jnp.dot(
        rot_table.reshape(rows * coefficients, rots),
        which,
        precision=HIGHEST,
        preferred_element_type=jnp.float32,
    )
    weight_row = edge_weight[None, :]
    ones = jnp.ones_like(weight_row)

    squares = lax.psum(jnp.sum(values * values, axis=(0, 1)), "chan")
    inverse = lax.rsqrt(squares / (25 * channels) + EPSILON)
    normed = (values * inverse[None, None, :] * gains[:, :, None]).astype(jnp.bfloat16)
    flat = normed.reshape(25 * local, atoms)
    faces = product(flat, hot_rows(atoms, face_atoms)).astype(jnp.bfloat16)
    table_end = from_beside(faces.reshape(25, local, 2 * halo), halo)

    grads = to_frames([(cotangent, hot_rows(atoms, edge_target))], rotations, weight_row)
    picks = hot_rows(atoms + 2 * halo, edge_source)
    own = to_frames([(normed, picks[:atoms]), (table_end, picks[atoms:])], rotations, ones)
    own, grads = lax.optimization_barrier((own, grads))
    piece = lax.all_gather(own, "chan", axis=1, tiled=True)

    grads_side = swap(grads, 2)
    pair = swap(jnp.stack([grads, grads_side]), 1)
    grads_all = [grads, grads_side, pair[0], pair[1]]

    back = lax.psum_scatter(
        mix_back(weights, grads, shares), "chan", scatter_dimension=0, tiled=False
    )
    frames, widths = column_frames(piece)
    mixed = mix_forward(weights, piece)
    mixed, frames = lax.optimization_barrier((mixed, frames))
    (update,) = to_atoms(
        mixed, rotations, weight_row, [hot_columns(edge_target, atoms)], [jnp.bfloat16]
    )
    leaving = hot_columns(edge_source, atoms + 2 * halo)
    mine, outward = to_atoms(
        back,
        rotations,
        ones,
        [leaving[:, :atoms], leaving[:, atoms:]],
        [jnp.float32, jnp.bfloat16],
    )
    incoming = from_beside(outward, halo)
    settled = product(incoming.reshape(25 * local, 2 * halo), hot_columns(face_atoms, atoms))
    grad_normed = mine + settled.reshape(25, local, atoms)
    scaled = inverse[None, None, :] * gains[:, :, None] * grad_normed
    tally = lax.psum(jnp.sum(values * scaled, axis=(0, 1)), "chan")
    grad_embed = (
        scaled
        - values * (inverse**2 * tally / (25 * channels))[None, None, :]
    ).astype(jnp.bfloat16)
    grad_zero, grad_one, grad_two = weight_grads(frames, widths, grads_all, local)
    return (update, grad_embed, grad_zero, grad_one, grad_two)


def shards_linked(
    embed,
    gain,
    w_zero,
    w_one,
    w_two,
    rot_table,
    face_atoms,
    edge_source,
    edge_target,
    rot_index,
    edge_weight,
    cotangent,
):
    arrays = (
        embed,
        cotangent,
        gain,
        w_zero,
        w_one,
        w_two,
        jnp.transpose(rot_table, (1, 0, 2)),
        face_atoms[None, :],
        edge_source[None, :],
        edge_target[None, :],
        rot_index[None, :],
        edge_weight[None, :],
    )
    sizes = (lax.axis_size("chan"), lax.axis_size("graph"))
    update, grad_embed, done_zero, done_one, done_two = carry_out(run_layer(arrays, sizes))
    grad_zero = jnp.transpose(done_zero, (0, 2, 1))
    grad_two = jnp.transpose(done_two, (0, 1, 3, 2))
    return (update, grad_embed, grad_zero, done_one, grad_two)


def solution(mesh):
    placed = (
        P(None, "chan", "graph"),
        P(None, "chan"),
        P(None, "chan", None),
        P(None, None, "chan", None),
        P(None, None, "chan", None),
        P(),
        P("graph"),
        P("graph"),
        P("graph"),
        P("graph"),
        P("graph"),
        P(None, "chan", "graph"),
    )
    linked = mesh.shape["graph"] == 16 and mesh.shape["chan"] == 2
    return jax.shard_map(
        shards_linked if linked else shards,
        mesh=mesh,
        in_specs=placed,
        out_specs=(
            P(None, "chan", "graph"),
            P(None, "chan", "graph"),
            P(None, "chan", "graph"),
            P(None, None, "chan", "graph"),
            P(None, None, "chan", "graph"),
        ),
        check_vma=False,
    )
```

```python
import functools

import jax
import jax.numpy as jnp
from jax import lax
from jax.experimental import pallas as pl
from jax.experimental.pallas import tpu as pltpu
from jax.sharding import PartitionSpec as P


EPSILON = 1e-06
HIGHEST = lax.Precision.HIGHEST
FRAME = (
    (0, 0),
    (1, 0),
    (2, 0),
    (3, 0),
    (4, 0),
    (1, 1),
    (2, 1),
    (3, 1),
    (4, 1),
    (1, -1),
    (2, -1),
    (3, -1),
    (4, -1),
    (2, 2),
    (3, 2),
    (4, 2),
    (2, -2),
    (3, -2),
    (4, -2),
)


def gain_rows(gain):
    pieces = [
        jnp.broadcast_to(gain[degree : degree + 1], (2 * degree + 1, gain.shape[1]))
        for degree in range(5)
    ]
    return jnp.concatenate(pieces, axis=0)


def product(left, right):
    return jnp.dot(left, right, preferred_element_type=jnp.float32)


def across(left, right):
    return lax.dot_general(
        left, right, (((0,), (0,)), ((), ())), preferred_element_type=jnp.float32
    )


def contract(left, right):
    return lax.dot_general(left, right, (((2,), (1,)), ((), ())), preferred_element_type=jnp.float32)


def frames_kernel(*refs):
    pairs, (rotations, scale, out) = refs[:-3], refs[-3:]
    count, width = pairs[0].shape[0], pairs[0].shape[1]
    total = None
    for values, picks in zip(pairs[0::2], pairs[1::2]):
        part = product(values[...].reshape(count * width, values.shape[2]), picks[...])
        total = part if total is None else total + part
    total = total.reshape(count, width, total.shape[1])
    for row, (degree, _) in enumerate(FRAME):
        first = degree * degree
        entry = row * count + first
        line = rotations[entry : entry + 1, :] * total[first]
        for step in range(1, 2 * degree + 1):
            entry = row * count + first + step
            line = line + rotations[entry : entry + 1, :] * total[first + step]
        out[row] = (line * scale[...]).astype(out.dtype)


def to_frames(pairs, rotations, scale):
    count, local = pairs[0][0].shape[0], pairs[0][0].shape[1]
    edges = scale.shape[1]
    block = min(64, local)
    operands, specs = [], []
    for values, picks in pairs:
        operands += [values, picks]
        specs.append(pl.BlockSpec((count, block, values.shape[2]), lambda i: (0, i, 0)))
        specs.append(pl.BlockSpec(picks.shape, lambda i: (0, 0)))
    for whole in (rotations, scale):
        operands.append(whole)
        specs.append(pl.BlockSpec(whole.shape, lambda i: (0, 0)))
    return pl.pallas_call(
        frames_kernel,
        grid=(local // block,),
        in_specs=specs,
        out_specs=pl.BlockSpec((len(FRAME), block, edges), lambda i: (0, i, 0)),
        out_shape=jax.ShapeDtypeStruct((len(FRAME), local, edges), jnp.bfloat16),
        compiler_params=pltpu.CompilerParams(dimension_semantics=("arbitrary",)),
    )(*operands)


def atoms_kernel(count, values, rotations, scale, *refs):
    picks, outs, held = refs[: len(refs) // 2], refs[len(refs) // 2 : -1], refs[-1]
    width, edges = values.shape[1], values.shape[2]
    for degree in range(5):
        members = [row for row, pair in enumerate(FRAME) if pair[0] == degree]
        lines = [values[row].astype(jnp.float32) * scale[...] for row in members]
        for column in range(degree * degree, (degree + 1) * (degree + 1)):
            total = None
            for row, line in zip(members, lines):
                entry = row * count + column
                term = rotations[entry : entry + 1, :] * line
                total = term if total is None else total + term
            held[column] = total.astype(held.dtype)
    flat = held[...].reshape(count * width, edges)
    for pick, out in zip(picks, outs):
        out[...] = product(flat, pick[...]).reshape(out.shape).astype(out.dtype)


def to_atoms(values, rotations, scale, picks, kinds):
    rows, local, edges = values.shape
    count = rotations.shape[0] // rows
    block = min(64, local)
    whole = lambda i: (0, 0)
    return pl.pallas_call(
        functools.partial(atoms_kernel, count),
        grid=(local // block,),
        in_specs=[
            pl.BlockSpec((rows, block, edges), lambda i: (0, i, 0)),
            pl.BlockSpec(rotations.shape, whole),
            pl.BlockSpec(scale.shape, whole),
        ]
        + [pl.BlockSpec(pick.shape, whole) for pick in picks],
        out_specs=[
            pl.BlockSpec((count, block, pick.shape[1]), lambda i: (0, i, 0)) for pick in picks
        ],
        out_shape=[
            jax.ShapeDtypeStruct((count, local, pick.shape[1]), kind)
            for pick, kind in zip(picks, kinds)
        ],
        scratch_shapes=[pltpu.VMEM((count, block, edges), jnp.bfloat16)],
        compiler_params=pltpu.CompilerParams(dimension_semantics=("arbitrary",)),
    )(values, rotations, scale, *picks)


def swap(block, bit):
    count = lax.axis_size("graph")
    return lax.ppermute(block, "graph", [(i, i ^ bit) for i in range(count)])


def from_beside(faces, width):
    count = lax.axis_size("graph")
    forward = [(i, (i + 1) % count) for i in range(count)]
    backward = [(target, source) for source, target in forward]
    low = lax.ppermute(faces[:, :, width:], "graph", forward)
    high = lax.ppermute(faces[:, :, :width], "graph", backward)
    return jnp.concatenate([low, high], axis=2)


def hot_rows(size, codes):
    return (jnp.arange(size, dtype=jnp.int32)[:, None] == codes[None, :]).astype(jnp.bfloat16)


def hot_columns(codes, size):
    return (codes[:, None] == jnp.arange(size, dtype=jnp.int32)[None, :]).astype(jnp.bfloat16)


def beside(plus, minus, axis=-1):
    return jnp.concatenate([plus, minus], axis=axis)


def mix_forward(weights, frame):
    w_zero, w_one, w_two = weights
    edges = frame.shape[2]
    local = w_zero.shape[1]
    mixed = [
        product(w_zero.reshape(-1, w_zero.shape[2]), frame[:5].reshape(-1, edges)).reshape(
            5, local, edges
        )
    ]
    for weight, first, blocks in ((w_one, 5, 4), (w_two, 13, 3)):
        plus = frame[first : first + blocks].reshape(-1, edges)
        minus = frame[first + blocks : first + 2 * blocks].reshape(-1, edges)
        both = product(weight.reshape(-1, weight.shape[-1]), beside(plus, minus))
        both = both.reshape(2, blocks, local, 2 * edges)
        mixed.append(both[0, :, :, :edges] - both[1, :, :, edges:])
        mixed.append(both[0, :, :, edges:] + both[1, :, :, :edges])
    return jnp.concatenate(mixed, axis=0)


def mix_back(weights, grads, shares):
    w_zero, w_one, w_two = weights
    edges = grads.shape[2]

    def shared(block, blocks):
        shaped = block.reshape(blocks, shares, -1, edges).astype(jnp.bfloat16)
        return jnp.transpose(shaped, (1, 0, 2, 3))

    back = [
        shared(across(w_zero.reshape(-1, w_zero.shape[2]), grads[:5].reshape(-1, edges)), 5)
    ]
    for weight, first, blocks in ((w_one, 5, 4), (w_two, 13, 3)):
        plus = grads[first : first + blocks].reshape(-1, edges)
        minus = grads[first + blocks : first + 2 * blocks].reshape(-1, edges)
        sides = jnp.concatenate([beside(plus, minus), beside(minus, -plus)], axis=0)
        both = across(weight.reshape(-1, weight.shape[-1]), sides)
        back.append(shared(both[:, :edges], blocks))
        back.append(shared(both[:, edges:], blocks))
    return jnp.concatenate(back, axis=1)


def column_frames(frame):
    count = lax.axis_size("graph")
    near = 4
    far = count // near
    edges = frame.shape[2]
    cuts = ((0, 5), (5, 4), (9, 4), (13, 3), (16, 3))
    parts = [
        frame[first : first + blocks].reshape(far, near, -1, edges) for first, blocks in cuts
    ]
    widths = [part.shape[2] for part in parts]
    packed = jnp.concatenate(parts, axis=2)
    mine = lax.axis_index("graph") % near
    frames = []
    for bit in (0, 2, 1, 3):
        target = mine ^ bit
        chunk = lax.dynamic_index_in_dim(packed, target, axis=1, keepdims=False)
        frames.append(swap(chunk, bit) if bit else chunk)
    return frames, widths


def weight_grads(frames, widths, grads_all, local):
    count = lax.axis_size("graph")
    near = 4
    far = count // near
    edges = frames[0].shape[2]
    starts = [sum(widths[:i]) for i in range(5)]
    groups = [[z * near + q for z in range(far)] for q in range(near)]

    def settle(partial):
        return lax.psum_scatter(
            partial.astype(jnp.bfloat16),
            "graph",
            scatter_dimension=0,
            axis_index_groups=groups,
            tiled=False,
        ).astype(jnp.float32)

    def settle_direct(partial):
        partial = partial.astype(jnp.bfloat16)
        place = lax.axis_index("graph") // near
        total = lax.dynamic_index_in_dim(partial, place, axis=0, keepdims=False)
        total = total.astype(jnp.float32)
        for step in range(1, far):
            chunk = lax.dynamic_index_in_dim(partial, (place + step) % far, axis=0, keepdims=False)
            shift = [(i, (i + step * near) % count) for i in range(count)]
            total = total + lax.ppermute(chunk, "graph", shift).astype(jnp.float32)
        return total

    def columns(index):
        return [chunk[:, starts[index] : starts[index] + widths[index]] for chunk in frames]

    left = jnp.concatenate(columns(0), axis=2)
    right = jnp.concatenate([g[:5].reshape(-1, edges) for g in grads_all], axis=1)
    done = settle_direct(contract(left, right))
    results = [jnp.transpose(done).reshape(5, local, widths[0])]
    for index, first, blocks in ((1, 5, 4), (3, 13, 3)):
        plus, minus = columns(index), columns(index + 1)
        real_part = jnp.concatenate([x for pair in zip(plus, minus) for x in pair], axis=2)
        imag_part = jnp.concatenate([x for pair in zip(minus, plus) for x in (-pair[0], pair[1])], axis=2)
        left = jnp.concatenate([real_part, imag_part], axis=1)
        right = jnp.concatenate(
            [
                g[start : start + blocks].reshape(-1, edges)
                for g in grads_all
                for start in (first, first + blocks)
            ],
            axis=1,
        )
        done = settle(contract(left, right))
        done = done.reshape(2, widths[index], blocks * local)
        results.append(jnp.transpose(done, (0, 2, 1)).reshape(2, blocks, local, widths[index]))
    return results


NEAR = 4
PARTS = ((5, 1), (4, 2), (3, 2))
FIRSTS = (0, 5, 13)


def lanes(start, size):
    return pl.ds(pl.multiple_of(start, 128), size)


def turned(left, right):
    return lax.dot_general(
        left, right, (((1,), (1,)), ((), ())), preferred_element_type=jnp.float32
    )


def hot(size, codes, first=0):
    places = lax.broadcasted_iota(jnp.int32, (size, codes.shape[1]), 0) + first
    return (places == codes).astype(jnp.bfloat16)


class Links:
    def __init__(self, sends, recvs):
        self.sends, self.recvs, self.count, self.started = sends, recvs, 0, []

    def start(self, source, target, device):
        index = self.count
        self.count += 1
        copy = pltpu.make_async_remote_copy(
            src_ref=source,
            dst_ref=target,
            send_sem=self.sends.at[index],
            recv_sem=self.recvs.at[index],
            device_id=device,
            device_id_type=pl.DeviceIdType.MESH,
        )
        copy.start()
        self.started.append(copy)
        return copy

    def settle(self, copy):
        copy.wait_send()
        self.started = [one for one in self.started if one is not copy]

    def finish(self):
        for copy in self.started:
            copy.wait_send()


def layer_kernel(shares, count, *refs):
    (embed, cotangent, gain, w_zero, w_one, w_two, table_home) = refs[:7]
    (face_row, source_row, target_row, which_row, weight_row) = refs[7:12]
    (update, grad_embed, out_zero, out_one, out_two) = refs[12:17]
    weights = refs[17:20]
    frames = refs[20:23]
    grads = refs[23:26]
    doubled = (None,) + tuple(refs[26:28])
    nears = refs[28:31]
    back_out, back_in = refs[31:34], refs[34:37]
    kept, leaving, arriving, final = refs[37:40], refs[40:43], refs[43:46], refs[46:49]
    (work, back, arrow, values, normed, rot, gains) = refs[49:56]
    (face_out, face_in, ends_out, ends_in) = refs[56:60]
    (square_out, square_in, tally_out, tally_in) = refs[60:64]
    table = refs[64]
    sends, recvs, local_sems = refs[65:68]
    outs = (out_zero, out_one, out_two)
    f32, bf16 = jnp.float32, jnp.bfloat16
    terms, width, atoms = values.shape
    edges = source_row.shape[1]
    halo = face_row.shape[1] // 2
    channels = width * shares
    me = lax.axis_index("graph")
    share = lax.axis_index("chan")
    low, side, pair, far = me % 2, (me // 2) % 2, (me // 4) % 2, (me // 8) % 2
    slot = pair * 2 + low
    batch = 5

    def flip(bit):
        digits = {1: low, 2: side, 4: pair, 8: far}
        place = me
        for one in (1, 2, 4, 8):
            if bit & one:
                place = place + one - 2 * one * digits[one]
        return (place, share)

    after, before = (lax.rem(me + 1, count), share), (lax.rem(me + count - 1, count), share)
    peers = [lax.rem(share + step, shares) for step in range(1, shares)]
    copies = []

    def bring(origin, target):
        copy = pltpu.make_async_copy(origin, target, local_sems.at[len(copies)])
        copy.start()
        copies.append(copy)
        return copy

    load_table = bring(table_home, table)
    load_embed = bring(embed, values)
    load_cotangent = bring(cotangent, arrow)
    order = (1, 0, 2)
    loads = {at: bring((w_zero, w_one, w_two)[at], weights[at]) for at in order}

    barrier = pltpu.get_barrier_semaphore()
    others = [flip(bit) for bit in (1, 2, 4, 5, 8)] + [after, before]
    others += [(me, peer) for peer in peers]
    for other in others:
        pl.semaphore_signal(
            barrier, inc=1, device_id=other, device_id_type=pl.DeviceIdType.MESH
        )
    links = Links(sends, recvs)
    which = hot(table.shape[2], which_row[...])
    load_table.wait()

    def turn(term, unused):
        rest, total = table[term], None
        for _ in range(3):
            part = rest.astype(bf16)
            rest = rest - part.astype(f32)
            value = product(part, which)
            total = value if total is None else total + value
        rot[term] = total
        return unused

    lax.fori_loop(0, terms, turn, 0, unroll=5)
    degrees = lax.broadcasted_iota(jnp.int32, (5, atoms), 0)
    for degree in range(5):
        gains[degree] = lax.dot_general(
            gain[...],
            (degrees == degree).astype(f32),
            (((0,), (0,)), ((), ())),
            precision=HIGHEST,
            preferred_element_type=f32,
        )
    to_target = hot(atoms, target_row[...])
    to_source = hot(atoms, source_row[...])
    to_halo = hot(2 * halo, source_row[...], atoms)
    faces = hot(atoms, face_row[...])
    square = lax.broadcasted_iota(jnp.int32, (2 * halo, 2 * halo), 0)
    unit = (square == lax.broadcasted_iota(jnp.int32, square.shape, 1)).astype(bf16)
    to_face = turned(unit, faces).astype(bf16)
    scale = weight_row[...]

    load_embed.wait()

    def squared(term, total):
        value = values[term].astype(f32)
        return total + value * value

    total = lax.fori_loop(0, terms, squared, jnp.zeros((width, atoms), f32))
    own_squares = jnp.sum(total, axis=0, keepdims=True)
    square_out[...] = jnp.broadcast_to(own_squares, square_out.shape)
    pl.semaphore_wait(barrier, len(others))
    summed = [
        links.start(square_out, square_in.at[index], (me, peer))
        for index, peer in enumerate(peers)
    ]

    def spread(values_ref, picks):
        def one(step, unused):
            some = pl.ds(step * batch, batch)
            value = values_ref[some].reshape(batch * width, atoms)
            work[some] = product(value, picks).reshape(batch, width, edges)
            return unused

        lax.fori_loop(0, terms // batch, one, 0)

    tall = min(32, width)

    def rotate(at, put):
        first, (blocks, parts) = FIRSTS[at], PARTS[at]

        def one(step, unused):
            rows = pl.ds(pl.multiple_of(step * tall, tall), tall)
            for degree in range(5):
                base = degree * degree
                members = [
                    row
                    for row in range(first, first + blocks * parts)
                    if FRAME[row][0] == degree
                ]
                if not members:
                    continue
                lines = [work[base + index, rows, :] for index in range(2 * degree + 1)]
                for row in members:
                    line = None
                    for index, entry in enumerate(lines):
                        term = rot[base + index, row : row + 1, :] * entry
                        line = term if line is None else line + term
                    part, block = divmod(row - first, blocks)
                    put(block, part, step * tall, line)
            return unused

        lax.fori_loop(0, width // tall, one, 0)

    load_cotangent.wait()
    spread(arrow, to_target)
    near = [None] * 3

    def near_send(at):
        spots = [
            grads[at].at[:, lanes((part * NEAR + slot) * edges, edges)]
            for part in range(PARTS[at][1])
        ]
        near[at] = [
            [links.start(spot, spot, flip(4)) for spot in spots],
            [links.start(spot, spot, flip(1)) for spot in spots],
        ]

    def frame_grad(at):
        def put_grad(block, part, start, line):
            rows = pl.ds(pl.multiple_of(block * width + start, tall), tall)
            grads[at][rows, lanes((part * NEAR + slot) * edges, edges)] = (line * scale).astype(bf16)

        rotate(at, put_grad)

    frame_grad(1)

    whole = own_squares
    for index, copy in enumerate(summed):
        copy.wait_recv()
        whole = whole + square_in[index, :1, :]
    inverse = lax.rsqrt(whole / (terms * channels) + EPSILON)
    for degree in range(5):

        def normal(term, unused):
            normed[term] = (values[term].astype(f32) * inverse * gains[degree]).astype(bf16)
            return unused

        lax.fori_loop(degree * degree, (degree + 1) * (degree + 1), normal, 0)

    def fold(picks, target):
        def one(step, unused):
            value = normed[pl.ds(step * batch, batch)].reshape(batch * width, atoms)
            value = turned(picks, value).astype(bf16).reshape(2, halo, batch * width)
            target[:, :, lanes(step * batch * width, batch * width)] = value
            return unused

        lax.fori_loop(0, terms // batch, one, 0)

    def unfold(origin, picks):
        def one(step, unused):
            some = pl.ds(step * batch, batch)
            value = origin[:, :, lanes(step * batch * width, batch * width)]
            value = across(value.reshape(2 * halo, batch * width), picks)
            work[some] += value.reshape(batch, width, atoms)
            return unused

        lax.fori_loop(0, terms // batch, one, 0)

    fold(to_face, face_out)
    halos = [
        links.start(face_out.at[1], face_in.at[0], after),
        links.start(face_out.at[0], face_in.at[1], before),
    ]

    near_send(1)
    frame_grad(0)
    frame_grad(2)
    for at in (1, 2):
        blocks = PARTS[at][0]
        height = blocks * width
        g = grads[at]
        plus = g[:, lanes(slot * edges, edges)]
        minus = g[:, lanes((NEAR + slot) * edges, edges)]
        doubled[at][:height, :edges] = plus
        doubled[at][:height, edges:] = minus
        doubled[at][height:, :edges] = minus
        doubled[at][height:, edges:] = -plus

    def backed(at, row, share_at):
        if at == 0:
            right = grads[0][:, lanes(slot * edges, edges)]
        else:
            right = doubled[at][...]
        left = weights[at][..., lanes(row * channels + share_at * width, width)]
        return across(left.reshape(-1, width), right)

    scattered = {at: [] for at in order}

    def back_leave(at, start, stop):
        if start == 0:
            loads[at].wait()
        for index, peer in enumerate(peers):

            def one(row, unused):
                back_out[at][index, row] = backed(at, row, peer).astype(bf16)
                return unused

            lax.fori_loop(start, stop, one, 0)

    def back_send(at, start, stop):
        rows = pl.ds(start, stop - start)
        scattered[at] += [
            links.start(back_out[at].at[index, rows], back_in[at].at[index, rows], (me, peer))
            for index, peer in enumerate(peers)
        ]

    def back_keep(at):
        first, (blocks, parts) = FIRSTS[at], PARTS[at]

        def one(row, unused):
            value = backed(at, row, share)
            for part in range(parts):
                back[first + part * blocks + row] = value[:, part * edges : (part + 1) * edges]
            return unused

        lax.fori_loop(0, blocks, one, 0)

    def relay(at):
        relays = []
        for part, copy in enumerate(near[at][0]):
            copy.wait_recv()
            spot = grads[at].at[:, lanes((part * NEAR + (1 - pair) * 2 + low) * edges, edges)]
            relays.append(links.start(spot, spot, flip(1)))
        near[at].append(relays)

    gathered = {}

    def share_frames(at, turn_at):
        blocks, parts = PARTS[at]
        size = (blocks + 1) // 2
        if turn_at == 0:
            start = (1 - far) * (blocks - size)
        else:
            start, size = far * size, blocks - size
        ours = frames[at].reshape(blocks, shares, width, parts * edges)
        ours = ours.at[pl.ds(start, size), share]
        gathered[at, turn_at] = [links.start(ours, ours, (me, peer)) for peer in peers]

    arrivals, passing, through = {}, {}, {}
    places = (1 - far, far)

    def scatter(at, turn_at, own):
        parts = PARTS[at][1]
        place = places[turn_at]
        short = nears[at].shape[2] // parts
        cut = frames[at].reshape(2, 2, 2, 2, short, parts * edges)
        one_side = share if own else 1 - share
        if not own:
            for copy in gathered[at, turn_at]:
                copy.wait_recv()
        waits = arrivals.setdefault((at, turn_at), [])
        for part in range(parts):
            spread_lanes = pl.ds(part * edges, edges)

            def here(first_slot, slots):
                start = (part * NEAR + first_slot) * edges
                return nears[at].at[
                    place, one_side, pl.ds(0, short), lanes(start, slots * edges)
                ]

            for bit in (4, 5, 1) if own else (1,):
                its_pair = 1 - pair if bit & 4 else pair
                its_low = 1 - low if bit & 1 else low
                piece = cut.at[place, its_pair, one_side, its_low, :, spread_lanes]
                copy = links.start(piece, here(slot, 1), flip(bit))
                if bit & 4:
                    passing.setdefault((at, turn_at, part), []).append(copy)
                else:
                    waits.append(copy.wait_recv)
            piece = cut.at[place, pair, one_side, low, :, spread_lanes]
            waits.append(bring(piece, here(slot, 1)).wait)
            if own:
                through[at, turn_at, part] = here((1 - pair) * 2, 2)

    def forward(at, turn_at):
        for part in range(PARTS[at][1]):
            for copy in passing[at, turn_at, part]:
                copy.wait_recv()
            spot = through[at, turn_at, part]
            arrivals[at, turn_at].append(links.start(spot, spot, (me, peers[0])).wait_recv)

    def scatter_both(at, turn_at):
        for copy in gathered[at, turn_at]:
            copy.wait_recv()
        parts = PARTS[at][1]
        place = places[turn_at]
        short = nears[at].shape[2] // parts
        cut = frames[at].reshape(2, 2, 2, 2, short, parts * edges)
        waits = []
        for part in range(parts):
            here = nears[at].at[
                place, :, pl.ds(0, short), lanes((part * NEAR + slot) * edges, edges)
            ]
            spread_lanes = pl.ds(part * edges, edges)
            for bit in (4, 5, 1):
                its_pair = 1 - pair if bit & 4 else pair
                its_low = 1 - low if bit & 1 else low
                piece = cut.at[place, its_pair, :, its_low, :, spread_lanes]
                waits.append(links.start(piece, here, flip(bit)).wait_recv)
            waits.append(bring(cut.at[place, pair, :, low, :, spread_lanes], here).wait)
        arrivals[at, turn_at] = waits

    def mix(at):
        first, (blocks, parts) = FIRSTS[at], PARTS[at]

        def one(row, unused):
            if parts == 1:
                work[first + row] = product(weights[at][row], frames[at][...])
            else:
                real = product(weights[at][0, row], frames[at][...])
                imag = product(weights[at][1, row], frames[at][...])
                work[first + row] = real[:, :edges] - imag[:, edges:]
                work[first + blocks + row] = real[:, edges:] + imag[:, :edges]
            return unused

        lax.fori_loop(0, blocks, one, 0)

    def grown(at, place, step, one_side):
        columns = nears[at][place, one_side]
        rows = grads[at][pl.ds(pl.multiple_of(step * width, width), width), :]
        return turned(rows, columns) if at == 1 else turned(columns, rows)

    aside = {}
    away = {}
    pieces = {1: ((0, 1), (1, 2), (2, 3), (3, 4)), 0: ((0, 3), (3, 5)), 2: ((0, 3),)}

    def grow_leave(at, turn_at):
        for arrive in arrivals[at, turn_at]:
            arrive()
        if turn_at == 0:
            for group in near[at][1:]:
                for copy in group:
                    copy.wait_recv()
        parts = PARTS[at][1]
        place = places[turn_at]
        f, span = nears[at], NEAR * edges
        short = f.shape[2] // parts
        if parts == 2:
            for one_side in range(2):
                f[place, one_side, short:, :span] = -f[place, one_side, :short, span:]
                f[place, one_side, short:, span:] = f[place, one_side, :short, :span]

        def leave(step, unused):
            leaving[at][place, step] = grown(at, place, step, 1 - side).astype(bf16)
            return unused

        for index, (start, stop) in enumerate(pieces[at]):
            lax.fori_loop(start, stop, leave, 0)
            steps = pl.ds(start, stop - start)
            aside[at, turn_at, index] = links.start(
                leaving[at].at[place, steps], arriving[at].at[place, steps], flip(2)
            )

    def grow_keep(at, turn_at):
        place = places[turn_at]

        def stay(step, unused):
            kept[at][place, step] = grown(at, place, step, side)
            return unused

        lax.fori_loop(0, PARTS[at][0], stay, 0)

    def pass_on(at, index):
        start, stop = pieces[at][index]
        aside[at, 0, index].wait_recv()
        links.settle(aside[at, 0, index])
        place = places[0]

        def one(step, unused):
            total = kept[at][place, step] + arriving[at][place, step].astype(f32)
            leaving[at][place, step] = total.astype(bf16)
            return unused

        lax.fori_loop(start, stop, one, 0)
        steps = pl.ds(start, stop - start)
        away[at, index] = links.start(
            leaving[at].at[place, steps], final[at].at[steps], flip(8)
        )

    back_leave(1, 0, 2)
    back_send(1, 0, 2)
    spread(normed, to_source)
    back_leave(1, 2, 4)
    for copy in halos:
        copy.wait_recv()
    unfold(face_in, to_halo)
    for at in order:
        blocks, _ = PARTS[at]

        def put_frame(block, part, start, line):
            rows = pl.ds(pl.multiple_of(block * channels + share * width + start, tall), tall)
            frames[at][rows, part * edges : (part + 1) * edges] = line.astype(bf16)

        rotate(at, put_frame)
        if at == 1:
            share_frames(1, 0)
            scatter(1, 0, True)
            scatter(1, 1, True)

    def unturn(origin, factor, put):
        def one(step, unused):
            rows = pl.ds(pl.multiple_of(step * tall, tall), tall)
            for degree in range(5):
                members = [row for row, entry in enumerate(FRAME) if entry[0] == degree]
                lines = [origin[row, rows, :] for row in members]
                if factor is not None:
                    lines = [line * factor for line in lines]
                for column in range(degree * degree, (degree + 1) * (degree + 1)):
                    value = None
                    for row, line in zip(members, lines):
                        term = rot[column, row : row + 1, :] * line
                        value = term if value is None else value + term
                    put(column, rows, value)
            return unused

        lax.fori_loop(0, width // tall, one, 0)

    def put_normed(column, rows, value):
        normed[column, rows, :] = value.astype(bf16)

    def gather(picks, target):
        def one(step, unused):
            some = pl.ds(step * batch, batch)
            value = turned(normed[some].reshape(batch * width, edges), picks)
            target[some] = value.reshape(batch, width, atoms).astype(target.dtype)
            return unused

        lax.fori_loop(0, terms // batch, one, 0)

    def back_add():
        for at in order:
            first, (blocks, parts) = FIRSTS[at], PARTS[at]
            for copy in scattered[at]:
                copy.wait_recv()
            for index in range(shares - 1):

                def add(row, unused):
                    arrived = back_in[at][index, row].astype(f32)
                    for part in range(parts):
                        back[first + part * blocks + row] += arrived[
                            :, part * edges : (part + 1) * edges
                        ]
                    return unused

                lax.fori_loop(0, blocks, add, 0)

    share_frames(0, 0)
    near_send(0)
    back_leave(0, 0, 5)
    back_leave(2, 0, 3)
    relay(1)
    forward(1, 0)
    scatter(1, 0, False)
    share_frames(2, 0)
    share_frames(1, 1)
    forward(1, 1)
    share_frames(0, 1)
    share_frames(2, 1)
    scatter_both(0, 0)
    near_send(2)
    grow_leave(1, 0)
    grow_keep(1, 0)
    back_send(1, 2, 4)
    back_send(0, 0, 5)
    scatter_both(2, 0)
    pass_on(1, 0)
    back_keep(1)
    pass_on(1, 1)
    back_keep(0)
    pass_on(1, 2)
    pass_on(1, 3)
    scatter(1, 1, False)
    relay(0)
    back_send(2, 0, 3)
    grow_leave(0, 0)
    grow_keep(0, 0)
    scatter_both(0, 1)
    back_keep(2)
    scatter_both(2, 1)
    grow_leave(1, 1)
    grow_keep(1, 1)
    mix(1)
    pass_on(0, 0)
    pass_on(0, 1)
    mix(0)
    relay(2)
    mix(2)
    unturn(work, scale, put_normed)
    gather(to_target, arrow)
    stored = [bring(arrow, update)]
    grow_leave(2, 0)
    grow_keep(2, 0)
    back_add()
    unturn(back, None, put_normed)
    fold(to_halo, ends_out)
    ends = [
        links.start(ends_out.at[1], ends_in.at[0], after),
        links.start(ends_out.at[0], ends_in.at[1], before),
    ]
    grow_leave(0, 1)
    pass_on(2, 0)
    grow_leave(2, 1)
    gather(to_source, work)
    grow_keep(0, 1)
    grow_keep(2, 1)
    for copy in ends:
        copy.wait_recv()
    unfold(ends_in, to_face)
    total = jnp.zeros((width, atoms), f32)
    for degree in range(5):

        def scaled(term, total):
            result = work[term] * inverse * gains[degree]
            work[term] = result
            return total + result * values[term].astype(f32)

        total = lax.fori_loop(degree * degree, (degree + 1) * (degree + 1), scaled, total)
    whole = jnp.sum(total, axis=0, keepdims=True)
    tally_out[...] = jnp.broadcast_to(whole, tally_out.shape)
    tallies = [
        links.start(tally_out, tally_in.at[index], (me, peer))
        for index, peer in enumerate(peers)
    ]
    for index, copy in enumerate(tallies):
        copy.wait_recv()
        whole = whole + tally_in[index, :1, :]
    factor = inverse * inverse * whole / (terms * channels)

    def finished(term, unused):
        normed[term] = (work[term] - values[term].astype(f32) * factor).astype(bf16)
        return unused

    lax.fori_loop(0, terms, finished, 0)
    stored.append(bring(normed, grad_embed))
    for at in order:
        for index in range(len(pieces[at])):
            aside[at, 1, index].wait_recv()
            away[at, index].wait_recv()

        def settled(step, unused):
            total = kept[at][far, step] + arriving[at][far, step].astype(f32)
            kept[at][far, step] = total + final[at][step].astype(f32)
            return unused

        lax.fori_loop(0, PARTS[at][0], settled, 0)
        ready = kept[at].at[far]
        if at == 0:
            stored.append(bring(ready, outs[at]))
        else:
            for part in range(2):
                short = outs[at].shape[-1 if at == 1 else -2]
                some = pl.ds(part * short, short)
                piece = ready.at[:, :, some] if at == 1 else ready.at[:, some]
                stored.append(bring(piece, outs[at].at[part]))
    links.finish()
    for copy in stored:
        copy.wait()


def run_layer(arrays, sizes):
    embed, w_zero, w_one, w_two = arrays[0], arrays[3], arrays[4], arrays[5]
    shares, count = sizes
    terms, width, atoms = embed.shape
    edges, halo = arrays[8].shape[1], arrays[7].shape[1] // 2
    channels = width * shares
    cuts = (w_zero.shape[2] // count, w_one.shape[3] // count, w_two.shape[3] // count)
    bf16, f32 = jnp.bfloat16, jnp.float32
    three = range(3)
    tall = [blocks * width for blocks, parts in PARTS]
    wide = [parts * cut for (blocks, parts), cut in zip(PARTS, cuts)]
    near = [NEAR * parts * edges for blocks, parts in PARTS]
    scratch = [(w.shape, bf16) for w in (w_zero, w_one, w_two)]
    scratch += [((blocks * channels, parts * edges), bf16) for blocks, parts in PARTS]
    scratch += [((tall[i], near[i]), bf16) for i in three]
    scratch += [((2 * tall[i], 2 * edges), bf16) for i in (1, 2)]
    scratch += [((2, 2, wide[i], near[i]), bf16) for i in three]
    scratch += 2 * [
        ((shares - 1, blocks, width, parts * edges), bf16) for blocks, parts in PARTS
    ]
    slabs = [
        (5, wide[0], width),
        (4, width, wide[1]),
        (3, wide[2], width),
    ]
    scratch += [((2,) + slab, f32) for slab in slabs]
    scratch += 2 * [((2,) + slab, bf16) for slab in slabs]
    scratch += [(slab, bf16) for slab in slabs]
    scratch += [
        ((terms, width, edges), f32),
        ((len(FRAME), width, edges), f32),
        ((terms, width, atoms), bf16),
        ((terms, width, atoms), bf16),
        ((terms, width, atoms), bf16),
        ((terms, len(FRAME), edges), f32),
        ((5, width, atoms), f32),
    ]
    scratch += 4 * [((2, halo, terms * width), bf16)]
    scratch += 2 * [((8, atoms), f32), ((shares - 1, 8, atoms), f32)]
    scratch += [(arrays[6].shape, f32)]
    number = 16 * (shares - 1) + 15 + 50 + 24 + 4
    anywhere = pl.BlockSpec(memory_space=pl.ANY)
    inside = pl.BlockSpec(memory_space=pltpu.VMEM)
    return pl.pallas_call(
        functools.partial(layer_kernel, shares, count),
        in_specs=[anywhere] * 2 + [inside] + [anywhere] * 4 + [inside] * 5,
        out_specs=[anywhere] * 5,
        out_shape=[jax.ShapeDtypeStruct(embed.shape, bf16)] * 2
        + [
            jax.ShapeDtypeStruct((5, cuts[0], width), f32),
            jax.ShapeDtypeStruct((2, 4, width, cuts[1]), f32),
            jax.ShapeDtypeStruct((2, 3, cuts[2], width), f32),
        ],
        scratch_shapes=[pltpu.VMEM(shape, kind) for shape, kind in scratch]
        + [
            pltpu.SemaphoreType.DMA((number,)),
            pltpu.SemaphoreType.DMA((number,)),
            pltpu.SemaphoreType.DMA((48,)),
        ],
        compiler_params=pltpu.CompilerParams(
            collective_id=0, has_side_effects=True, vmem_limit_bytes=67043328
        ),
    )(*arrays)


def carry_kernel(*refs):
    count = (len(refs) - 1) // 3
    sems = refs[-1]
    origins, targets, held = refs[:count], refs[count : 2 * count], refs[2 * count : 3 * count]
    reads = [
        pltpu.make_async_copy(origin, here, sems.at[0, index])
        for index, (origin, here) in enumerate(zip(origins, held))
    ]
    writes = [
        pltpu.make_async_copy(here, target, sems.at[1, index])
        for index, (here, target) in enumerate(zip(held, targets))
    ]
    for read in reads:
        read.start()
    for read, write in zip(reads, writes):
        read.wait()
        write.start()
    for write in writes:
        write.wait()


def carry_out(arrays):
    anywhere = [pl.BlockSpec(memory_space=pl.ANY)] * len(arrays)
    return pl.pallas_call(
        carry_kernel,
        in_specs=anywhere,
        out_specs=anywhere,
        out_shape=[jax.ShapeDtypeStruct(array.shape, array.dtype) for array in arrays],
        scratch_shapes=[pltpu.VMEM(array.shape, array.dtype) for array in arrays]
        + [pltpu.SemaphoreType.DMA((2, len(arrays)))],
        compiler_params=pltpu.CompilerParams(vmem_limit_bytes=67043328),
    )(*arrays)


def shards(
    embed,
    gain,
    w_zero,
    w_one,
    w_two,
    rot_table,
    face_atoms,
    edge_source,
    edge_target,
    rot_index,
    edge_weight,
    cotangent,
):
    atoms = embed.shape[2]
    local = embed.shape[1]
    halo = face_atoms.shape[0] // 2
    shares = lax.axis_size("chan")
    channels = local * shares
    weights = (w_zero, w_one, w_two)
    values = embed.astype(jnp.float32)
    gains = gain_rows(gain)
    rows, coefficients, rots = rot_table.shape
    which = (jnp.arange(rots, dtype=jnp.int32)[:, None] == rot_index[None, :]).astype(jnp.float32)
    rotations = jnp.dot(
        rot_table.reshape(rows * coefficients, rots),
        which,
        precision=HIGHEST,
        preferred_element_type=jnp.float32,
    )
    weight_row = edge_weight[None, :]
    ones = jnp.ones_like(weight_row)

    squares = lax.psum(jnp.sum(values * values, axis=(0, 1)), "chan")
    inverse = lax.rsqrt(squares / (25 * channels) + EPSILON)
    normed = (values * inverse[None, None, :] * gains[:, :, None]).astype(jnp.bfloat16)
    flat = normed.reshape(25 * local, atoms)
    faces = product(flat, hot_rows(atoms, face_atoms)).astype(jnp.bfloat16)
    table_end = from_beside(faces.reshape(25, local, 2 * halo), halo)

    grads = to_frames([(cotangent, hot_rows(atoms, edge_target))], rotations, weight_row)
    picks = hot_rows(atoms + 2 * halo, edge_source)
    own = to_frames([(normed, picks[:atoms]), (table_end, picks[atoms:])], rotations, ones)
    own, grads = lax.optimization_barrier((own, grads))
    piece = lax.all_gather(own, "chan", axis=1, tiled=True)

    grads_side = swap(grads, 2)
    pair = swap(jnp.stack([grads, grads_side]), 1)
    grads_all = [grads, grads_side, pair[0], pair[1]]

    back = lax.psum_scatter(
        mix_back(weights, grads, shares), "chan", scatter_dimension=0, tiled=False
    )
    frames, widths = column_frames(piece)
    mixed = mix_forward(weights, piece)
    mixed, frames = lax.optimization_barrier((mixed, frames))
    (update,) = to_atoms(
        mixed, rotations, weight_row, [hot_columns(edge_target, atoms)], [jnp.bfloat16]
    )
    leaving = hot_columns(edge_source, atoms + 2 * halo)
    mine, outward = to_atoms(
        back,
        rotations,
        ones,
        [leaving[:, :atoms], leaving[:, atoms:]],
        [jnp.float32, jnp.bfloat16],
    )
    incoming = from_beside(outward, halo)
    settled = product(incoming.reshape(25 * local, 2 * halo), hot_columns(face_atoms, atoms))
    grad_normed = mine + settled.reshape(25, local, atoms)
    scaled = inverse[None, None, :] * gains[:, :, None] * grad_normed
    tally = lax.psum(jnp.sum(values * scaled, axis=(0, 1)), "chan")
    grad_embed = (
        scaled
        - values * (inverse**2 * tally / (25 * channels))[None, None, :]
    ).astype(jnp.bfloat16)
    grad_zero, grad_one, grad_two = weight_grads(frames, widths, grads_all, local)
    return (update, grad_embed, grad_zero, grad_one, grad_two)


def shards_linked(
    embed,
    gain,
    w_zero,
    w_one,
    w_two,
    rot_table,
    face_atoms,
    edge_source,
    edge_target,
    rot_index,
    edge_weight,
    cotangent,
):
    arrays = (
        embed,
        cotangent,
        gain,
        w_zero,
        w_one,
        w_two,
        jnp.transpose(rot_table, (1, 0, 2)),
        face_atoms[None, :],
        edge_source[None, :],
        edge_target[None, :],
        rot_index[None, :],
        edge_weight[None, :],
    )
    sizes = (lax.axis_size("chan"), lax.axis_size("graph"))
    update, grad_embed, done_zero, done_one, done_two = carry_out(run_layer(arrays, sizes))
    grad_zero = jnp.transpose(done_zero, (0, 2, 1))
    grad_two = jnp.transpose(done_two, (0, 1, 3, 2))
    return (update, grad_embed, grad_zero, done_one, grad_two)


def solution(mesh):
    placed = (
        P(None, "chan", "graph"),
        P(None, "chan"),
        P(None, "chan", None),
        P(None, None, "chan", None),
        P(None, None, "chan", None),
        P(),
        P("graph"),
        P("graph"),
        P("graph"),
        P("graph"),
        P("graph"),
        P(None, "chan", "graph"),
    )
    linked = mesh.shape["graph"] == 16 and mesh.shape["chan"] == 2
    return jax.shard_map(
        shards_linked if linked else shards,
        mesh=mesh,
        in_specs=placed,
        out_specs=(
            P(None, "chan", "graph"),
            P(None, "chan", "graph"),
            P(None, "chan", "graph"),
            P(None, None, "chan", "graph"),
            P(None, None, "chan", "graph"),
        ),
        check_vma=False,
    )
```
